512 devices in a mesh: lat: 16 (over y, core), lon: 32 (over z, x).
Axes of the slice: x: 4, y: 8, z: 8, core: 2. Of those that a mesh axis runs over, the one named last changes fastest.
Arguments:
- forcing: float32 [2560, 4096], P('lat', 'lon'), may hold values from -28 to 28
- search_direction: float32 [2560, 4096], P('lat', 'lon'), may hold values from -28 to 28
- ocean_depth: float32 [2560, 4096], P('lat', 'lon'), may hold values from 0.5 to 8
- land_mask: int32 [2560, 4096], P('lat', 'lon'), may hold values 0 or 1
- fold_map: int32 [4096], replicated, may hold values from 0 to 4095, as said below
Outputs:
- scaled_height: float32 [2560, 4096], P('lat', 'lon')
- residual: float32 [2560, 4096], P('lat', 'lon')
The draws below stay inside these ranges and needn't reach their ends.
Inputs may be any that keep to these rules, and one draw needn't show every extreme that they name: `fold_map`: column j's partner across the fold is (c - j) mod 4096 for one c of 0 to 4095, so the map is its own inverse.
All inputs are finite; a program needn't handle non-finite values. No bound on the sum of `land_mask` on one device may be relied on, other than what follows from the above.
Results may differ from the reference program's by a relative error of at most 0.0003.
Values sent between devices are 32-bit elements; how exact they have to be, the bound alone decides.
A program may use at most 64 MiB of HBM per device.

```python
import math
import jax
import jax.numpy as jnp
import numpy as np
from jax import lax

STEPS = 8
OUTER = 1
REACH = 256
NX = 2560
NY = 4096


def field_profile():
    lat_ramp = jnp.arange(NX, dtype=jnp.float32) / NX
    lon_ramp = jnp.arange(NY, dtype=jnp.float32) / NY
    north_gap = (NX - 1 - jnp.arange(NX, dtype=jnp.float32)) / 8.0
    north_boost = 1.0 + 1.5 * jnp.exp(-north_gap)
    return jnp.exp(jnp.log(3.0) * (lat_ramp[:, None] + lon_ramp[None, :])) * north_boost[:, None]


def rough_field(key):
    first_key = jax.random.fold_in(key, 0)
    values = jax.random.truncated_normal(first_key, -4.0, 4.0, (NX, NY), jnp.float32)
    return (0.3 * values * field_profile()).astype(jnp.float32)


def draw_forcing(key, part):
    return rough_field(jax.random.fold_in(key, 11))


def draw_search_direction(key, part):
    return rough_field(jax.random.fold_in(key, 23))


def draw_fold_map(key, part):
    pivot_column = jax.random.randint(jax.random.fold_in(key, 7), (), 0, NY, dtype=jnp.int32)
    return ((pivot_column - jnp.arange(NY, dtype=jnp.int32)) % NY).astype(jnp.int32)


def set_ends(drawn, stream_key, smallest, top_value):
    longest = drawn.shape.index(max(drawn.shape))
    spots = []
    for shift in (0, 1):
        where = [jax.random.randint(jax.random.fold_in(stream_key, axis), (), 0, length) for axis, length in enumerate(drawn.shape)]
        where[longest] = (where[longest] + shift) % drawn.shape[longest]
        spots.append(tuple(where))
    return drawn.at[spots[0]].set(smallest).at[spots[1]].set(top_value)


def level_of(key, extent, pieces, low, largest):
    level = 1.0
    for dim, shards_of in pieces:
        draws = jax.random.uniform(jax.random.fold_in(jax.random.fold_in(key, 6), dim), (shards_of,), jnp.float32, low / len(pieces), largest / len(pieces))
        level = level * jnp.repeat(jnp.exp(draws), extent[dim] // shards_of).reshape((-1,) + (1,) * (len(extent) - 1 - dim))
    return level


def setup_inputs(seed: int = 0) -> dict:
    key_of = jax.random.split(jax.random.key(seed), 6)
    forcing = draw_forcing(jax.random.fold_in(key_of[5], 71), 0)
    search_direction = draw_search_direction(jax.random.fold_in(key_of[5], 71), 0)
    ocean_depth = jnp.clip(jnp.exp(math.log(8.0) - 2.7725887 * jax.random.uniform(key_of[2], (NX, NY), jnp.float32) ** level_of(key_of[2], (NX, NY), ((0, 16), (1, 32)), -0.2, 0.2)), 0.5, 8.0)
    land_mask = set_ends((jax.random.randint(key_of[3], (NX, NY), 0, 8) < 7).astype(jnp.int32), jax.random.fold_in(key_of[3], 1), 0, 1)
    fold_map = draw_fold_map(jax.random.fold_in(key_of[5], 71), 0)
    return dict(forcing=forcing, search_direction=search_direction, ocean_depth=ocean_depth, land_mask=land_mask, fold_map=fold_map)


PRECISE = lax.Precision.HIGHEST
DIRECTIONS = ((1, 0), (-1, 0), (0, 1), (0, -1), (1, 1), (-1, -1), (1, -1), (-1, 1))
LINK_FACTORS = (1.0, 1.0, 1.0, 1.0, 0.5, 0.5, 0.5, 0.5)

def chebyshev_table(basis_steps):
    number = 2 * basis_steps + 1
    matrix = np.zeros((number, number), np.float32)
    for offset, length in ((0, basis_steps + 1), (basis_steps + 1, basis_steps)):
        for column in range(length - 1):
            matrix[offset + column, offset + column] = 1.0
            if column == 0:
                matrix[offset + 1, offset] = 1.0
            else:
                matrix[offset + column + 1, offset + column] = 0.5
                matrix[offset + column - 1, offset + column] = 0.5
    return matrix

def coordinates(gram_matrix, basis_steps):
    number = 2 * basis_steps + 1
    shift_matrix = jnp.asarray(chebyshev_table(basis_steps))
    unit_rows = jnp.eye(number, dtype=jnp.float32)
    solution_coords = jnp.zeros((number,), jnp.float32)
    direction_coords = unit_rows[0]
    residual_coords = unit_rows[basis_steps + 1]
    norm_now = jnp.dot(residual_coords, jnp.dot(gram_matrix, residual_coords, precision=PRECISE), precision=PRECISE)
    for inner_step in range(basis_steps):
        mapped = jnp.dot(shift_matrix, direction_coords, precision=PRECISE)
        curvature = jnp.dot(direction_coords, jnp.dot(gram_matrix, mapped, precision=PRECISE), precision=PRECISE)
        step_length = norm_now / curvature
        solution_coords = solution_coords + step_length * direction_coords
        residual_coords = residual_coords - step_length * mapped
        norm_next = jnp.dot(residual_coords, jnp.dot(gram_matrix, residual_coords, precision=PRECISE), precision=PRECISE)
        direction_coords = residual_coords + norm_next / norm_now * direction_coords
        norm_now = norm_next
    return (solution_coords, residual_coords, direction_coords)

def pad_ghosts(source, fold_map):
    fold_row = jnp.take(source[-1], fold_map)
    zeros_row = jnp.zeros((1, source.shape[1]), source.dtype)
    stacked = jnp.concatenate([zeros_row, source, fold_row[None, :]], axis=0)
    return jnp.concatenate([stacked[:, -1:], stacked, stacked[:, :1]], axis=1)

def neighbour(padded, north_step, east_step):
    row_total = padded.shape[0] - 2
    column_total = padded.shape[1] - 2
    return padded[1 + north_step:1 + north_step + row_total, 1 + east_step:1 + east_step + column_total]

def reference(forcing, search_direction, ocean_depth, land_mask, fold_map):
    ocean_flag = land_mask.astype(jnp.float32)
    column_depth = ocean_depth * ocean_flag
    padded_depth = pad_ghosts(column_depth, fold_map)
    padded_wet = (padded_depth > 0.0).astype(jnp.float32)
    centre_wet = padded_wet[1:-1, 1:-1]
    weight_list = []
    link_sum = jnp.zeros_like(column_depth)
    for direction_index in range(8):
        north_step, east_step = DIRECTIONS[direction_index]
        weight = LINK_FACTORS[direction_index] * 0.5 * (column_depth + neighbour(padded_depth, north_step, east_step)) * centre_wet * neighbour(padded_wet, north_step, east_step)
        weight_list.append(weight)
        link_sum = link_sum + weight
    diagonal = centre_wet * (column_depth / (REACH * REACH) + link_sum) + (1.0 - centre_wet)
    inverse_root = lax.rsqrt(diagonal)

    def operate(source):
        padded = pad_ghosts(inverse_root * source, fold_map)
        running = jnp.zeros_like(source)
        for direction_index in range(8):
            north_step, east_step = DIRECTIONS[direction_index]
            running = running + weight_list[direction_index] * neighbour(padded, north_step, east_step)
        return -inverse_root * running
    operate_many = jax.vmap(operate)
    scaled_height = jnp.zeros_like(forcing)
    residual = ocean_flag * forcing
    direction = ocean_flag * search_direction
    for outer_step in range(OUTER):
        earlier = jnp.stack([direction, residual])
        current = operate_many(earlier)
        stored = [earlier, current]
        for power in range(1, STEPS):
            if power == STEPS - 1:
                earlier = earlier[:1]
                current = current[:1]
            upcoming = 2.0 * operate_many(current) - earlier
            earlier = current
            current = upcoming
            stored.append(current)
        krylov_basis = jnp.stack([member[0] for member in stored] + [member[1] for member in stored[:STEPS]])
        flattened = krylov_basis.reshape(krylov_basis.shape[0], -1)
        gram_matrix = jnp.dot(flattened, flattened.T, precision=PRECISE)
        solution_coords, residual_coords, direction_coords = coordinates(gram_matrix, STEPS)
        scaled_height = scaled_height + jnp.einsum('k,kij->ij', solution_coords, krylov_basis, precision=PRECISE)
        residual = jnp.einsum('k,kij->ij', residual_coords, krylov_basis, precision=PRECISE)
        direction = jnp.einsum('k,kij->ij', direction_coords, krylov_basis, precision=PRECISE)
    return (scaled_height, residual)
```

```python
import functools

import jax
import jax.numpy as jnp
from jax import lax
from jax.experimental import pallas as pl
from jax.experimental.pallas import tpu as pltpu
from jax.sharding import PartitionSpec as P

STEPS = 8
REACH = 256
LAT, LON, NX, NZ = 16, 32, 4, 8
ROWS, COLS = 160, 128
EXT = ROWS + 32
LO, HI = 8, 184
FIELDS = 2 * STEPS + 1
FIRST = STEPS + 1
HIGHEST = lax.Precision.HIGHEST
F32 = jnp.float32


def lanes_of(shape):
    return lax.broadcasted_iota(jnp.int32, shape, len(shape) - 1)


def from_east(main, side):
    lane = lanes_of(main.shape)
    a, b = pltpu.roll(main, COLS - 1, 1), pltpu.roll(side, COLS - 1, 1)
    last = lane == COLS - 1
    return jnp.where(last, b, a), jnp.where(last, a, b)


def from_west(main, side):
    lane = lanes_of(main.shape)
    a, b = pltpu.roll(main, 1, 1), pltpu.roll(side, 1, 1)
    head = lane == 0
    return jnp.where(head, b, a), jnp.where(head, a, b)


def remote(src, dst, send, recv, lat, lon):
    return pltpu.make_async_remote_copy(
        src_ref=src,
        dst_ref=dst,
        send_sem=send,
        recv_sem=recv,
        device_id={"lat": lat, "lon": lon},
        device_id_type=pl.DeviceIdType.MESH,
    )


CHUNK = 16


def far_first(count):
    return sorted(range(1, count), key=lambda d: (-min(d, count - d), d))


def chunks():
    return [(r, min(CHUNK, HI - r)) for r in range(LO, HI, CHUNK)]


def basis_kernel(
    fold_ref, forcing_ref, search_ref, depth_ref, mask_ref,
    basis_out, moments_out,
    raw_m, raw_h, depth_buf, mask_buf, pack_w, pack_e, got_w, got_e, corner,
    fold_x, fold_src, fold_z, fold_send, fold_got,
    wet_m, wet_h, s_m, s_h, de_m, de_h, se_m, se_h,
    w_m, w_h, b_m, b_h, rows_acc, part, red_x, red_z, red_y,
    local_sem, out_sem, halo_send, halo_recv, fz_send, fz_recv, fx_send, fx_recv,
    rx_send, rx_recv, rz_send, rz_recv, ry_send, ry_recv,
):
    lat = lax.axis_index("lat")
    lon = lax.axis_index("lon")
    zi, xi = lon // NX, lon % NX
    top = lat == LAT - 1
    bottom = lat == 0
    north, south = (lat + 1) % LAT, (lat + LAT - 1) % LAT
    east, west = (lon + 1) % LON, (lon + LON - 1) % LON
    barrier = pltpu.get_barrier_semaphore()

    peers = [(lat, ((zi + d) % NZ) * NX + xi) for d in far_first(NZ)]
    peers += [((lat + d) % LAT, lon) for d in far_first(LAT)]
    peers += [(north, east), (north, west), (south, east), (south, west)]
    peers += [(lat, zi * NX + (xi + d) % NX) for d in far_first(NX)]
    peers += [(lat, east), (lat, west)]
    for a, b in peers:
        pl.semaphore_signal(
            barrier, inc=1, device_id={"lat": a, "lon": b}, device_id_type=pl.DeviceIdType.MESH
        )

    loads = [
        pltpu.make_async_copy(depth_ref, depth_buf, local_sem.at[0]),
        pltpu.make_async_copy(mask_ref, mask_buf, local_sem.at[1]),
        pltpu.make_async_copy(forcing_ref, raw_m.at[1, pl.ds(16, ROWS), :], local_sem.at[2]),
        pltpu.make_async_copy(search_ref, raw_m.at[2, pl.ds(16, ROWS), :], local_sem.at[3]),
    ]
    for copy in loads:
        copy.start()
    rows_acc[...] = jnp.zeros_like(rows_acc)
    for copy in loads:
        copy.wait()
    raw_m[0, 16 : 16 + ROWS, :] = depth_buf[...] * mask_buf[...].astype(F32)

    lane40 = lanes_of((40, COLS))
    acc_w = jnp.zeros((40, COLS), F32)
    acc_e = jnp.zeros((40, COLS), F32)
    for g in range(4):
        for f in range(3):
            at = 32 * g + 9 * f
            block = raw_m[f, 16 + 40 * g : 56 + 40 * g, :]
            here = (lane40 >= at) & (lane40 < at + 9)
            acc_w = jnp.where(here, pltpu.roll(block, at, 1) if at else block, acc_w)
            acc_e = jnp.where(here, pltpu.roll(block, (at - 119) % COLS, 1), acc_e)
    pack_w[...] = acc_w
    pack_e[...] = acc_e

    pivot = fold_ref[0]
    pivot_block, pivot_lane = lax.shift_right_logical(pivot, 7), pivot & (COLS - 1)

    @pl.when(top)
    def _():
        fold_x[...] = jnp.zeros_like(fold_x)
        for m in range(9):
            fold_x[m : m + 1, :] = raw_m[0, 175 - m : 176 - m, :]
        for m in range(8):
            fold_x[9 + m : 10 + m, :] = raw_m[1, 175 - m : 176 - m, :]
            fold_x[17 + m : 18 + m, :] = raw_m[2, 175 - m : 176 - m, :]
        source = lax.broadcasted_iota(jnp.int32, (COLS, COLS), 0)
        target = lax.broadcasted_iota(jnp.int32, (COLS, COLS), 1)
        choose = (source == ((pivot - target) & (COLS - 1))).astype(F32)
        turned = jnp.dot(fold_x[...], choose, precision=HIGHEST, preferred_element_type=F32)
        fold_src[...] = turned
        fold_z[zi] = turned

    pl.semaphore_wait(barrier, len(peers))

    to_north = remote(raw_m.at[:, pl.ds(160, 16), :], raw_m.at[:, pl.ds(0, 16), :],
                      halo_send.at[0], halo_recv.at[0], north, lon)
    to_south = remote(raw_m.at[:, pl.ds(16, 16), :], raw_m.at[:, pl.ds(176, 16), :],
                      halo_send.at[1], halo_recv.at[1], south, lon)
    to_east = remote(pack_e, got_w, halo_send.at[2], halo_recv.at[2], lat, east)
    to_west = remote(pack_w, got_e, halo_send.at[3], halo_recv.at[3], lat, west)
    to_ne = remote(pack_e.at[pl.ds(24, 16), :], corner.at[0], halo_send.at[4], halo_recv.at[4], north, east)
    to_nw = remote(pack_w.at[pl.ds(24, 16), :], corner.at[1], halo_send.at[5], halo_recv.at[5], north, west)
    to_se = remote(pack_e.at[pl.ds(0, 16), :], corner.at[2], halo_send.at[6], halo_recv.at[6], south, east)
    to_sw = remote(pack_w.at[pl.ds(0, 16), :], corner.at[3], halo_send.at[7], halo_recv.at[7], south, west)

    fold_z_copies = []
    for d in range(1, NZ):
        peer = (zi + d) % NZ
        fold_z_copies.append(
            remote(fold_src, fold_z.at[zi], fz_send.at[d - 1], fz_recv.at[d - 1], lat, peer * NX + xi)
        )

    @pl.when(top)
    def _():
        for d in far_first(NZ):
            fold_z_copies[d - 1].start()

    @pl.when(jnp.logical_not(top))
    def _():
        to_ne.start()
        to_nw.start()
        to_north.start()

    @pl.when(jnp.logical_not(bottom))
    def _():
        to_se.start()
        to_sw.start()
        to_south.start()

    to_east.start()
    to_west.start()

    def fold_want(xt):
        want = (pivot_block - zi * NX - xt) & (LON - 1)
        return want

    @pl.when(top)
    def _():
        for d in range(1, NZ):
            fold_z_copies[d - 1].wait_recv()
        picks = []
        for d in range(NX):
            xt = (xi + d) % NX
            ahead = fold_want(xt) + 1
            block = ahead - ((ahead - xi) & (NX - 1))
            picks.append(fold_z[lax.shift_right_logical(block & (LON - 1), 2)])
        fold_got[xi] = picks[0]
        copies = []
        for d in range(1, NX):
            fold_send[d] = picks[d]
        for d in range(1, NX):
            copy = remote(fold_send.at[d], fold_got.at[xi], fx_send.at[d - 1], fx_recv.at[d - 1],
                          lat, zi * NX + (xi + d) % NX)
            copy.start()
            copies.append(copy)
        for copy in copies:
            copy.wait_recv()
        want = fold_want(xi)
        ahead2, here2, behind, behind2 = (
            fold_got[(want + 1) & 3], fold_got[want & 3], fold_got[(want - 1) & 3], fold_got[(want - 2) & 3]
        )
        lane = lanes_of((32, COLS))
        near = lane <= pivot_lane
        ghost_m = jnp.where(near, here2, behind)
        ghost_e = jnp.where(near, behind, behind2)
        ghost_w = jnp.where(near, ahead2, here2)
        ghost_h = jnp.where(lane < 9, ghost_e, jnp.where(lane >= 119, ghost_w, 0.0))
        for ref, ghost in ((raw_m, ghost_m), (raw_h, ghost_h)):
            for f in range(3):
                ref[f, 176:192, :] = jnp.zeros((16, COLS), F32)
            ref[0, 176:185, :] = ghost[0:9]
            ref[1, 176:184, :] = ghost[9:17]
            ref[2, 176:184, :] = ghost[17:25]
        for copy in copies:
            copy.wait_send()
        for copy in fold_z_copies:
            copy.wait_send()

    to_east.wait()
    to_west.wait()

    lane16 = lanes_of((16, COLS))
    for g in range(4):
        for f in range(3):
            at = 32 * g + 9 * f
            near_e = pltpu.roll(got_e[...], (COLS - at) % COLS, 1) if at else got_e[...]
            near_w = pltpu.roll(got_w[...], (119 - at) % COLS, 1)
            raw_h[f, 16 + 40 * g : 56 + 40 * g, :] = jnp.where(
                lane40 < 9, near_e, jnp.where(lane40 >= 119, near_w, 0.0)
            )

    @pl.when(jnp.logical_not(bottom))
    def _():
        to_se.wait_send()
        to_sw.wait_send()
        to_south.wait_send()
        to_ne.wait_recv()
        to_nw.wait_recv()
        to_north.wait_recv()
        for f in range(3):
            at = 96 + 9 * f
            near_e = pltpu.roll(corner[1], (COLS - at) % COLS, 1)
            near_w = pltpu.roll(corner[0], (119 - at) % COLS, 1)
            raw_h[f, 0:16, :] = jnp.where(lane16 < 9, near_e, jnp.where(lane16 >= 119, near_w, 0.0))

    @pl.when(bottom)
    def _():
        for f in range(3):
            raw_m[f, 0:16, :] = jnp.zeros((16, COLS), F32)
            raw_h[f, 0:16, :] = jnp.zeros((16, COLS), F32)

    @pl.when(jnp.logical_not(top))
    def _():
        to_ne.wait_send()
        to_nw.wait_send()
        to_north.wait_send()
        to_se.wait_recv()
        to_sw.wait_recv()
        to_south.wait_recv()
        for f in range(3):
            at = 9 * f
            near_e = pltpu.roll(corner[3], (COLS - at) % COLS, 1) if at else corner[3]
            near_w = pltpu.roll(corner[2], (119 - at) % COLS, 1)
            raw_h[f, 176:192, :] = jnp.where(lane16 < 9, near_e, jnp.where(lane16 >= 119, near_w, 0.0))

    for r, n in chunks():
        sums = []
        for raw in (raw_m, raw_h):
            up, mid, low = (raw[0, r + o : r + o + n, :] for o in (1, 0, -1))
            both = up + low
            wets = [(v > 0.0).astype(F32) for v in (up, mid, low)]
            both_wet = wets[0] + wets[2]
            sums.append((mid, both, mid + 0.5 * both, wets[1], both_wet, wets[1] + 0.5 * both_wet))
        (dm, bm, cm, wm, bwm, cwm), (dh, bh, ch, wh, bwh, cwh) = sums
        e_m, e_h = from_east(cm, ch)
        w_m_, w_h_ = from_west(cm, ch)
        ew_m, ew_h = from_east(cwm, cwh)
        ww_m, ww_h = from_west(cwm, cwh)
        rooted = []
        for depth, wet, all_depth, all_wet in (
            (dm, wm, bm + (e_m + w_m_), bwm + (ew_m + ww_m)),
            (dh, wh, bh + (e_h + w_h_), bwh + (ew_h + ww_h)),
        ):
            links = 0.5 * (depth * all_wet + all_depth)
            diagonal = wet * (depth * (1.0 / (REACH * REACH)) + links) + (1.0 - wet)
            rooted.append(wet * lax.rsqrt(diagonal))
        s_m[r : r + n, :], s_h[r : r + n, :] = rooted
        se_m[r : r + n, :], se_h[r : r + n, :] = from_east(*rooted)
        de_m[r : r + n, :], de_h[r : r + n, :] = from_east(dm, dh)
        b_m[0, r : r + n, :] = wm * raw_m[2, r : r + n, :]
        b_h[0, r : r + n, :] = wh * raw_h[2, r : r + n, :]
        b_m[FIRST, r : r + n, :] = wm * raw_m[1, r : r + n, :]
        b_h[FIRST, r : r + n, :] = wh * raw_h[1, r : r + n, :]

    for r, n in chunks():
        made = []
        for raw, s, de, se, w in ((raw_m, s_m, de_m, se_m, w_m), (raw_h, s_h, de_h, se_h, w_h)):
            d0, d1 = raw[0, r : r + n, :], raw[0, r + 1 : r + 1 + n, :]
            s0, s1 = s[r : r + n, :], s[r + 1 : r + 1 + n, :]
            de0, de1 = de[r : r + n, :], de[r + 1 : r + 1 + n, :]
            se0, se1 = se[r : r + n, :], se[r + 1 : r + 1 + n, :]
            east_w = -(d0 + de0) * (s0 * se0)
            ne_w = -0.5 * (d0 + de1) * (s0 * se1)
            nw_e = -0.5 * (de0 + d1) * (se0 * s1)
            w[0, r : r + n, :] = -(d0 + d1) * (s0 * s1)
            w[1, r : r + n, :] = east_w
            w[3, r : r + n, :] = ne_w
            w[6, r : r + n, :] = nw_e
            made.append((east_w, ne_w, nw_e))
        for slot, item in ((2, 0), (4, 1), (5, 2)):
            w_m[slot, r : r + n, :], w_h[slot, r : r + n, :] = from_west(made[0][item], made[1][item])

    def fold8(x):
        return sum(x[8 * k : 8 * k + 8] for k in range(x.shape[0] // 8))

    def row_slices(r, n):
        return max(r, 16) - r, min(r + n, 16 + ROWS) - r

    def step(n, both, first):
        bases = (0, FIRST) if both else (0,)
        total = [jnp.zeros((8, COLS), F32) for _ in range(6)]
        for r, size in chunks():
            weights = []
            for w in (w_m, w_h):
                weights.append((
                    w[0, r : r + size, :], w[0, r - 1 : r - 1 + size, :],
                    w[4, r : r + size, :], w[2, r : r + size, :], w[5, r - 1 : r - 1 + size, :],
                    w[6, r : r + size, :], w[1, r : r + size, :], w[3, r - 1 : r - 1 + size, :],
                ))
            news, olds = [], []
            for base in bases:
                zs = []
                for b, (a_u, a_d, e_u, e_c, e_d, f_u, f_c, f_d) in zip((b_m, b_h), weights):
                    k = base + n - 1
                    up = b[k, r + 1 : r + 1 + size, :]
                    mid = b[k, r : r + size, :]
                    low = b[k, r - 1 : r - 1 + size, :]
                    z0 = a_u * up + a_d * low
                    ze = e_u * up + e_c * mid + e_d * low
                    zw = f_u * up + f_c * mid + f_d * low
                    zs.append((mid, z0, ze, zw))
                (mid_m, z0_m, ze_m, zw_m), (mid_h, z0_h, ze_h, zw_h) = zs
                ze_m, ze_h = from_east(ze_m, ze_h)
                zw_m, zw_h = from_west(zw_m, zw_h)
                out_m, out_h = z0_m + (ze_m + zw_m), z0_h + (ze_h + zw_h)
                if first:
                    out_m, out_h = 0.5 * out_m, 0.5 * out_h
                else:
                    out_m = out_m - b_m[base + n - 2, r : r + size, :]
                    out_h = out_h - b_h[base + n - 2, r : r + size, :]
                b_m[base + n, r : r + size, :] = out_m
                b_h[base + n, r : r + size, :] = out_h
                news.append(out_m)
                olds.append(mid_m)
            lo, hi = row_slices(r, size)
            if hi > lo:
                p1, p0 = news[0][lo:hi], olds[0][lo:hi]
                total[0] = total[0] + fold8(p1 * p1)
                total[1] = total[1] + fold8(p1 * p0)
                if both:
                    r1, r0 = news[1][lo:hi], olds[1][lo:hi]
                    total[2] = total[2] + fold8(r1 * r1)
                    total[3] = total[3] + fold8(r1 * r0)
                    total[4] = total[4] + fold8(p1 * r1)
                else:
                    r0 = b_m[FIRST + STEPS - 1, r + lo : r + hi, :]
                total[5] = total[5] + fold8(p1 * r0)
        for c in range(6):
            rows_acc[pl.ds(6 * n + c, 1), :] = jnp.sum(total[c], axis=0, keepdims=True)

    start = [jnp.zeros((8, COLS), F32) for _ in range(3)]
    for r in range(16, 16 + ROWS, CHUNK):
        p0, r0 = b_m[0, r : r + CHUNK, :], b_m[FIRST, r : r + CHUNK, :]
        start = [t + fold8(v) for t, v in zip(start, (p0 * p0, r0 * r0, p0 * r0))]
    for c in range(3):
        rows_acc[2 * c : 2 * c + 1, :] = jnp.sum(start[c], axis=0, keepdims=True)

    step(1, True, True)

    @pl.loop(2, STEPS)
    def _(n):
        step(n, True, False)

    step(STEPS, False, False)

    outs = [
        pltpu.make_async_copy(b_m.at[k, pl.ds(16, ROWS), :], basis_out.at[k], out_sem.at[k])
        for k in range(FIELDS)
    ]
    for copy in outs:
        copy.start()

    ones = jnp.ones((8, COLS), F32)
    sums = lax.dot_general(
        ones, rows_acc[...], (((1,), (1,)), ((), ())), precision=HIGHEST, preferred_element_type=F32
    )[0:1]

    def reduce(stage, value, slots, send, recv, count, mine, peer_of, order):
        slots[mine] = value
        part[stage] = value
        copies = [
            remote(part.at[stage], slots.at[mine], send.at[d - 1], recv.at[d - 1], *peer_of(d))
            for d in range(1, count)
        ]
        for d in order:
            copies[d - 1].start()
        for copy in copies:
            copy.wait_recv()
        total = slots[0]
        for k in range(1, count):
            total = total + slots[k]
        return total, copies

    sums, first_copies = reduce(
        0, sums, red_x, rx_send, rx_recv, NX, xi,
        lambda d: (lat, zi * NX + (xi + d) % NX), far_first(NX))
    sums, second_copies = reduce(
        1, sums, red_z, rz_send, rz_recv, NZ, zi,
        lambda d: (lat, ((zi + d) % NZ) * NX + xi), far_first(NZ))
    sums, third_copies = reduce(
        2, sums, red_y, ry_send, ry_recv, LAT, lat,
        lambda d: ((lat + d) % LAT, lon), far_first(LAT))
    moments_out[...] = sums
    for copy in first_copies + second_copies + third_copies:
        copy.wait_send()
    for copy in outs:
        copy.wait()


def basis_and_moments(forcing, search, depth, mask, fold_map):
    vm = pltpu.VMEM
    dma = pltpu.SemaphoreType.DMA
    ext = (EXT, COLS)
    return pl.pallas_call(
        basis_kernel,
        grid=(1,),
        out_shape=(
            jax.ShapeDtypeStruct((FIELDS, ROWS, COLS), F32),
            jax.ShapeDtypeStruct((1, COLS), F32),
        ),
        in_specs=[pl.BlockSpec((1024,), lambda i: (0,), memory_space=pltpu.SMEM)]
        + [pl.BlockSpec(memory_space=pl.ANY)] * 4,
        out_specs=(
            pl.BlockSpec(memory_space=pl.ANY),
            pl.BlockSpec((1, COLS), lambda i: (0, 0)),
        ),
        scratch_shapes=[
            vm((3,) + ext, F32), vm((3,) + ext, F32),
            vm((ROWS, COLS), F32), vm((ROWS, COLS), jnp.int32),
            vm((40, COLS), F32), vm((40, COLS), F32), vm((40, COLS), F32), vm((40, COLS), F32),
            vm((4, 16, COLS), F32),
            vm((32, COLS), F32), vm((32, COLS), F32), vm((NZ, 32, COLS), F32),
            vm((NX, 32, COLS), F32), vm((NX, 32, COLS), F32),
        ]
        + [vm(ext, F32)] * 8
        + [vm((7,) + ext, F32)] * 2
        + [vm((FIELDS,) + ext, F32)] * 2
        + [
            vm((COLS, COLS), F32), vm((3, 1, COLS), F32),
            vm((NX, 1, COLS), F32), vm((NZ, 1, COLS), F32), vm((LAT, 1, COLS), F32),
            dma((4,)), dma((FIELDS,)), dma((8,)), dma((8,)),
            dma((NZ - 1,)), dma((NZ - 1,)), dma((NX - 1,)), dma((NX - 1,)),
            dma((NX - 1,)), dma((NX - 1,)), dma((NZ - 1,)), dma((NZ - 1,)),
            dma((LAT - 1,)), dma((LAT - 1,)),
        ],
        compiler_params=pltpu.CompilerParams(collective_id=0, has_side_effects=True),
        name="basis",
    )(fold_map, forcing, search, depth, mask)


def combine_kernel(moments_ref, basis_ref, height_ref, residual_ref):
    shape = (24, COLS)
    row = lax.broadcasted_iota(jnp.int32, shape, 0)
    col = lanes_of(shape)

    def power(i):
        return jnp.where(i >= FIRST, i - FIRST, i)

    kind = jnp.where((row >= FIRST) & (col >= FIRST), 1, jnp.where((row >= FIRST) | (col >= FIRST), 2, 0))
    valid = (row < FIELDS) & (col < FIELDS)
    ka, kb = power(row), power(col)
    high, low = ka + kb, jnp.abs(ka - kb)
    odd = high & 1

    def slot(k):
        return jnp.where(valid, 6 * ((k + 1) >> 1) + 2 * kind + odd, 0)

    base = jnp.where(odd == 1, 7 + 2 * kind, 2 * kind)
    raw = jnp.broadcast_to(moments_ref[...], shape)

    def take(index):
        return jnp.take_along_axis(raw, index, axis=1)

    gram = jnp.where(valid, take(slot(high)) + take(slot(low)) - take(jnp.where(valid, base, 0)), 0.0)

    def lower(i):
        return jnp.where((i == 1) | (i == FIRST + 1), 1.0, jnp.where((i >= 1) & (i < FIELDS) & (i != FIRST), 0.5, 0.0))

    def upper(i):
        return jnp.where((i < FIELDS - 2) & (i != FIRST - 2) & (i != FIRST - 1), 0.5, 0.0)

    low_l, up_l = lower(col).astype(F32), upper(col).astype(F32)
    low_s, up_s = lower(row).astype(F32), upper(row).astype(F32)

    def shifted(v, axis):
        length = v.shape[axis]
        low_c, up_c = (low_s, up_s) if axis == 0 else (low_l, up_l)
        return v + low_c * pltpu.roll(v, 1, axis) + up_c * pltpu.roll(v, length - 1, axis)

    below = pltpu.roll(low_l, COLS - 1, 1)
    above = pltpu.roll(up_l, 1, 1)
    ends = (col == FIRST - 1) | (col == FIELDS - 1)
    gram_h = jnp.where(
        ends, 0.0,
        gram + below * pltpu.roll(gram, COLS - 1, 1) + jnp.where(col > 0, above, 0.0) * pltpu.roll(gram, 1, 1),
    )

    def form(matrix, left, right):
        return jnp.sum(matrix * left * right, keepdims=True)

    unit = lambda at: ((row == at).astype(F32), (col == at).astype(F32))
    p_s, p_l = unit(0)
    r_s, r_l = unit(FIRST)
    q_s, q_l = shifted(p_s, 0), shifted(p_l, 1)
    x_s = jnp.zeros(shape, F32)
    norm = form(gram, r_s, r_l)
    curvature = form(gram_h, p_s, p_l)
    for inner in range(STEPS):
        t = norm / curvature
        x_s = x_s + t * p_s
        r_s = r_s - t * q_s
        if inner == STEPS - 1:
            break
        r_l = r_l - t * q_l
        h_s, h_l = shifted(r_s, 0), shifted(r_l, 1)
        fresh = form(gram, r_s, r_l)
        own = form(gram_h, r_s, r_l)
        cross = form(gram_h, r_s, p_l)
        beta = fresh / norm
        curvature = own + beta * (2.0 * cross + beta * curvature)
        norm = fresh
        p_s, p_l = r_s + beta * p_s, r_l + beta * p_l
        q_s, q_l = h_s + beta * q_s, h_l + beta * q_l

    size = 32
    for at in range(0, ROWS, size):
        height = jnp.zeros((size, COLS), F32)
        residual = jnp.zeros((size, COLS), F32)
        for k in range(FIELDS):
            field = basis_ref[k, at : at + size, :]
            height = height + x_s[k : k + 1, :] * field
            residual = residual + r_s[k : k + 1, :] * field
        height_ref[at : at + size, :] = height
        residual_ref[at : at + size, :] = residual


def per_device(forcing, search, depth, mask, fold_map):
    basis, moments = basis_and_moments(forcing, search, depth, mask, fold_map)
    block = jax.ShapeDtypeStruct((ROWS, COLS), F32)
    return pl.pallas_call(
        combine_kernel,
        out_shape=(block, block),
        name="combine",
    )(moments, basis)


def solution(mesh):
    return jax.shard_map(
        per_device,
        mesh=mesh,
        in_specs=(P("lat", "lon"),) * 4 + (P(),),
        out_specs=(P("lat", "lon"),) * 2,
        check_vma=False,
    )
```

```python
import functools

import jax
import jax.numpy as jnp
from jax import lax
from jax.experimental import pallas as pl
from jax.experimental.pallas import tpu as pltpu
from jax.sharding import PartitionSpec as P

STEPS = 8
REACH = 256
LAT, LON, NX, NZ = 16, 32, 4, 8
ROWS, COLS = 160, 128
EXT = ROWS + 32
LO = 8
FIELDS = 2 * STEPS + 1
FIRST = STEPS + 1
HIGHEST = lax.Precision.HIGHEST
F32 = jnp.float32


def lanes_of(shape):
    return lax.broadcasted_iota(jnp.int32, shape, len(shape) - 1)


def from_east(main, side):
    lane = lanes_of(main.shape)
    a, b = pltpu.roll(main, COLS - 1, 1), pltpu.roll(side, COLS - 1, 1)
    last = lane == COLS - 1
    return jnp.where(last, b, a), jnp.where(last, a, b)


def from_west(main, side):
    lane = lanes_of(main.shape)
    a, b = pltpu.roll(main, 1, 1), pltpu.roll(side, 1, 1)
    head = lane == 0
    return jnp.where(head, b, a), jnp.where(head, a, b)


def remote(src, dst, send, recv, lat, lon):
    return pltpu.make_async_remote_copy(
        src_ref=src,
        dst_ref=dst,
        send_sem=send,
        recv_sem=recv,
        device_id={"lat": lat, "lon": lon},
        device_id_type=pl.DeviceIdType.MESH,
    )


CHUNK = 16


def far_first(count):
    return sorted(range(1, count), key=lambda d: (-min(d, count - d), d))


def chunks(start, stop):
    return [(r, min(CHUNK, stop - r)) for r in range(start, stop, CHUNK)]


def basis_kernel(
    fold_ref, forcing_ref, search_ref, depth_ref, mask_ref,
    b_m, moments_out,
    fold_buf, raw_m, raw_h, depth_buf, mask_buf, pack_w, pack_e, got_w, got_e, corner,
    fold_x, fold_src, fold_row, fold_send, fold_got,
    wet_m, wet_h, s_m, s_h, de_m, de_h, se_m, se_h,
    w_m, w_h, b_h, rows_acc, part, red_p, red_y,
    plane_sem, local_sem, halo_send, halo_recv, fz_send, fz_recv, fx_send, fx_recv,
    rp_send, rp_recv, ry_send, ry_recv,
):
    lat = lax.axis_index("lat")
    lon = lax.axis_index("lon")
    zi, xi = lon // NX, lon % NX
    top = lat == LAT - 1
    bottom = lat == 0
    north, south = (lat + 1) % LAT, (lat + LAT - 1) % LAT
    east, west = (lon + 1) % LON, (lon + LON - 1) % LON
    barrier = pltpu.get_barrier_semaphore()

    loads = [
        pltpu.make_async_copy(depth_ref, depth_buf, local_sem.at[0]),
        pltpu.make_async_copy(mask_ref, mask_buf, local_sem.at[1]),
        pltpu.make_async_copy(forcing_ref, raw_m.at[1, pl.ds(16, ROWS), :], local_sem.at[2]),
        pltpu.make_async_copy(search_ref, raw_m.at[2, pl.ds(16, ROWS), :], local_sem.at[3]),
        pltpu.make_async_copy(fold_ref.at[pl.ds(0, 1024)], fold_buf, local_sem.at[4]),
    ]
    for copy in loads:
        copy.start()
    peers = [(lat, ((zi + d) % NZ) * NX + xi) for d in far_first(NZ)]
    peers += [((lat + d) % LAT, lon) for d in far_first(LAT)]
    peers += [(north, east), (north, west), (south, east), (south, west)]
    peers += [(lat, zi * NX + (xi + d) % NX) for d in far_first(NX)]
    peers += [(lat, east), (lat, west)]
    for a, b in peers:
        pl.semaphore_signal(
            barrier, inc=1, device_id={"lat": a, "lon": b}, device_id_type=pl.DeviceIdType.MESH
        )

    rows_acc[...] = jnp.zeros_like(rows_acc)
    for copy in loads:
        copy.wait()
    raw_m[0, 16 : 16 + ROWS, :] = depth_buf[...] * mask_buf[...].astype(F32)

    lane40 = lanes_of((40, COLS))
    acc_w = jnp.zeros((40, COLS), F32)
    acc_e = jnp.zeros((40, COLS), F32)
    for g in range(4):
        for f in range(3):
            at = 32 * g + 9 * f
            block = raw_m[f, 16 + 40 * g : 56 + 40 * g, :]
            here = (lane40 >= at) & (lane40 < at + 9)
            acc_w = jnp.where(here, pltpu.roll(block, at, 1) if at else block, acc_w)
            acc_e = jnp.where(here, pltpu.roll(block, (at - 119) % COLS, 1), acc_e)
    pack_w[...] = acc_w
    pack_e[...] = acc_e

    pivot = fold_buf[0]
    pivot_block, pivot_lane = lax.shift_right_logical(pivot, 7), pivot & (COLS - 1)

    @pl.when(top)
    def _():
        fold_x[...] = jnp.zeros_like(fold_x)
        for m in range(9):
            fold_x[m : m + 1, :] = raw_m[0, 175 - m : 176 - m, :]
        for m in range(8):
            fold_x[9 + m : 10 + m, :] = raw_m[1, 175 - m : 176 - m, :]
            fold_x[17 + m : 18 + m, :] = raw_m[2, 175 - m : 176 - m, :]
        source = lax.broadcasted_iota(jnp.int32, (COLS, COLS), 0)
        target = lax.broadcasted_iota(jnp.int32, (COLS, COLS), 1)
        choose = (source == ((pivot - target) & (COLS - 1))).astype(F32)
        turned = jnp.dot(fold_x[...], choose, precision=HIGHEST, preferred_element_type=F32)
        fold_src[...] = turned
        fold_row[xi] = turned
        fold_row[NX] = jnp.zeros_like(turned)

    pl.semaphore_wait(barrier, len(peers))

    fold_x_copies = [
        remote(fold_src, fold_row.at[xi], fx_send.at[d - 1], fx_recv.at[d - 1], lat, zi * NX + (xi + d) % NX)
        for d in range(1, NX)
    ]

    @pl.when(top)
    def _():
        for d in far_first(NX):
            fold_x_copies[d - 1].start()

    to_north = remote(raw_m.at[:, pl.ds(160, 16), :], raw_m.at[:, pl.ds(0, 16), :],
                      halo_send.at[0], halo_recv.at[0], north, lon)
    to_south = remote(raw_m.at[:, pl.ds(16, 16), :], raw_m.at[:, pl.ds(176, 16), :],
                      halo_send.at[1], halo_recv.at[1], south, lon)
    to_east = remote(pack_e, got_w, halo_send.at[2], halo_recv.at[2], lat, east)
    to_west = remote(pack_w, got_e, halo_send.at[3], halo_recv.at[3], lat, west)
    to_ne = remote(pack_e.at[pl.ds(24, 16), :], corner.at[0], halo_send.at[4], halo_recv.at[4], north, east)
    to_nw = remote(pack_w.at[pl.ds(24, 16), :], corner.at[1], halo_send.at[5], halo_recv.at[5], north, west)
    to_se = remote(pack_e.at[pl.ds(0, 16), :], corner.at[2], halo_send.at[6], halo_recv.at[6], south, east)
    to_sw = remote(pack_w.at[pl.ds(0, 16), :], corner.at[3], halo_send.at[7], halo_recv.at[7], south, west)

    @pl.when(jnp.logical_not(top))
    def _():
        to_ne.start()
        to_nw.start()
        to_north.start()

    @pl.when(jnp.logical_not(bottom))
    def _():
        to_se.start()
        to_sw.start()
        to_south.start()

    to_east.start()
    to_west.start()

    to_east.wait()
    to_west.wait()

    lane16 = lanes_of((16, COLS))
    for g in range(4):
        for f in range(3):
            at = 32 * g + 9 * f
            near_e = pltpu.roll(got_e[...], (COLS - at) % COLS, 1) if at else got_e[...]
            near_w = pltpu.roll(got_w[...], (119 - at) % COLS, 1)
            raw_h[f, 16 + 40 * g : 56 + 40 * g, :] = jnp.where(
                lane40 < 9, near_e, jnp.where(lane40 >= 119, near_w, 0.0)
            )

    for d in far_first(NZ):
        pl.semaphore_signal(
            plane_sem, inc=1, device_id={"lat": lat, "lon": ((zi + d) % NZ) * NX + xi},
            device_id_type=pl.DeviceIdType.MESH,
        )

    fold_z_copies = [
        remote(fold_send.at[d], fold_got.at[zi], fz_send.at[d - 1], fz_recv.at[d - 1],
               lat, ((zi + d) % NZ) * NX + xi)
        for d in range(1, NZ)
    ]
    lane32 = lanes_of((32, COLS))
    near = lane32 <= pivot_lane

    @pl.when(top)
    def _():
        for copy in fold_x_copies:
            copy.wait_recv()
        for d in far_first(NZ) + [0]:
            want = pivot_block - ((zi + d) % NZ) * NX - xi

            def block(b):
                mine = (lax.shift_right_logical(b & (LON - 1), 2) == zi)
                return fold_row[jnp.where(mine, b & (NX - 1), NX)]

            ahead, here, behind, beyond = (block(want + o) for o in (1, 0, -1, -2))
            window = jnp.where(near, here, behind)
            edge = jnp.where(
                lane32 < 9, jnp.where(near, behind, beyond),
                jnp.where(lane32 >= 119, jnp.where(near, ahead, here), 0.0),
            )
            edges = sum(pltpu.roll(edge[8 * g : 8 * g + 8], 16 + 32 * g, 1) for g in range(4))
            if d:
                fold_send[d, 0:32, :] = window
                fold_send[d, 32:40, :] = edges
                fold_z_copies[d - 1].start()
            else:
                fold_got[zi, 0:32, :] = window
                fold_got[zi, 32:40, :] = edges

    @pl.when(jnp.logical_not(bottom))
    def _():
        to_se.wait_send()
        to_sw.wait_send()
        to_south.wait_send()
        to_ne.wait_recv()
        to_nw.wait_recv()
        to_north.wait_recv()
        for f in range(3):
            at = 96 + 9 * f
            near_e = pltpu.roll(corner[1], (COLS - at) % COLS, 1)
            near_w = pltpu.roll(corner[0], (119 - at) % COLS, 1)
            raw_h[f, 0:16, :] = jnp.where(lane16 < 9, near_e, jnp.where(lane16 >= 119, near_w, 0.0))

    @pl.when(bottom)
    def _():
        for f in range(3):
            raw_m[f, 0:16, :] = jnp.zeros((16, COLS), F32)
            raw_h[f, 0:16, :] = jnp.zeros((16, COLS), F32)

    def fields(spans):
        for r, n in spans:
            for raw, b in ((raw_m, b_m), (raw_h, b_h)):
                wet = (raw[0, r : r + n, :] > 0.0).astype(F32)
                b[0, r : r + n, :] = wet * raw[2, r : r + n, :]
                b[FIRST, r : r + n, :] = wet * raw[1, r : r + n, :]

    def roots(spans):
        for r, n in spans:
            sums = []
            for raw in (raw_m, raw_h):
                up, mid, low = (raw[0, r + o : r + o + n, :] for o in (1, 0, -1))
                both = up + low
                wets = [(v > 0.0).astype(F32) for v in (up, mid, low)]
                both_wet = wets[0] + wets[2]
                sums.append((mid, both, mid + 0.5 * both, wets[1], both_wet, wets[1] + 0.5 * both_wet))
            (dm, bm, cm, wm, bwm, cwm), (dh, bh, ch, wh, bwh, cwh) = sums
            e_m, e_h = from_east(cm, ch)
            w_m_, w_h_ = from_west(cm, ch)
            ew_m, ew_h = from_east(cwm, cwh)
            ww_m, ww_h = from_west(cwm, cwh)
            rooted = []
            for depth, wet, all_depth, all_wet in (
                (dm, wm, bm + (e_m + w_m_), bwm + (ew_m + ww_m)),
                (dh, wh, bh + (e_h + w_h_), bwh + (ew_h + ww_h)),
            ):
                links = 0.5 * (depth * all_wet + all_depth)
                diagonal = wet * (depth * (1.0 / (REACH * REACH)) + links) + (1.0 - wet)
                rooted.append(wet * lax.rsqrt(diagonal))
            s_m[r : r + n, :], s_h[r : r + n, :] = rooted
            se_m[r : r + n, :], se_h[r : r + n, :] = from_east(*rooted)
            de_m[r : r + n, :], de_h[r : r + n, :] = from_east(dm, dh)

    def links(spans):
        for r, n in spans:
            made = []
            for raw, s, de, se, w in ((raw_m, s_m, de_m, se_m, w_m), (raw_h, s_h, de_h, se_h, w_h)):
                d0, d1 = raw[0, r : r + n, :], raw[0, r + 1 : r + 1 + n, :]
                s0, s1 = s[r : r + n, :], s[r + 1 : r + 1 + n, :]
                de0, de1 = de[r : r + n, :], de[r + 1 : r + 1 + n, :]
                se0, se1 = se[r : r + n, :], se[r + 1 : r + 1 + n, :]
                east_w = -(d0 + de0) * (s0 * se0)
                ne_w = -0.5 * (d0 + de1) * (s0 * se1)
                nw_e = -0.5 * (de0 + d1) * (se0 * s1)
                w[0, r : r + n, :] = -(d0 + d1) * (s0 * s1)
                w[1, r : r + n, :] = east_w
                w[3, r : r + n, :] = ne_w
                w[6, r : r + n, :] = nw_e
                made.append((east_w, ne_w, nw_e))
            for slot, item in ((2, 0), (4, 1), (5, 2)):
                w_m[slot, r : r + n, :], w_h[slot, r : r + n, :] = from_west(made[0][item], made[1][item])

    def fold8(x):
        return sum(x[8 * k : 8 * k + 8] for k in range(x.shape[0] // 8))

    def step(n, both, first, spans, gram_rows, add):
        bases = (0, FIRST) if both else (0,)
        total = [jnp.zeros((8, COLS), F32) for _ in range(6)]
        for r, size in spans:
            weights = []
            for w in (w_m, w_h):
                weights.append((
                    w[0, r : r + size, :], w[0, r - 1 : r - 1 + size, :],
                    w[4, r : r + size, :], w[2, r : r + size, :], w[5, r - 1 : r - 1 + size, :],
                    w[6, r : r + size, :], w[1, r : r + size, :], w[3, r - 1 : r - 1 + size, :],
                ))
            news, olds = [], []
            for base in bases:
                zs = []
                for b, (a_u, a_d, e_u, e_c, e_d, f_u, f_c, f_d) in zip((b_m, b_h), weights):
                    k = base + n - 1
                    up = b[k, r + 1 : r + 1 + size, :]
                    mid = b[k, r : r + size, :]
                    low = b[k, r - 1 : r - 1 + size, :]
                    z0 = a_u * up + a_d * low
                    ze = e_u * up + e_c * mid + e_d * low
                    zw = f_u * up + f_c * mid + f_d * low
                    zs.append((mid, z0, ze, zw))
                (mid_m, z0_m, ze_m, zw_m), (mid_h, z0_h, ze_h, zw_h) = zs
                ze_m, ze_h = from_east(ze_m, ze_h)
                zw_m, zw_h = from_west(zw_m, zw_h)
                out_m, out_h = z0_m + (ze_m + zw_m), z0_h + (ze_h + zw_h)
                if first:
                    out_m, out_h = 0.5 * out_m, 0.5 * out_h
                else:
                    out_m = out_m - b_m[base + n - 2, r : r + size, :]
                    out_h = out_h - b_h[base + n - 2, r : r + size, :]
                b_m[base + n, r : r + size, :] = out_m
                b_h[base + n, r : r + size, :] = out_h
                news.append(out_m)
                olds.append(mid_m)
            lo, hi = max(r, gram_rows[0]) - r, min(r + size, gram_rows[1]) - r
            if hi > lo:
                p1, p0 = news[0][lo:hi], olds[0][lo:hi]
                total[0] = total[0] + fold8(p1 * p1)
                total[1] = total[1] + fold8(p1 * p0)
                if both:
                    r1, r0 = news[1][lo:hi], olds[1][lo:hi]
                    total[2] = total[2] + fold8(r1 * r1)
                    total[3] = total[3] + fold8(r1 * r0)
                    total[4] = total[4] + fold8(p1 * r1)
                else:
                    r0 = b_m[FIRST + STEPS - 1, r + lo : r + hi, :]
                total[5] = total[5] + fold8(p1 * r0)
        for c in range(6):
            row = jnp.sum(total[c], axis=0, keepdims=True)
            at = pl.ds(6 * n + c, 1)
            rows_acc[at, :] = rows_acc[at, :] + row if add else row

    def steps(spans, gram_rows, add):
        step(1, True, True, spans, gram_rows, add)

        @pl.loop(2, STEPS)
        def _(n):
            step(n, True, False, spans, gram_rows, add)

        step(STEPS, False, False, spans, gram_rows, add)

    fields(chunks(LO, 176))
    roots(chunks(LO, 168) + [(168, 7)])
    links(chunks(LO, 168))
    start = [jnp.zeros((8, COLS), F32) for _ in range(3)]
    for r in range(16, 16 + ROWS, CHUNK):
        p0, r0 = b_m[0, r : r + CHUNK, :], b_m[FIRST, r : r + CHUNK, :]
        start = [t + fold8(v) for t, v in zip(start, (p0 * p0, r0 * r0, p0 * r0))]
    for c in range(3):
        rows_acc[2 * c : 2 * c + 1, :] = jnp.sum(start[c], axis=0, keepdims=True)

    steps(chunks(LO, 168), (16, 160), False)

    @pl.when(jnp.logical_not(top))
    def _():
        to_ne.wait_send()
        to_nw.wait_send()
        to_north.wait_send()
        to_se.wait_recv()
        to_sw.wait_recv()
        to_south.wait_recv()
        for f in range(3):
            at = 9 * f
            near_e = pltpu.roll(corner[3], (COLS - at) % COLS, 1) if at else corner[3]
            near_w = pltpu.roll(corner[2], (119 - at) % COLS, 1)
            raw_h[f, 176:192, :] = jnp.where(lane16 < 9, near_e, jnp.where(lane16 >= 119, near_w, 0.0))

    @pl.when(top)
    def _():
        for copy in fold_z_copies:
            copy.wait_recv()
        ghost = fold_got[0]
        for k in range(1, NZ):
            ghost = ghost + fold_got[k]
        edges = ghost[32:40]
        lane8 = lanes_of((8, COLS))
        side = []
        for g in range(4):
            edge = pltpu.roll(edges, (COLS - 16 - 32 * g) % COLS, 1)
            side.append(jnp.where((lane8 < 9) | (lane8 >= 119), edge, 0.0))
        side = jnp.concatenate(side, axis=0)
        for ref, got in ((raw_m, ghost), (raw_h, side)):
            for f in range(3):
                ref[f, 176:192, :] = jnp.zeros((16, COLS), F32)
            ref[0, 176:185, :] = got[0:9]
            ref[1, 176:184, :] = got[9:17]
            ref[2, 176:184, :] = got[17:25]
        for copy in fold_x_copies + fold_z_copies:
            copy.wait_send()

    fields([(176, 8)])
    roots([(168, 16)])
    links([(168, 16)])
    steps([(160, 24)], (160, 176), True)

    ones = jnp.ones((8, COLS), F32)
    sums = lax.dot_general(
        ones, rows_acc[...], (((1,), (1,)), ((), ())), precision=HIGHEST, preferred_element_type=F32
    )[0:1]

    def reduce(stage, value, slots, send, recv, count, mine, peer_of, order):
        slots[mine] = value
        part[stage] = value
        copies = [
            remote(part.at[stage], slots.at[mine], send.at[d - 1], recv.at[d - 1], *peer_of(d))
            for d in range(1, count)
        ]
        for d in order:
            copies[d - 1].start()
        for copy in copies:
            copy.wait_recv()
        terms = [slots[k] for k in range(count)]
        while len(terms) > 1:
            terms = [a + b for a, b in zip(terms[::2], terms[1::2])]
        return terms[0], copies

    pl.semaphore_wait(plane_sem, NZ - 1)
    sums, first_copies = reduce(
        0, sums, red_p, rp_send, rp_recv, LON, lon,
        lambda d: (lat, (lon + d) % LON), far_first(LON))
    sums, second_copies = reduce(
        1, sums, red_y, ry_send, ry_recv, LAT, lat,
        lambda d: ((lat + d) % LAT, lon), far_first(LAT))
    moments_out[...] = sums
    for copy in first_copies + second_copies:
        copy.wait_send()


def held(shape):
    return pltpu.VMEM(shape, F32)


def basis_and_moments(forcing, search, depth, mask, fold_map):
    vm = pltpu.VMEM
    dma = pltpu.SemaphoreType.DMA
    ext = (EXT, COLS)
    return pl.pallas_call(
        basis_kernel,
        out_shape=(held((FIELDS,) + ext), held((1, COLS))),
        in_specs=[pl.BlockSpec(memory_space=pl.ANY)] * 5,
        out_specs=(pl.BlockSpec(memory_space=vm), pl.BlockSpec(memory_space=vm)),
        scratch_shapes=[
            pltpu.SMEM((1024,), jnp.int32),
            vm((3,) + ext, F32), vm((3,) + ext, F32),
            vm((ROWS, COLS), F32), vm((ROWS, COLS), jnp.int32),
            vm((40, COLS), F32), vm((40, COLS), F32), vm((40, COLS), F32), vm((40, COLS), F32),
            vm((4, 16, COLS), F32),
            vm((32, COLS), F32), vm((32, COLS), F32), vm((NX + 1, 32, COLS), F32),
            vm((NZ, 40, COLS), F32), vm((NZ, 40, COLS), F32),
        ]
        + [vm(ext, F32)] * 8
        + [vm((7,) + ext, F32)] * 2
        + [vm((FIELDS,) + ext, F32)]
        + [
            vm((COLS, COLS), F32), vm((2, 1, COLS), F32),
            vm((LON, 1, COLS), F32), vm((LAT, 1, COLS), F32),
            pltpu.SemaphoreType.REGULAR, dma((5,)), dma((8,)), dma((8,)),
            dma((NZ - 1,)), dma((NZ - 1,)), dma((NX - 1,)), dma((NX - 1,)),
            dma((LON - 1,)), dma((LON - 1,)), dma((LAT - 1,)), dma((LAT - 1,)),
        ],
        compiler_params=pltpu.CompilerParams(collective_id=0, has_side_effects=True),
        name="basis",
    )(fold_map, forcing, search, depth, mask)


def combine_kernel(moments_ref, basis_ref, height_ref, residual_ref):
    shape = (24, COLS)
    row = lax.broadcasted_iota(jnp.int32, shape, 0)
    col = lanes_of(shape)

    def power(i):
        return jnp.where(i >= FIRST, i - FIRST, i)

    kind = jnp.where((row >= FIRST) & (col >= FIRST), 1, jnp.where((row >= FIRST) | (col >= FIRST), 2, 0))
    valid = (row < FIELDS) & (col < FIELDS)
    ka, kb = power(row), power(col)
    high, low = ka + kb, jnp.abs(ka - kb)
    odd = high & 1

    def slot(k):
        return jnp.where(valid, 6 * ((k + 1) >> 1) + 2 * kind + odd, 0)

    base = jnp.where(odd == 1, 7 + 2 * kind, 2 * kind)
    raw = jnp.broadcast_to(moments_ref[...], shape)

    def take(index):
        return jnp.take_along_axis(raw, index, axis=1)

    gram = jnp.where(valid, take(slot(high)) + take(slot(low)) - take(jnp.where(valid, base, 0)), 0.0)

    def lower(i):
        return jnp.where((i == 1) | (i == FIRST + 1), 1.0, jnp.where((i >= 1) & (i < FIELDS) & (i != FIRST), 0.5, 0.0))

    def upper(i):
        return jnp.where((i < FIELDS - 2) & (i != FIRST - 2) & (i != FIRST - 1), 0.5, 0.0)

    low_l, up_l = lower(col).astype(F32), upper(col).astype(F32)
    low_s, up_s = lower(row).astype(F32), upper(row).astype(F32)

    def shifted(v, axis):
        length = v.shape[axis]
        low_c, up_c = (low_s, up_s) if axis == 0 else (low_l, up_l)
        return v + low_c * pltpu.roll(v, 1, axis) + up_c * pltpu.roll(v, length - 1, axis)

    below = pltpu.roll(low_l, COLS - 1, 1)
    above = pltpu.roll(up_l, 1, 1)
    ends = (col == FIRST - 1) | (col == FIELDS - 1)
    gram_h = jnp.where(
        ends, 0.0,
        gram + below * pltpu.roll(gram, COLS - 1, 1) + jnp.where(col > 0, above, 0.0) * pltpu.roll(gram, 1, 1),
    )

    def form(matrix, left, right):
        return jnp.sum(matrix * left * right, keepdims=True)

    unit = lambda at: ((row == at).astype(F32), (col == at).astype(F32))
    p_s, p_l = unit(0)
    r_s, r_l = unit(FIRST)
    q_s, q_l = shifted(p_s, 0), shifted(p_l, 1)
    x_s = jnp.zeros(shape, F32)
    norm = form(gram, r_s, r_l)
    curvature = form(gram_h, p_s, p_l)
    for inner in range(STEPS):
        t = norm / curvature
        x_s = x_s + t * p_s
        r_s = r_s - t * q_s
        if inner == STEPS - 1:
            break
        r_l = r_l - t * q_l
        h_s, h_l = shifted(r_s, 0), shifted(r_l, 1)
        fresh = form(gram, r_s, r_l)
        own = form(gram_h, r_s, r_l)
        cross = form(gram_h, r_s, p_l)
        beta = fresh / norm
        curvature = own + beta * (2.0 * cross + beta * curvature)
        norm = fresh
        p_s, p_l = r_s + beta * p_s, r_l + beta * p_l
        q_s, q_l = h_s + beta * q_s, h_l + beta * q_l

    size = 32
    for at in range(0, ROWS, size):
        height = jnp.zeros((size, COLS), F32)
        residual = jnp.zeros((size, COLS), F32)
        for k in range(FIELDS):
            field = basis_ref[k, 16 + at : 16 + at + size, :]
            height = height + x_s[k : k + 1, :] * field
            residual = residual + r_s[k : k + 1, :] * field
        height_ref[at : at + size, :] = height
        residual_ref[at : at + size, :] = residual


def per_device(forcing, search, depth, mask, fold_map):
    basis, moments = basis_and_moments(forcing, search, depth, mask, fold_map)
    basis, moments = (pltpu.with_memory_space_constraint(v, pltpu.VMEM) for v in (basis, moments))
    block = jax.ShapeDtypeStruct((ROWS, COLS), F32)
    return pl.pallas_call(
        combine_kernel,
        out_shape=(block, block),
        in_specs=[pl.BlockSpec(memory_space=pltpu.VMEM)] * 2,
        name="combine",
    )(moments, basis)


def solution(mesh):
    return jax.shard_map(
        per_device,
        mesh=mesh,
        in_specs=(P("lat", "lon"),) * 4 + (P(),),
        out_specs=(P("lat", "lon"),) * 2,
        check_vma=False,
    )
```

```python
import functools

import jax
import jax.numpy as jnp
from jax import lax
from jax.experimental import pallas as pl
from jax.experimental.pallas import tpu as pltpu
from jax.sharding import PartitionSpec as P

STEPS = 8
REACH = 256
LAT, LON, NX, NZ = 16, 32, 4, 8
ROWS, COLS = 160, 128
EXT = ROWS + 32
LO = 8
FIELDS = 2 * STEPS + 1
FIRST = STEPS + 1
HIGHEST = lax.Precision.HIGHEST
F32 = jnp.float32


def lanes_of(shape):
    return lax.broadcasted_iota(jnp.int32, shape, len(shape) - 1)


def from_east(main, side):
    lane = lanes_of(main.shape)
    a, b = pltpu.roll(main, COLS - 1, 1), pltpu.roll(side, COLS - 1, 1)
    last = lane == COLS - 1
    return jnp.where(last, b, a), jnp.where(last, a, b)


def from_west(main, side):
    lane = lanes_of(main.shape)
    a, b = pltpu.roll(main, 1, 1), pltpu.roll(side, 1, 1)
    head = lane == 0
    return jnp.where(head, b, a), jnp.where(head, a, b)


def remote(src, dst, send, recv, lat, lon):
    return pltpu.make_async_remote_copy(
        src_ref=src,
        dst_ref=dst,
        send_sem=send,
        recv_sem=recv,
        device_id={"lat": lat, "lon": lon},
        device_id_type=pl.DeviceIdType.MESH,
    )


CHUNK = 16


def far_first(count):
    return sorted(range(1, count), key=lambda d: (-min(d, count - d), d))


def chunks(start, stop):
    return [(r, min(CHUNK, stop - r)) for r in range(start, stop, CHUNK)]


def basis_kernel(
    fold_ref, forcing_ref, search_ref, depth_ref, mask_ref,
    b_m, moments_out,
    fold_buf, raw_m, raw_h, depth_buf, mask_buf, pack_w, pack_e, got_w, got_e, corner,
    fold_x, fold_src, fold_row, fold_send, fold_got,
    wet_m, wet_h, s_m, s_h, de_m, de_h, se_m, se_h,
    w_m, w_h, b_h, rows_acc, part, red_p, red_y,
    plane_sem, local_sem, halo_send, halo_recv, fz_send, fz_recv, fx_send, fx_recv,
    rp_send, rp_recv, ry_send, ry_recv,
):
    lat = lax.axis_index("lat")
    lon = lax.axis_index("lon")
    zi, xi = lon // NX, lon % NX
    top = lat == LAT - 1
    bottom = lat == 0
    north, south = (lat + 1) % LAT, (lat + LAT - 1) % LAT
    east, west = (lon + 1) % LON, (lon + LON - 1) % LON
    barrier = pltpu.get_barrier_semaphore()

    loads = [
        pltpu.make_async_copy(depth_ref, depth_buf, local_sem.at[0]),
        pltpu.make_async_copy(mask_ref, mask_buf, local_sem.at[1]),
        pltpu.make_async_copy(forcing_ref, raw_m.at[1, pl.ds(16, ROWS), :], local_sem.at[2]),
        pltpu.make_async_copy(search_ref, raw_m.at[2, pl.ds(16, ROWS), :], local_sem.at[3]),
        pltpu.make_async_copy(fold_ref.at[pl.ds(0, 1024)], fold_buf, local_sem.at[4]),
    ]
    for copy in loads:
        copy.start()
    def greet(semaphore, to):
        for a, b in to:
            pl.semaphore_signal(
                semaphore, inc=1, device_id={"lat": a, "lon": b}, device_id_type=pl.DeviceIdType.MESH
            )

    fold_peers = [(lat, ((zi + d) % NZ) * NX + xi) for d in far_first(NZ)]
    fold_peers += [(lat, zi * NX + (xi + d) % NX) for d in far_first(NX)]
    beside = [(lat, east), (lat, west), (north, east), (north, west), (south, east), (south, west),
              (north, lon), (south, lon)]

    @pl.when(top)
    def _():
        greet(barrier, fold_peers)

    greet(barrier, beside)

    def distant(level):
        far = 1 << level
        to = [(lat, (lon + far) % LON), (lat, (lon + LON - far) % LON)]
        if 2 * far <= LAT // 2:
            to += [((lat + far) % LAT, lon), ((lat + LAT - far) % LAT, lon)]
        return to

    levels = 1
    while (2 << (levels - 1)) < LON // 2:
        levels += 1

    passed = set()

    def next_level(level):
        if level > levels or level in passed:
            return
        passed.add(level)
        if level > 0:
            pl.semaphore_wait(plane_sem.at[level - 1], len(distant(level - 1)))
        if level < levels:
            greet(plane_sem.at[level], distant(level))

    rows_acc[...] = jnp.zeros_like(rows_acc)
    for copy in loads:
        copy.wait()
    raw_m[0, 16 : 16 + ROWS, :] = depth_buf[...] * mask_buf[...].astype(F32)

    lane40 = lanes_of((40, COLS))
    acc_w = jnp.zeros((40, COLS), F32)
    acc_e = jnp.zeros((40, COLS), F32)
    for g in range(4):
        for f in range(3):
            at = 32 * g + 9 * f
            block = raw_m[f, 16 + 40 * g : 56 + 40 * g, :]
            here = (lane40 >= at) & (lane40 < at + 9)
            acc_w = jnp.where(here, pltpu.roll(block, at, 1) if at else block, acc_w)
            acc_e = jnp.where(here, pltpu.roll(block, (at - 119) % COLS, 1), acc_e)
    pack_w[...] = acc_w
    pack_e[...] = acc_e

    pivot = fold_buf[0]
    pivot_block, pivot_lane = lax.shift_right_logical(pivot, 7), pivot & (COLS - 1)

    @pl.when(top)
    def _():
        fold_x[...] = jnp.zeros_like(fold_x)
        for m in range(9):
            fold_x[m : m + 1, :] = raw_m[0, 175 - m : 176 - m, :]
        for m in range(8):
            fold_x[9 + m : 10 + m, :] = raw_m[1, 175 - m : 176 - m, :]
            fold_x[17 + m : 18 + m, :] = raw_m[2, 175 - m : 176 - m, :]
        source = lax.broadcasted_iota(jnp.int32, (COLS, COLS), 0)
        target = lax.broadcasted_iota(jnp.int32, (COLS, COLS), 1)
        choose = (source == ((pivot - target) & (COLS - 1))).astype(F32)
        turned = jnp.dot(fold_x[...], choose, precision=HIGHEST, preferred_element_type=F32)
        fold_src[...] = turned
        fold_row[xi] = turned
        fold_row[NX] = jnp.zeros_like(turned)

    pl.semaphore_wait(barrier, len(beside) + jnp.where(top, len(fold_peers), 0))

    fold_x_copies = [
        remote(fold_src, fold_row.at[xi], fx_send.at[d - 1], fx_recv.at[d - 1], lat, zi * NX + (xi + d) % NX)
        for d in range(1, NX)
    ]

    @pl.when(top)
    def _():
        for d in far_first(NX):
            fold_x_copies[d - 1].start()

    to_north = remote(raw_m.at[:, pl.ds(160, 16), :], raw_m.at[:, pl.ds(0, 16), :],
                      halo_send.at[0], halo_recv.at[0], north, lon)
    to_south = remote(raw_m.at[:, pl.ds(16, 16), :], raw_m.at[:, pl.ds(176, 16), :],
                      halo_send.at[1], halo_recv.at[1], south, lon)
    to_east = remote(pack_e, got_w, halo_send.at[2], halo_recv.at[2], lat, east)
    to_west = remote(pack_w, got_e, halo_send.at[3], halo_recv.at[3], lat, west)
    to_ne = remote(pack_e.at[pl.ds(24, 16), :], corner.at[0], halo_send.at[4], halo_recv.at[4], north, east)
    to_nw = remote(pack_w.at[pl.ds(24, 16), :], corner.at[1], halo_send.at[5], halo_recv.at[5], north, west)
    to_se = remote(pack_e.at[pl.ds(0, 16), :], corner.at[2], halo_send.at[6], halo_recv.at[6], south, east)
    to_sw = remote(pack_w.at[pl.ds(0, 16), :], corner.at[3], halo_send.at[7], halo_recv.at[7], south, west)

    to_east.start()
    to_west.start()
    next_level(0)

    @pl.when(jnp.logical_not(top))
    def _():
        to_ne.start()
        to_nw.start()
        to_north.start()

    @pl.when(jnp.logical_not(bottom))
    def _():
        to_se.start()
        to_sw.start()
        to_south.start()

    to_east.wait()
    to_west.wait()

    lane16 = lanes_of((16, COLS))
    for g in range(4):
        for f in range(3):
            at = 32 * g + 9 * f
            near_e = pltpu.roll(got_e[...], (COLS - at) % COLS, 1) if at else got_e[...]
            near_w = pltpu.roll(got_w[...], (119 - at) % COLS, 1)
            raw_h[f, 16 + 40 * g : 56 + 40 * g, :] = jnp.where(
                lane40 < 9, near_e, jnp.where(lane40 >= 119, near_w, 0.0)
            )

    fold_z_copies = [
        remote(fold_send.at[d], fold_got.at[zi], fz_send.at[d - 1], fz_recv.at[d - 1],
               lat, ((zi + d) % NZ) * NX + xi)
        for d in range(1, NZ)
    ]
    lane32 = lanes_of((32, COLS))
    near = lane32 <= pivot_lane

    @pl.when(top)
    def _():
        for copy in fold_x_copies:
            copy.wait_recv()
        for d in far_first(NZ) + [0]:
            want = pivot_block - ((zi + d) % NZ) * NX - xi

            def block(b):
                mine = (lax.shift_right_logical(b & (LON - 1), 2) == zi)
                return fold_row[jnp.where(mine, b & (NX - 1), NX)]

            ahead, here, behind, beyond = (block(want + o) for o in (1, 0, -1, -2))
            window = jnp.where(near, here, behind)
            edge = jnp.where(
                lane32 < 9, jnp.where(near, behind, beyond),
                jnp.where(lane32 >= 119, jnp.where(near, ahead, here), 0.0),
            )
            edges = sum(pltpu.roll(edge[8 * g : 8 * g + 8], 16 + 32 * g, 1) for g in range(4))
            if d:
                fold_send[d, 0:32, :] = window
                fold_send[d, 32:40, :] = edges
                fold_z_copies[d - 1].start()
            else:
                fold_got[zi, 0:32, :] = window
                fold_got[zi, 32:40, :] = edges

    next_level(1)

    def fields(spans):
        for r, n in spans:
            for raw, b in ((raw_m, b_m), (raw_h, b_h)):
                wet = (raw[0, r : r + n, :] > 0.0).astype(F32)
                b[0, r : r + n, :] = wet * raw[2, r : r + n, :]
                b[FIRST, r : r + n, :] = wet * raw[1, r : r + n, :]

    def roots(spans):
        for r, n in spans:
            sums = []
            for raw in (raw_m, raw_h):
                up, mid, low = (raw[0, r + o : r + o + n, :] for o in (1, 0, -1))
                both = up + low
                wets = [(v > 0.0).astype(F32) for v in (up, mid, low)]
                both_wet = wets[0] + wets[2]
                sums.append((mid, both, mid + 0.5 * both, wets[1], both_wet, wets[1] + 0.5 * both_wet))
            (dm, bm, cm, wm, bwm, cwm), (dh, bh, ch, wh, bwh, cwh) = sums
            e_m, e_h = from_east(cm, ch)
            w_m_, w_h_ = from_west(cm, ch)
            ew_m, ew_h = from_east(cwm, cwh)
            ww_m, ww_h = from_west(cwm, cwh)
            rooted = []
            for depth, wet, all_depth, all_wet in (
                (dm, wm, bm + (e_m + w_m_), bwm + (ew_m + ww_m)),
                (dh, wh, bh + (e_h + w_h_), bwh + (ew_h + ww_h)),
            ):
                links = 0.5 * (depth * all_wet + all_depth)
                diagonal = wet * (depth * (1.0 / (REACH * REACH)) + links) + (1.0 - wet)
                rooted.append(wet * lax.rsqrt(diagonal))
            s_m[r : r + n, :], s_h[r : r + n, :] = rooted
            se_m[r : r + n, :], se_h[r : r + n, :] = from_east(*rooted)
            de_m[r : r + n, :], de_h[r : r + n, :] = from_east(dm, dh)

    def links(spans):
        for r, n in spans:
            made = []
            for raw, s, de, se, w in ((raw_m, s_m, de_m, se_m, w_m), (raw_h, s_h, de_h, se_h, w_h)):
                d0, d1 = raw[0, r : r + n, :], raw[0, r + 1 : r + 1 + n, :]
                s0, s1 = s[r : r + n, :], s[r + 1 : r + 1 + n, :]
                de0, de1 = de[r : r + n, :], de[r + 1 : r + 1 + n, :]
                se0, se1 = se[r : r + n, :], se[r + 1 : r + 1 + n, :]
                east_w = -(d0 + de0) * (s0 * se0)
                ne_w = -0.5 * (d0 + de1) * (s0 * se1)
                nw_e = -0.5 * (de0 + d1) * (se0 * s1)
                w[0, r : r + n, :] = -(d0 + d1) * (s0 * s1)
                w[1, r : r + n, :] = east_w
                w[3, r : r + n, :] = ne_w
                w[6, r : r + n, :] = nw_e
                made.append((east_w, ne_w, nw_e))
            for slot, item in ((2, 0), (4, 1), (5, 2)):
                w_m[slot, r : r + n, :], w_h[slot, r : r + n, :] = from_west(made[0][item], made[1][item])

    def fold8(x):
        return sum(x[8 * k : 8 * k + 8] for k in range(x.shape[0] // 8))

    def step(n, both, first, spans, add):
        bases = (0, FIRST) if both else (0,)
        total = [jnp.zeros((8, COLS), F32) for _ in range(6)]
        for r, size, gram_rows in spans:
            weights = []
            for w in (w_m, w_h):
                weights.append((
                    w[0, r : r + size, :], w[0, r - 1 : r - 1 + size, :],
                    w[4, r : r + size, :], w[2, r : r + size, :], w[5, r - 1 : r - 1 + size, :],
                    w[6, r : r + size, :], w[1, r : r + size, :], w[3, r - 1 : r - 1 + size, :],
                ))
            news, olds = [], []
            for base in bases:
                zs = []
                for b, (a_u, a_d, e_u, e_c, e_d, f_u, f_c, f_d) in zip((b_m, b_h), weights):
                    k = base + n - 1
                    up = b[k, r + 1 : r + 1 + size, :]
                    mid = b[k, r : r + size, :]
                    low = b[k, r - 1 : r - 1 + size, :]
                    z0 = a_u * up + a_d * low
                    ze = e_u * up + e_c * mid + e_d * low
                    zw = f_u * up + f_c * mid + f_d * low
                    zs.append((mid, z0, ze, zw))
                (mid_m, z0_m, ze_m, zw_m), (mid_h, z0_h, ze_h, zw_h) = zs
                ze_m, ze_h = from_east(ze_m, ze_h)
                zw_m, zw_h = from_west(zw_m, zw_h)
                out_m, out_h = z0_m + (ze_m + zw_m), z0_h + (ze_h + zw_h)
                if first:
                    out_m, out_h = 0.5 * out_m, 0.5 * out_h
                else:
                    out_m = out_m - b_m[base + n - 2, r : r + size, :]
                    out_h = out_h - b_h[base + n - 2, r : r + size, :]
                b_m[base + n, r : r + size, :] = out_m
                b_h[base + n, r : r + size, :] = out_h
                news.append(out_m)
                olds.append(mid_m)
            lo, hi = max(r, gram_rows[0]) - r, min(r + size, gram_rows[1]) - r
            if hi > lo:
                p1, p0 = news[0][lo:hi], olds[0][lo:hi]
                total[0] = total[0] + fold8(p1 * p1)
                total[1] = total[1] + fold8(p1 * p0)
                if both:
                    r1, r0 = news[1][lo:hi], olds[1][lo:hi]
                    total[2] = total[2] + fold8(r1 * r1)
                    total[3] = total[3] + fold8(r1 * r0)
                    total[4] = total[4] + fold8(p1 * r1)
                else:
                    r0 = b_m[FIRST + STEPS - 1, r + lo : r + hi, :]
                total[5] = total[5] + fold8(p1 * r0)
        for c in range(6):
            row = jnp.sum(total[c], axis=0, keepdims=True)
            at = pl.ds(6 * n + c, 1)
            rows_acc[at, :] = rows_acc[at, :] + row if add else row

    def steps(spans, add):
        step(1, True, True, spans, add)

        @pl.loop(2, STEPS)
        def _(n):
            step(n, True, False, spans, add)

        step(STEPS, False, False, spans, add)

    fields(chunks(16, 176))
    roots([(17, 7)] + chunks(24, 168) + [(168, 7)])
    links(chunks(16, 168))
    next_level(2)
    start = [jnp.zeros((8, COLS), F32) for _ in range(3)]
    for r in range(16, 16 + ROWS, CHUNK):
        p0, r0 = b_m[0, r : r + CHUNK, :], b_m[FIRST, r : r + CHUNK, :]
        start = [t + fold8(v) for t, v in zip(start, (p0 * p0, r0 * r0, p0 * r0))]
    for c in range(3):
        rows_acc[2 * c : 2 * c + 1, :] = jnp.sum(start[c], axis=0, keepdims=True)

    steps([(r, n, (32, 160)) for r, n in chunks(16, 168)], False)
    next_level(3)

    @pl.when(jnp.logical_not(bottom))
    def _():
        to_se.wait_send()
        to_sw.wait_send()
        to_south.wait_send()
        to_ne.wait_recv()
        to_nw.wait_recv()
        to_north.wait_recv()
        for f in range(3):
            at = 96 + 9 * f
            near_e = pltpu.roll(corner[1], (COLS - at) % COLS, 1)
            near_w = pltpu.roll(corner[0], (119 - at) % COLS, 1)
            raw_h[f, 0:16, :] = jnp.where(lane16 < 9, near_e, jnp.where(lane16 >= 119, near_w, 0.0))

    @pl.when(bottom)
    def _():
        for f in range(3):
            raw_m[f, 0:16, :] = jnp.zeros((16, COLS), F32)
            raw_h[f, 0:16, :] = jnp.zeros((16, COLS), F32)

    @pl.when(jnp.logical_not(top))
    def _():
        to_ne.wait_send()
        to_nw.wait_send()
        to_north.wait_send()
        to_se.wait_recv()
        to_sw.wait_recv()
        to_south.wait_recv()
        for f in range(3):
            at = 9 * f
            near_e = pltpu.roll(corner[3], (COLS - at) % COLS, 1) if at else corner[3]
            near_w = pltpu.roll(corner[2], (119 - at) % COLS, 1)
            raw_h[f, 176:192, :] = jnp.where(lane16 < 9, near_e, jnp.where(lane16 >= 119, near_w, 0.0))

    @pl.when(top)
    def _():
        for copy in fold_z_copies:
            copy.wait_recv()
        ghost = fold_got[0]
        for k in range(1, NZ):
            ghost = ghost + fold_got[k]
        edges = ghost[32:40]
        lane8 = lanes_of((8, COLS))
        side = []
        for g in range(4):
            edge = pltpu.roll(edges, (COLS - 16 - 32 * g) % COLS, 1)
            side.append(jnp.where((lane8 < 9) | (lane8 >= 119), edge, 0.0))
        side = jnp.concatenate(side, axis=0)
        for ref, got in ((raw_m, ghost), (raw_h, side)):
            for f in range(3):
                ref[f, 176:192, :] = jnp.zeros((16, COLS), F32)
            ref[0, 176:185, :] = got[0:9]
            ref[1, 176:184, :] = got[9:17]
            ref[2, 176:184, :] = got[17:25]
        for copy in fold_x_copies + fold_z_copies:
            copy.wait_send()

    fields([(LO, 8), (176, 8)])
    roots([(LO, 16), (168, 16)])
    links([(LO, 16), (168, 16)])
    steps([(LO, 24, (16, 32)), (160, 24, (160, 176))], True)
    ones = jnp.ones((8, COLS), F32)
    sums = lax.dot_general(
        ones, rows_acc[...], (((1,), (1,)), ((), ())), precision=HIGHEST, preferred_element_type=F32
    )[0:1]

    def reduce(stage, value, slots, send, recv, count, mine, peer_of, order):
        slots[mine] = value
        part[stage] = value
        copies = [
            remote(part.at[stage], slots.at[mine], send.at[d - 1], recv.at[d - 1], *peer_of(d))
            for d in range(1, count)
        ]
        for d in order:
            copies[d - 1].start()
        for copy in copies:
            copy.wait_recv()
        terms = [slots[k] for k in range(count)]
        while len(terms) > 1:
            terms = [a + b for a, b in zip(terms[::2], terms[1::2])]
        return terms[0], copies

    sums, first_copies = reduce(
        0, sums, red_y, ry_send, ry_recv, LAT, lat,
        lambda d: ((lat + d) % LAT, lon), far_first(LAT))
    next_level(levels)
    sums, second_copies = reduce(
        1, sums, red_p, rp_send, rp_recv, LON, lon,
        lambda d: (lat, (lon + d) % LON), far_first(LON))
    moments_out[...] = sums
    for copy in first_copies + second_copies:
        copy.wait_send()


def held(shape):
    return pltpu.VMEM(shape, F32)


def basis_and_moments(forcing, search, depth, mask, fold_map):
    vm = pltpu.VMEM
    dma = pltpu.SemaphoreType.DMA
    ext = (EXT, COLS)
    return pl.pallas_call(
        basis_kernel,
        out_shape=(held((FIELDS,) + ext), held((1, COLS))),
        in_specs=[pl.BlockSpec(memory_space=pl.ANY)] * 5,
        out_specs=(pl.BlockSpec(memory_space=vm), pl.BlockSpec(memory_space=vm)),
        scratch_shapes=[
            pltpu.SMEM((1024,), jnp.int32),
            vm((3,) + ext, F32), vm((3,) + ext, F32),
            vm((ROWS, COLS), F32), vm((ROWS, COLS), jnp.int32),
            vm((40, COLS), F32), vm((40, COLS), F32), vm((40, COLS), F32), vm((40, COLS), F32),
            vm((4, 16, COLS), F32),
            vm((32, COLS), F32), vm((32, COLS), F32), vm((NX + 1, 32, COLS), F32),
            vm((NZ, 40, COLS), F32), vm((NZ, 40, COLS), F32),
        ]
        + [vm(ext, F32)] * 8
        + [vm((7,) + ext, F32)] * 2
        + [vm((FIELDS,) + ext, F32)]
        + [
            vm((COLS, COLS), F32), vm((2, 1, COLS), F32),
            vm((LON, 1, COLS), F32), vm((LAT, 1, COLS), F32),
            pltpu.SemaphoreType.REGULAR((4,)), dma((5,)), dma((8,)), dma((8,)),
            dma((NZ - 1,)), dma((NZ - 1,)), dma((NX - 1,)), dma((NX - 1,)),
            dma((LON - 1,)), dma((LON - 1,)), dma((LAT - 1,)), dma((LAT - 1,)),
        ],
        compiler_params=pltpu.CompilerParams(collective_id=0, has_side_effects=True),
        name="basis",
    )(fold_map, forcing, search, depth, mask)


def combine_kernel(moments_ref, basis_ref, height_ref, residual_ref):
    shape = (24, COLS)
    row = lax.broadcasted_iota(jnp.int32, shape, 0)
    col = lanes_of(shape)

    def power(i):
        return jnp.where(i >= FIRST, i - FIRST, i)

    kind = jnp.where((row >= FIRST) & (col >= FIRST), 1, jnp.where((row >= FIRST) | (col >= FIRST), 2, 0))
    valid = (row < FIELDS) & (col < FIELDS)
    ka, kb = power(row), power(col)
    high, low = ka + kb, jnp.abs(ka - kb)
    odd = high & 1

    def slot(k):
        return jnp.where(valid, 6 * ((k + 1) >> 1) + 2 * kind + odd, 0)

    base = jnp.where(odd == 1, 7 + 2 * kind, 2 * kind)
    raw = jnp.broadcast_to(moments_ref[...], shape)

    def take(index):
        return jnp.take_along_axis(raw, index, axis=1)

    gram = jnp.where(valid, take(slot(high)) + take(slot(low)) - take(jnp.where(valid, base, 0)), 0.0)

    def lower(i):
        return jnp.where((i == 1) | (i == FIRST + 1), 1.0, jnp.where((i >= 1) & (i < FIELDS) & (i != FIRST), 0.5, 0.0))

    def upper(i):
        return jnp.where((i < FIELDS - 2) & (i != FIRST - 2) & (i != FIRST - 1), 0.5, 0.0)

    low_l, up_l = lower(col).astype(F32), upper(col).astype(F32)
    low_s, up_s = lower(row).astype(F32), upper(row).astype(F32)

    def shifted(v, axis):
        length = v.shape[axis]
        low_c, up_c = (low_s, up_s) if axis == 0 else (low_l, up_l)
        return v + low_c * pltpu.roll(v, 1, axis) + up_c * pltpu.roll(v, length - 1, axis)

    below = pltpu.roll(low_l, COLS - 1, 1)
    above = pltpu.roll(up_l, 1, 1)
    ends = (col == FIRST - 1) | (col == FIELDS - 1)
    gram_h = jnp.where(
        ends, 0.0,
        gram + below * pltpu.roll(gram, COLS - 1, 1) + jnp.where(col > 0, above, 0.0) * pltpu.roll(gram, 1, 1),
    )

    def form(matrix, left, right):
        return jnp.sum(matrix * left * right, keepdims=True)

    unit = lambda at: ((row == at).astype(F32), (col == at).astype(F32))
    p_s, p_l = unit(0)
    r_s, r_l = unit(FIRST)
    q_s, q_l = shifted(p_s, 0), shifted(p_l, 1)
    x_s = jnp.zeros(shape, F32)
    norm = form(gram, r_s, r_l)
    curvature = form(gram_h, p_s, p_l)
    for inner in range(STEPS):
        t = norm / curvature
        x_s = x_s + t * p_s
        r_s = r_s - t * q_s
        if inner == STEPS - 1:
            break
        r_l = r_l - t * q_l
        h_s, h_l = shifted(r_s, 0), shifted(r_l, 1)
        fresh = form(gram, r_s, r_l)
        own = form(gram_h, r_s, r_l)
        cross = form(gram_h, r_s, p_l)
        beta = fresh / norm
        curvature = own + beta * (2.0 * cross + beta * curvature)
        norm = fresh
        p_s, p_l = r_s + beta * p_s, r_l + beta * p_l
        q_s, q_l = h_s + beta * q_s, h_l + beta * q_l

    size = 32
    for at in range(0, ROWS, size):
        height = jnp.zeros((size, COLS), F32)
        residual = jnp.zeros((size, COLS), F32)
        for k in range(FIELDS):
            field = basis_ref[k, 16 + at : 16 + at + size, :]
            height = height + x_s[k : k + 1, :] * field
            residual = residual + r_s[k : k + 1, :] * field
        height_ref[at : at + size, :] = height
        residual_ref[at : at + size, :] = residual


def per_device(forcing, search, depth, mask, fold_map):
    basis, moments = basis_and_moments(forcing, search, depth, mask, fold_map)
    basis, moments = (pltpu.with_memory_space_constraint(v, pltpu.VMEM) for v in (basis, moments))
    block = jax.ShapeDtypeStruct((ROWS, COLS), F32)
    return pl.pallas_call(
        combine_kernel,
        out_shape=(block, block),
        in_specs=[pl.BlockSpec(memory_space=pltpu.VMEM)] * 2,
        name="combine",
    )(moments, basis)


def solution(mesh):
    return jax.shard_map(
        per_device,
        mesh=mesh,
        in_specs=(P("lat", "lon"),) * 4 + (P(),),
        out_specs=(P("lat", "lon"),) * 2,
        check_vma=False,
    )
```

```python
import functools

import jax
import jax.numpy as jnp
from jax import lax
from jax.experimental import pallas as pl
from jax.experimental.pallas import tpu as pltpu
from jax.sharding import PartitionSpec as P

STEPS = 8
REACH = 256
LAT, LON, NX, NZ = 16, 32, 4, 8
ROWS, COLS = 160, 128
EXT = ROWS + 32
LO = 8
FIELDS = 2 * STEPS + 1
FIRST = STEPS + 1
HIGHEST = lax.Precision.HIGHEST
F32 = jnp.float32


def lanes_of(shape):
    return lax.broadcasted_iota(jnp.int32, shape, len(shape) - 1)


def from_east(main, side):
    lane = lanes_of(main.shape)
    a, b = pltpu.roll(main, COLS - 1, 1), pltpu.roll(side, COLS - 1, 1)
    last = lane == COLS - 1
    return jnp.where(last, b, a), jnp.where(last, a, b)


def from_west(main, side):
    lane = lanes_of(main.shape)
    a, b = pltpu.roll(main, 1, 1), pltpu.roll(side, 1, 1)
    head = lane == 0
    return jnp.where(head, b, a), jnp.where(head, a, b)


def remote(src, dst, send, recv, lat, lon):
    return pltpu.make_async_remote_copy(
        src_ref=src,
        dst_ref=dst,
        send_sem=send,
        recv_sem=recv,
        device_id={"lat": lat, "lon": lon},
        device_id_type=pl.DeviceIdType.MESH,
    )


CHUNK = 16


def far_first(count):
    return sorted(range(1, count), key=lambda d: (-min(d, count - d), d))


def chunks(start, stop):
    return [(r, min(CHUNK, stop - r)) for r in range(start, stop, CHUNK)]


def basis_kernel(
    fold_ref, forcing_ref, search_ref, depth_ref, mask_ref,
    b_m, moments_out,
    fold_buf, raw_m, raw_h, depth_buf, mask_buf, pack_w, pack_e, got_w, got_e, corner,
    fold_x, fold_src, fold_row, fold_send, fold_got,
    wet_m, wet_h, s_m, s_h, de_m, de_h, se_m, se_h,
    w_m, w_h, b_h, rows_acc, part, red_p, red_y,
    plane_sem, local_sem, halo_send, halo_recv, fz_send, fz_recv, fx_send, fx_recv,
    rp_send, rp_recv, ry_send, ry_recv,
):
    lat = lax.axis_index("lat")
    lon = lax.axis_index("lon")
    zi, xi = lon // NX, lon % NX
    top = lat == LAT - 1
    bottom = lat == 0
    north, south = (lat + 1) % LAT, (lat + LAT - 1) % LAT
    east, west = (lon + 1) % LON, (lon + LON - 1) % LON
    barrier = pltpu.get_barrier_semaphore()

    loads = [
        pltpu.make_async_copy(depth_ref, depth_buf, local_sem.at[0]),
        pltpu.make_async_copy(mask_ref, mask_buf, local_sem.at[1]),
        pltpu.make_async_copy(forcing_ref, raw_m.at[1, pl.ds(16, ROWS), :], local_sem.at[2]),
        pltpu.make_async_copy(search_ref, raw_m.at[2, pl.ds(16, ROWS), :], local_sem.at[3]),
        pltpu.make_async_copy(fold_ref.at[pl.ds(0, 1024)], fold_buf, local_sem.at[4]),
    ]
    for copy in loads:
        copy.start()
    def greet(semaphore, to):
        for a, b in to:
            pl.semaphore_signal(
                semaphore, inc=1, device_id={"lat": a, "lon": b}, device_id_type=pl.DeviceIdType.MESH
            )

    fold_peers = [(lat, ((zi + d) % NZ) * NX + xi) for d in far_first(NZ)]

    def around(far):
        if 2 * far == NZ:
            return [(lat, (lon + NX * far) % LON)]
        to = [(lat, (lon + NX * far) % LON), (lat, (lon + LON - NX * far) % LON)]
        if 2 * far < LAT:
            to += [((lat + 2 * far) % LAT, lon), ((lat + LAT - 2 * far) % LAT, lon)]
        return to

    beside = [(lat, zi * NX + (xi + d) % NX) for d in far_first(NX)]
    beside += [(north, east), (north, west), (south, east), (south, west)]
    beside += [(lat, east), (lat, west), (north, lon), (south, lon)] + around(1)

    @pl.when(top)
    def _():
        greet(barrier, fold_peers)

    greet(barrier, beside)

    levels = 3

    def next_level(level):
        if level > 0:
            pl.semaphore_wait(plane_sem.at[level - 1], len(around(1 << (level - 1))))
        if level < levels:
            greet(plane_sem.at[level], around(1 << level))

    rows_acc[...] = jnp.zeros_like(rows_acc)
    for copy in loads:
        copy.wait()
    raw_m[0, 16 : 16 + ROWS, :] = depth_buf[...] * mask_buf[...].astype(F32)

    lane40 = lanes_of((40, COLS))
    acc_w = jnp.zeros((40, COLS), F32)
    acc_e = jnp.zeros((40, COLS), F32)
    for g in range(4):
        for f in range(3):
            at = 32 * g + 9 * f
            block = raw_m[f, 16 + 40 * g : 56 + 40 * g, :]
            here = (lane40 >= at) & (lane40 < at + 9)
            acc_w = jnp.where(here, pltpu.roll(block, at, 1) if at else block, acc_w)
            acc_e = jnp.where(here, pltpu.roll(block, (at - 119) % COLS, 1), acc_e)
    pack_w[...] = acc_w
    pack_e[...] = acc_e

    pivot = fold_buf[0]
    pivot_block, pivot_lane = lax.shift_right_logical(pivot, 7), pivot & (COLS - 1)

    @pl.when(top)
    def _():
        fold_x[...] = jnp.zeros_like(fold_x)
        for m in range(9):
            fold_x[m : m + 1, :] = raw_m[0, 175 - m : 176 - m, :]
        for m in range(8):
            fold_x[9 + m : 10 + m, :] = raw_m[1, 175 - m : 176 - m, :]
            fold_x[17 + m : 18 + m, :] = raw_m[2, 175 - m : 176 - m, :]
        source = lax.broadcasted_iota(jnp.int32, (COLS, COLS), 0)
        target = lax.broadcasted_iota(jnp.int32, (COLS, COLS), 1)
        choose = (source == ((pivot - target) & (COLS - 1))).astype(F32)
        turned = jnp.dot(fold_x[...], choose, precision=HIGHEST, preferred_element_type=F32)
        fold_src[...] = turned
        fold_row[xi] = turned
        fold_row[NX] = jnp.zeros_like(turned)

    pl.semaphore_wait(barrier, len(beside) + jnp.where(top, len(fold_peers), 0))

    fold_x_copies = [
        remote(fold_src, fold_row.at[xi], fx_send.at[d - 1], fx_recv.at[d - 1], lat, zi * NX + (xi + d) % NX)
        for d in range(1, NX)
    ]

    @pl.when(top)
    def _():
        for d in far_first(NX):
            fold_x_copies[d - 1].start()

    to_north = remote(raw_m.at[:, pl.ds(160, 16), :], raw_m.at[:, pl.ds(0, 16), :],
                      halo_send.at[0], halo_recv.at[0], north, lon)
    to_south = remote(raw_m.at[:, pl.ds(16, 16), :], raw_m.at[:, pl.ds(176, 16), :],
                      halo_send.at[1], halo_recv.at[1], south, lon)
    to_east = remote(pack_e, got_w, halo_send.at[2], halo_recv.at[2], lat, east)
    to_west = remote(pack_w, got_e, halo_send.at[3], halo_recv.at[3], lat, west)
    to_ne = remote(pack_e.at[pl.ds(24, 16), :], corner.at[0], halo_send.at[4], halo_recv.at[4], north, east)
    to_nw = remote(pack_w.at[pl.ds(24, 16), :], corner.at[1], halo_send.at[5], halo_recv.at[5], north, west)
    to_se = remote(pack_e.at[pl.ds(0, 16), :], corner.at[2], halo_send.at[6], halo_recv.at[6], south, east)
    to_sw = remote(pack_w.at[pl.ds(0, 16), :], corner.at[3], halo_send.at[7], halo_recv.at[7], south, west)

    to_east.start()
    to_west.start()
    next_level(0)

    @pl.when(jnp.logical_not(top))
    def _():
        to_ne.start()
        to_nw.start()
        to_north.start()

    @pl.when(jnp.logical_not(bottom))
    def _():
        to_se.start()
        to_sw.start()
        to_south.start()

    to_east.wait()
    to_west.wait()

    lane16 = lanes_of((16, COLS))
    for g in range(4):
        for f in range(3):
            at = 32 * g + 9 * f
            near_e = pltpu.roll(got_e[...], (COLS - at) % COLS, 1) if at else got_e[...]
            near_w = pltpu.roll(got_w[...], (119 - at) % COLS, 1)
            raw_h[f, 16 + 40 * g : 56 + 40 * g, :] = jnp.where(
                lane40 < 9, near_e, jnp.where(lane40 >= 119, near_w, 0.0)
            )

    fold_z_copies = [
        remote(fold_send.at[d], fold_got.at[zi], fz_send.at[d - 1], fz_recv.at[d - 1],
               lat, ((zi + d) % NZ) * NX + xi)
        for d in range(1, NZ)
    ]
    lane32 = lanes_of((32, COLS))
    near = lane32 <= pivot_lane

    @pl.when(top)
    def _():
        for copy in fold_x_copies:
            copy.wait_recv()
        for d in far_first(NZ) + [0]:
            want = pivot_block - ((zi + d) % NZ) * NX - xi

            def block(b):
                mine = (lax.shift_right_logical(b & (LON - 1), 2) == zi)
                return fold_row[jnp.where(mine, b & (NX - 1), NX)]

            ahead, here, behind, beyond = (block(want + o) for o in (1, 0, -1, -2))
            window = jnp.where(near, here, behind)
            edge = jnp.where(
                lane32 < 9, jnp.where(near, behind, beyond),
                jnp.where(lane32 >= 119, jnp.where(near, ahead, here), 0.0),
            )
            edges = sum(pltpu.roll(edge[8 * g : 8 * g + 8], 16 + 32 * g, 1) for g in range(4))
            if d:
                fold_send[d, 0:32, :] = window
                fold_send[d, 32:40, :] = edges
                fold_z_copies[d - 1].start()
            else:
                fold_got[zi, 0:32, :] = window
                fold_got[zi, 32:40, :] = edges

    next_level(1)

    def fields(spans):
        for r, n in spans:
            for raw, b in ((raw_m, b_m), (raw_h, b_h)):
                wet = (raw[0, r : r + n, :] > 0.0).astype(F32)
                b[0, r : r + n, :] = wet * raw[2, r : r + n, :]
                b[FIRST, r : r + n, :] = wet * raw[1, r : r + n, :]

    def roots(spans):
        for r, n in spans:
            sums = []
            for raw in (raw_m, raw_h):
                up, mid, low = (raw[0, r + o : r + o + n, :] for o in (1, 0, -1))
                both = up + low
                wets = [(v > 0.0).astype(F32) for v in (up, mid, low)]
                both_wet = wets[0] + wets[2]
                sums.append((mid, both, mid + 0.5 * both, wets[1], both_wet, wets[1] + 0.5 * both_wet))
            (dm, bm, cm, wm, bwm, cwm), (dh, bh, ch, wh, bwh, cwh) = sums
            e_m, e_h = from_east(cm, ch)
            w_m_, w_h_ = from_west(cm, ch)
            ew_m, ew_h = from_east(cwm, cwh)
            ww_m, ww_h = from_west(cwm, cwh)
            rooted = []
            for depth, wet, all_depth, all_wet in (
                (dm, wm, bm + (e_m + w_m_), bwm + (ew_m + ww_m)),
                (dh, wh, bh + (e_h + w_h_), bwh + (ew_h + ww_h)),
            ):
                links = 0.5 * (depth * all_wet + all_depth)
                diagonal = wet * (depth * (1.0 / (REACH * REACH)) + links) + (1.0 - wet)
                rooted.append(wet * lax.rsqrt(diagonal))
            s_m[r : r + n, :], s_h[r : r + n, :] = rooted
            se_m[r : r + n, :], se_h[r : r + n, :] = from_east(*rooted)
            de_m[r : r + n, :], de_h[r : r + n, :] = from_east(dm, dh)

    def links(spans):
        for r, n in spans:
            made = []
            for raw, s, de, se, w in ((raw_m, s_m, de_m, se_m, w_m), (raw_h, s_h, de_h, se_h, w_h)):
                d0, d1 = raw[0, r : r + n, :], raw[0, r + 1 : r + 1 + n, :]
                s0, s1 = s[r : r + n, :], s[r + 1 : r + 1 + n, :]
                de0, de1 = de[r : r + n, :], de[r + 1 : r + 1 + n, :]
                se0, se1 = se[r : r + n, :], se[r + 1 : r + 1 + n, :]
                east_w = -(d0 + de0) * (s0 * se0)
                ne_w = -0.5 * (d0 + de1) * (s0 * se1)
                nw_e = -0.5 * (de0 + d1) * (se0 * s1)
                w[0, r : r + n, :] = -(d0 + d1) * (s0 * s1)
                w[1, r : r + n, :] = east_w
                w[3, r : r + n, :] = ne_w
                w[6, r : r + n, :] = nw_e
                made.append((east_w, ne_w, nw_e))
            for slot, item in ((2, 0), (4, 1), (5, 2)):
                w_m[slot, r : r + n, :], w_h[slot, r : r + n, :] = from_west(made[0][item], made[1][item])

    def fold8(x):
        return sum(x[8 * k : 8 * k + 8] for k in range(x.shape[0] // 8))

    def step(n, both, first, spans, add):
        bases = (0, FIRST) if both else (0,)
        total = [jnp.zeros((8, COLS), F32) for _ in range(6)]
        for r, size, gram_rows in spans:
            weights = []
            for w in (w_m, w_h):
                weights.append((
                    w[0, r : r + size, :], w[0, r - 1 : r - 1 + size, :],
                    w[4, r : r + size, :], w[2, r : r + size, :], w[5, r - 1 : r - 1 + size, :],
                    w[6, r : r + size, :], w[1, r : r + size, :], w[3, r - 1 : r - 1 + size, :],
                ))
            news, olds = [], []
            for base in bases:
                zs = []
                for b, (a_u, a_d, e_u, e_c, e_d, f_u, f_c, f_d) in zip((b_m, b_h), weights):
                    k = base + n - 1
                    up = b[k, r + 1 : r + 1 + size, :]
                    mid = b[k, r : r + size, :]
                    low = b[k, r - 1 : r - 1 + size, :]
                    z0 = a_u * up + a_d * low
                    ze = e_u * up + e_c * mid + e_d * low
                    zw = f_u * up + f_c * mid + f_d * low
                    zs.append((mid, z0, ze, zw))
                (mid_m, z0_m, ze_m, zw_m), (mid_h, z0_h, ze_h, zw_h) = zs
                ze_m, ze_h = from_east(ze_m, ze_h)
                zw_m, zw_h = from_west(zw_m, zw_h)
                out_m, out_h = z0_m + (ze_m + zw_m), z0_h + (ze_h + zw_h)
                if first:
                    out_m, out_h = 0.5 * out_m, 0.5 * out_h
                else:
                    out_m = out_m - b_m[base + n - 2, r : r + size, :]
                    out_h = out_h - b_h[base + n - 2, r : r + size, :]
                b_m[base + n, r : r + size, :] = out_m
                b_h[base + n, r : r + size, :] = out_h
                news.append(out_m)
                olds.append(mid_m)
            lo, hi = max(r, gram_rows[0]) - r, min(r + size, gram_rows[1]) - r
            if hi > lo:
                p1, p0 = news[0][lo:hi], olds[0][lo:hi]
                total[0] = total[0] + fold8(p1 * p1)
                total[1] = total[1] + fold8(p1 * p0)
                if both:
                    r1, r0 = news[1][lo:hi], olds[1][lo:hi]
                    total[2] = total[2] + fold8(r1 * r1)
                    total[3] = total[3] + fold8(r1 * r0)
                    total[4] = total[4] + fold8(p1 * r1)
                else:
                    r0 = b_m[FIRST + STEPS - 1, r + lo : r + hi, :]
                total[5] = total[5] + fold8(p1 * r0)
        for c in range(6):
            row = jnp.sum(total[c], axis=0, keepdims=True)
            at = pl.ds(6 * n + c, 1)
            rows_acc[at, :] = rows_acc[at, :] + row if add else row

    def steps(spans, add):
        step(1, True, True, spans, add)

        @pl.loop(2, STEPS)
        def _(n):
            step(n, True, False, spans, add)

        step(STEPS, False, False, spans, add)

    fields(chunks(16, 176))
    roots([(17, 7)] + chunks(24, 168) + [(168, 7)])
    links(chunks(16, 168))
    start = [jnp.zeros((8, COLS), F32) for _ in range(3)]
    for r in range(16, 16 + ROWS, CHUNK):
        p0, r0 = b_m[0, r : r + CHUNK, :], b_m[FIRST, r : r + CHUNK, :]
        start = [t + fold8(v) for t, v in zip(start, (p0 * p0, r0 * r0, p0 * r0))]
    for c in range(3):
        rows_acc[2 * c : 2 * c + 1, :] = jnp.sum(start[c], axis=0, keepdims=True)

    steps([(r, n, (32, 160)) for r, n in chunks(16, 168)], False)
    next_level(2)

    @pl.when(jnp.logical_not(bottom))
    def _():
        to_se.wait_send()
        to_sw.wait_send()
        to_south.wait_send()
        to_ne.wait_recv()
        to_nw.wait_recv()
        to_north.wait_recv()
        for f in range(3):
            at = 96 + 9 * f
            near_e = pltpu.roll(corner[1], (COLS - at) % COLS, 1)
            near_w = pltpu.roll(corner[0], (119 - at) % COLS, 1)
            raw_h[f, 0:16, :] = jnp.where(lane16 < 9, near_e, jnp.where(lane16 >= 119, near_w, 0.0))

    @pl.when(bottom)
    def _():
        for f in range(3):
            raw_m[f, 0:16, :] = jnp.zeros((16, COLS), F32)
            raw_h[f, 0:16, :] = jnp.zeros((16, COLS), F32)

    @pl.when(jnp.logical_not(top))
    def _():
        to_ne.wait_send()
        to_nw.wait_send()
        to_north.wait_send()
        to_se.wait_recv()
        to_sw.wait_recv()
        to_south.wait_recv()
        for f in range(3):
            at = 9 * f
            near_e = pltpu.roll(corner[3], (COLS - at) % COLS, 1) if at else corner[3]
            near_w = pltpu.roll(corner[2], (119 - at) % COLS, 1)
            raw_h[f, 176:192, :] = jnp.where(lane16 < 9, near_e, jnp.where(lane16 >= 119, near_w, 0.0))

    @pl.when(top)
    def _():
        for copy in fold_z_copies:
            copy.wait_recv()
        ghost = fold_got[0]
        for k in range(1, NZ):
            ghost = ghost + fold_got[k]
        edges = ghost[32:40]
        lane8 = lanes_of((8, COLS))
        side = []
        for g in range(4):
            edge = pltpu.roll(edges, (COLS - 16 - 32 * g) % COLS, 1)
            side.append(jnp.where((lane8 < 9) | (lane8 >= 119), edge, 0.0))
        side = jnp.concatenate(side, axis=0)
        for ref, got in ((raw_m, ghost), (raw_h, side)):
            for f in range(3):
                ref[f, 176:192, :] = jnp.zeros((16, COLS), F32)
            ref[0, 176:185, :] = got[0:9]
            ref[1, 176:184, :] = got[9:17]
            ref[2, 176:184, :] = got[17:25]
        for copy in fold_x_copies + fold_z_copies:
            copy.wait_send()

    fields([(LO, 8), (176, 8)])
    roots([(LO, 16), (168, 16)])
    links([(LO, 16), (168, 16)])
    steps([(LO, 24, (16, 32)), (160, 24, (160, 176))], True)
    ones = jnp.ones((8, COLS), F32)
    sums = lax.dot_general(
        ones, rows_acc[...], (((1,), (1,)), ((), ())), precision=HIGHEST, preferred_element_type=F32
    )[0:1]

    def reduce(stage, value, slots, send, recv, count, mine, peer_of, order):
        slots[mine] = value
        part[stage] = value
        copies = [
            remote(part.at[stage], slots.at[mine], send.at[d - 1], recv.at[d - 1], *peer_of(d))
            for d in range(1, count)
        ]
        for d in order:
            copies[d - 1].start()
        for copy in copies:
            copy.wait_recv()
        terms = [slots[k] for k in range(count)]
        while len(terms) > 1:
            terms = [a + b for a, b in zip(terms[::2], terms[1::2])]
        return terms[0], copies

    sums, first_copies = reduce(
        0, sums, red_y, ry_send, ry_recv, LAT, lat,
        lambda d: ((lat + d) % LAT, lon), far_first(LAT))
    next_level(levels)
    sums, second_copies = reduce(
        1, sums, red_p, rp_send, rp_recv, LON, lon,
        lambda d: (lat, (lon + d) % LON), far_first(LON))
    moments_out[...] = sums
    for copy in first_copies + second_copies:
        copy.wait_send()


def held(shape):
    return pltpu.VMEM(shape, F32)


def basis_and_moments(forcing, search, depth, mask, fold_map):
    vm = pltpu.VMEM
    dma = pltpu.SemaphoreType.DMA
    ext = (EXT, COLS)
    return pl.pallas_call(
        basis_kernel,
        out_shape=(held((FIELDS,) + ext), held((1, COLS))),
        in_specs=[pl.BlockSpec(memory_space=pl.ANY)] * 5,
        out_specs=(pl.BlockSpec(memory_space=vm), pl.BlockSpec(memory_space=vm)),
        scratch_shapes=[
            pltpu.SMEM((1024,), jnp.int32),
            vm((3,) + ext, F32), vm((3,) + ext, F32),
            vm((ROWS, COLS), F32), vm((ROWS, COLS), jnp.int32),
            vm((40, COLS), F32), vm((40, COLS), F32), vm((40, COLS), F32), vm((40, COLS), F32),
            vm((4, 16, COLS), F32),
            vm((32, COLS), F32), vm((32, COLS), F32), vm((NX + 1, 32, COLS), F32),
            vm((NZ, 40, COLS), F32), vm((NZ, 40, COLS), F32),
        ]
        + [vm(ext, F32)] * 8
        + [vm((7,) + ext, F32)] * 2
        + [vm((FIELDS,) + ext, F32)]
        + [
            vm((COLS, COLS), F32), vm((2, 1, COLS), F32),
            vm((LON, 1, COLS), F32), vm((LAT, 1, COLS), F32),
            pltpu.SemaphoreType.REGULAR((4,)), dma((5,)), dma((8,)), dma((8,)),
            dma((NZ - 1,)), dma((NZ - 1,)), dma((NX - 1,)), dma((NX - 1,)),
            dma((LON - 1,)), dma((LON - 1,)), dma((LAT - 1,)), dma((LAT - 1,)),
        ],
        compiler_params=pltpu.CompilerParams(collective_id=0, has_side_effects=True),
        name="basis",
    )(fold_map, forcing, search, depth, mask)


def combine_kernel(moments_ref, basis_ref, height_ref, residual_ref):
    shape = (24, COLS)
    row = lax.broadcasted_iota(jnp.int32, shape, 0)
    col = lanes_of(shape)

    def power(i):
        return jnp.where(i >= FIRST, i - FIRST, i)

    kind = jnp.where((row >= FIRST) & (col >= FIRST), 1, jnp.where((row >= FIRST) | (col >= FIRST), 2, 0))
    valid = (row < FIELDS) & (col < FIELDS)
    ka, kb = power(row), power(col)
    high, low = ka + kb, jnp.abs(ka - kb)
    odd = high & 1

    def slot(k):
        return jnp.where(valid, 6 * ((k + 1) >> 1) + 2 * kind + odd, 0)

    base = jnp.where(odd == 1, 7 + 2 * kind, 2 * kind)
    raw = jnp.broadcast_to(moments_ref[...], shape)

    def take(index):
        return jnp.take_along_axis(raw, index, axis=1)

    gram = jnp.where(valid, take(slot(high)) + take(slot(low)) - take(jnp.where(valid, base, 0)), 0.0)

    def lower(i):
        return jnp.where((i == 1) | (i == FIRST + 1), 1.0, jnp.where((i >= 1) & (i < FIELDS) & (i != FIRST), 0.5, 0.0))

    def upper(i):
        return jnp.where((i < FIELDS - 2) & (i != FIRST - 2) & (i != FIRST - 1), 0.5, 0.0)

    low_l, up_l = lower(col).astype(F32), upper(col).astype(F32)
    low_s, up_s = lower(row).astype(F32), upper(row).astype(F32)

    def shifted(v, axis):
        length = v.shape[axis]
        low_c, up_c = (low_s, up_s) if axis == 0 else (low_l, up_l)
        return v + low_c * pltpu.roll(v, 1, axis) + up_c * pltpu.roll(v, length - 1, axis)

    below = pltpu.roll(low_l, COLS - 1, 1)
    above = pltpu.roll(up_l, 1, 1)
    ends = (col == FIRST - 1) | (col == FIELDS - 1)
    gram_h = jnp.where(
        ends, 0.0,
        gram + below * pltpu.roll(gram, COLS - 1, 1) + jnp.where(col > 0, above, 0.0) * pltpu.roll(gram, 1, 1),
    )

    def form(matrix, left, right):
        return jnp.sum(matrix * left * right, keepdims=True)

    unit = lambda at: ((row == at).astype(F32), (col == at).astype(F32))
    p_s, p_l = unit(0)
    r_s, r_l = unit(FIRST)
    q_s, q_l = shifted(p_s, 0), shifted(p_l, 1)
    x_s = jnp.zeros(shape, F32)
    norm = form(gram, r_s, r_l)
    curvature = form(gram_h, p_s, p_l)
    for inner in range(STEPS):
        t = norm / curvature
        x_s = x_s + t * p_s
        r_s = r_s - t * q_s
        if inner == STEPS - 1:
            break
        r_l = r_l - t * q_l
        h_s, h_l = shifted(r_s, 0), shifted(r_l, 1)
        fresh = form(gram, r_s, r_l)
        own = form(gram_h, r_s, r_l)
        cross = form(gram_h, r_s, p_l)
        beta = fresh / norm
        curvature = own + beta * (2.0 * cross + beta * curvature)
        norm = fresh
        p_s, p_l = r_s + beta * p_s, r_l + beta * p_l
        q_s, q_l = h_s + beta * q_s, h_l + beta * q_l

    size = 32
    for at in range(0, ROWS, size):
        height = jnp.zeros((size, COLS), F32)
        residual = jnp.zeros((size, COLS), F32)
        for k in range(FIELDS):
            field = basis_ref[k, 16 + at : 16 + at + size, :]
            height = height + x_s[k : k + 1, :] * field
            residual = residual + r_s[k : k + 1, :] * field
        height_ref[at : at + size, :] = height
        residual_ref[at : at + size, :] = residual


def per_device(forcing, search, depth, mask, fold_map):
    basis, moments = basis_and_moments(forcing, search, depth, mask, fold_map)
    basis, moments = (pltpu.with_memory_space_constraint(v, pltpu.VMEM) for v in (basis, moments))
    block = jax.ShapeDtypeStruct((ROWS, COLS), F32)
    return pl.pallas_call(
        combine_kernel,
        out_shape=(block, block),
        in_specs=[pl.BlockSpec(memory_space=pltpu.VMEM)] * 2,
        name="combine",
    )(moments, basis)


def solution(mesh):
    return jax.shard_map(
        per_device,
        mesh=mesh,
        in_specs=(P("lat", "lon"),) * 4 + (P(),),
        out_specs=(P("lat", "lon"),) * 2,
        check_vma=False,
    )
```

```python
import functools

import jax
import jax.numpy as jnp
from jax import lax
from jax.experimental import pallas as pl
from jax.experimental.pallas import tpu as pltpu
from jax.sharding import PartitionSpec as P

STEPS = 8
REACH = 256
LAT, LON, NX, NZ = 16, 32, 4, 8
ROWS, COLS = 160, 128
EXT = ROWS + 32
LO = 8
FIELDS = 2 * STEPS + 1
FIRST = STEPS + 1
HIGHEST = lax.Precision.HIGHEST
F32 = jnp.float32


def lanes_of(shape):
    return lax.broadcasted_iota(jnp.int32, shape, len(shape) - 1)


def from_east(x):
    return pltpu.roll(x, COLS - 1, 1)


def from_west(x):
    return pltpu.roll(x, 1, 1)


def shift(x, by):
    by %= COLS
    return pltpu.roll(x, by, 1) if by else x


WEST = 28


def strip_lanes(lane, half):
    lane = (lane - half) & (COLS - 1)
    return (lane >= 119) | ((lane >= WEST) & (lane < WEST + 9))


def within(lane, start, stop):
    return (lane >= start) & (lane < stop)


def remote(src, dst, send, recv, lat, lon):
    return pltpu.make_async_remote_copy(
        src_ref=src,
        dst_ref=dst,
        send_sem=send,
        recv_sem=recv,
        device_id={"lat": lat, "lon": lon},
        device_id_type=pl.DeviceIdType.MESH,
    )


CHUNK = 16


def far_first(count):
    return sorted(range(1, count), key=lambda d: (-min(d, count - d), d))


def chunks(start, stop):
    return [(r, min(CHUNK, stop - r)) for r in range(start, stop, CHUNK)]


def basis_kernel(
    fold_ref, forcing_ref, search_ref, depth_ref, mask_ref,
    b_m, b_s, moments_out,
    fold_buf, raw_m, side_depth, side_state, depth_buf, mask_buf, pack_w, pack_e, got_w, got_e, corner,
    fold_x, fold_src, fold_row, fold_send, fold_got,
    s_m, s_s, de_m, de_s, se_m, se_s,
    w_m, w_s, rows_acc, part, red_p, red_y,
    plane_sem, local_sem, halo_send, halo_recv, fz_send, fz_recv, fx_send, fx_recv,
    rp_send, rp_recv, ry_send, ry_recv,
):
    lat = lax.axis_index("lat")
    lon = lax.axis_index("lon")
    zi, xi = lon // NX, lon % NX
    top = lat == LAT - 1
    bottom = lat == 0
    north, south = (lat + 1) % LAT, (lat + LAT - 1) % LAT
    east, west = (lon + 1) % LON, (lon + LON - 1) % LON
    barrier = pltpu.get_barrier_semaphore()

    loads = [
        pltpu.make_async_copy(depth_ref, depth_buf, local_sem.at[0]),
        pltpu.make_async_copy(mask_ref, mask_buf, local_sem.at[1]),
        pltpu.make_async_copy(forcing_ref, raw_m.at[1, pl.ds(16, ROWS), :], local_sem.at[2]),
        pltpu.make_async_copy(search_ref, raw_m.at[2, pl.ds(16, ROWS), :], local_sem.at[3]),
        pltpu.make_async_copy(fold_ref.at[pl.ds(0, 1024)], fold_buf, local_sem.at[4]),
    ]
    for copy in loads:
        copy.start()

    def greet(semaphore, to):
        for a, b in to:
            pl.semaphore_signal(
                semaphore, inc=1, device_id={"lat": a, "lon": b}, device_id_type=pl.DeviceIdType.MESH
            )

    def around(far):
        if 2 * far == NZ:
            return [(lat, (lon + NX * far) % LON)]
        to = [(lat, (lon + NX * far) % LON), (lat, (lon + LON - NX * far) % LON)]
        if 2 * far < LAT:
            to += [((lat + 2 * far) % LAT, lon), ((lat + LAT - 2 * far) % LAT, lon)]
        return to

    beside = [(lat, zi * NX + (xi + d) % NX) for d in far_first(NX)]
    beside += [(north, east), (north, west), (south, east), (south, west)]
    beside += [(lat, east), (lat, west), (north, lon), (south, lon)] + around(1)

    greet(barrier, beside)

    levels = 3

    def next_level(level):
        if level > 0:
            pl.semaphore_wait(plane_sem.at[level - 1], len(around(1 << (level - 1))))
        if level < levels:
            greet(plane_sem.at[level], around(1 << level))

    rows_acc[...] = jnp.zeros_like(rows_acc)
    for copy in loads:
        copy.wait()
    raw_m[0, 16 : 16 + ROWS, :] = depth_buf[...] * mask_buf[...].astype(F32)

    lane40 = lanes_of((40, COLS))
    acc_w = jnp.zeros((40, COLS), F32)
    acc_e = jnp.zeros((40, COLS), F32)
    for g in range(4):
        for f in range(3):
            at = 32 * g + 9 * f
            block = raw_m[f, 16 + 40 * g : 56 + 40 * g, :]
            here = (lane40 >= at) & (lane40 < at + 9)
            acc_w = jnp.where(here, pltpu.roll(block, at, 1) if at else block, acc_w)
            acc_e = jnp.where(here, pltpu.roll(block, (at - 119) % COLS, 1), acc_e)
    pack_w[...] = acc_w
    pack_e[...] = acc_e

    pivot = fold_buf[0]
    pivot_block, pivot_lane = lax.shift_right_logical(pivot, 7), pivot & (COLS - 1)

    @pl.when(top)
    def _():
        fold_x[...] = jnp.zeros_like(fold_x)
        for m in range(9):
            fold_x[m : m + 1, :] = raw_m[0, 175 - m : 176 - m, :]
        for m in range(8):
            fold_x[9 + m : 10 + m, :] = raw_m[1, 175 - m : 176 - m, :]
            fold_x[17 + m : 18 + m, :] = raw_m[2, 175 - m : 176 - m, :]
        source = lax.broadcasted_iota(jnp.int32, (COLS, COLS), 0)
        target = lax.broadcasted_iota(jnp.int32, (COLS, COLS), 1)
        choose = (source == ((pivot - target) & (COLS - 1))).astype(F32)
        turned = jnp.dot(fold_x[...], choose, precision=HIGHEST, preferred_element_type=F32)
        fold_src[...] = turned
        fold_row[xi] = turned
        fold_row[NX] = jnp.zeros_like(turned)

    pl.semaphore_wait(barrier, len(beside))

    fold_x_copies = [
        remote(fold_src, fold_row.at[xi], fx_send.at[d - 1], fx_recv.at[d - 1], lat, zi * NX + (xi + d) % NX)
        for d in range(1, NX)
    ]

    @pl.when(top)
    def _():
        for d in far_first(NX):
            fold_x_copies[d - 1].start()

    to_north = remote(raw_m.at[:, pl.ds(160, 16), :], raw_m.at[:, pl.ds(0, 16), :],
                      halo_send.at[0], halo_recv.at[0], north, lon)
    to_south = remote(raw_m.at[:, pl.ds(16, 16), :], raw_m.at[:, pl.ds(176, 16), :],
                      halo_send.at[1], halo_recv.at[1], south, lon)
    to_east = remote(pack_e, got_w, halo_send.at[2], halo_recv.at[2], lat, east)
    to_west = remote(pack_w, got_e, halo_send.at[3], halo_recv.at[3], lat, west)
    to_ne = remote(pack_e.at[pl.ds(24, 16), :], corner.at[0], halo_send.at[4], halo_recv.at[4], north, east)
    to_nw = remote(pack_w.at[pl.ds(24, 16), :], corner.at[1], halo_send.at[5], halo_recv.at[5], north, west)
    to_se = remote(pack_e.at[pl.ds(0, 16), :], corner.at[2], halo_send.at[6], halo_recv.at[6], south, east)
    to_sw = remote(pack_w.at[pl.ds(0, 16), :], corner.at[3], halo_send.at[7], halo_recv.at[7], south, west)

    to_east.start()
    to_west.start()
    next_level(0)

    @pl.when(jnp.logical_not(top))
    def _():
        to_ne.start()
        to_nw.start()
        to_north.start()

    @pl.when(jnp.logical_not(bottom))
    def _():
        to_se.start()
        to_sw.start()
        to_south.start()

    fold_z_copies = [
        remote(fold_send.at[d], fold_got.at[zi], fz_send.at[d - 1], fz_recv.at[d - 1],
               lat, ((zi + d) % NZ) * NX + xi)
        for d in range(1, NZ)
    ]
    lane32 = lanes_of((32, COLS))
    near = lane32 <= pivot_lane

    @pl.when(top)
    def _():
        next_level(1)
        next_level(2)
        for copy in fold_x_copies:
            copy.wait_recv()
        for d in far_first(NZ) + [0]:
            want = pivot_block - ((zi + d) % NZ) * NX - xi

            def block(b):
                mine = (lax.shift_right_logical(b & (LON - 1), 2) == zi)
                return fold_row[jnp.where(mine, b & (NX - 1), NX)]

            ahead, here, behind, beyond = (block(want + o) for o in (1, 0, -1, -2))
            window = jnp.where(near, here, behind)
            edge = jnp.where(
                lane32 < 9, jnp.where(near, behind, beyond),
                jnp.where(lane32 >= 119, jnp.where(near, ahead, here), 0.0),
            )
            edges = sum(pltpu.roll(edge[8 * g : 8 * g + 8], 16 + 32 * g, 1) for g in range(4))
            if d:
                fold_send[d, 0:32, :] = window
                fold_send[d, 32:40, :] = edges
                fold_z_copies[d - 1].start()
            else:
                fold_got[zi, 0:32, :] = window
                fold_got[zi, 32:40, :] = edges

    def own_strips(spans):
        for r, n in spans:
            depth, residual, search = (raw_m[f, r : r + n, :] for f in range(3))
            lane = lanes_of((n, COLS))
            west_p, east_r, west_r = (within(lane, a, a + 18) for a in (WEST, 46, WEST + 64))
            east_p = lane >= 110
            for ref, p, q in ((side_depth, depth, depth), (side_state, search, residual)):
                ref[r : r + n, :] = jnp.where(
                    east_p, p, jnp.where(west_p, shift(p, WEST), jnp.where(
                        east_r, shift(q, 64), jnp.where(west_r, shift(q, WEST + 64), 0.0))))

    def far_strips(r, n, from_e, from_w, places):
        lane = lanes_of((n, COLS))
        west_p, east_r, west_r = (within(lane, a, a + 9) for a in (WEST - 9, 64, WEST + 55))
        east_p = lane < 9
        at_d, at_r, at_p = places
        for ref, p, q in ((side_depth, at_d, at_d), (side_state, at_p, at_r)):
            ref[r : r + n, :] = jnp.where(
                east_p, shift(from_e, -p), jnp.where(west_p, shift(from_w, WEST - 9 - p), jnp.where(
                    east_r, shift(from_e, 64 - q), jnp.where(
                        west_r, shift(from_w, WEST + 55 - q), ref[r : r + n, :]))))

    kinds = {
        "m": (raw_m.at[0], s_m, de_m, se_m, w_m),
        "s": (side_depth, s_s, de_s, se_s, w_s),
    }

    def fields(kind, spans):
        for r, n in spans:
            wet = (kinds[kind][0][r : r + n, :] > 0.0).astype(F32)
            if kind == "m":
                b_m[0, r : r + n, :] = wet * raw_m[2, r : r + n, :]
                b_m[FIRST, r : r + n, :] = wet * raw_m[1, r : r + n, :]
            else:
                b_s[0, r : r + n, :] = wet * side_state[r : r + n, :]

    def roots(kind, spans):
        depth_ref_, s, de, se, _ = kinds[kind]
        for r, n in spans:
            up, depth, low = (depth_ref_[r + o : r + o + n, :] for o in (1, 0, -1))
            both = up + low
            column = depth + 0.5 * both
            wet_up, wet, wet_low = ((v > 0.0).astype(F32) for v in (up, depth, low))
            both_wet = wet_up + wet_low
            column_wet = wet + 0.5 * both_wet
            all_depth = both + (from_east(column) + from_west(column))
            all_wet = both_wet + (from_east(column_wet) + from_west(column_wet))
            total = 0.5 * (depth * all_wet + all_depth)
            diagonal = wet * (depth * (1.0 / (REACH * REACH)) + total) + (1.0 - wet)
            root = wet * lax.rsqrt(diagonal)
            s[r : r + n, :] = root
            se[r : r + n, :] = from_east(root)
            de[r : r + n, :] = from_east(depth)

    def links(kind, spans):
        depth_ref_, s, de, se, w = kinds[kind]
        for r, n in spans:
            d0, d1 = depth_ref_[r : r + n, :], depth_ref_[r + 1 : r + 1 + n, :]
            s0, s1 = s[r : r + n, :], s[r + 1 : r + 1 + n, :]
            de0, de1 = de[r : r + n, :], de[r + 1 : r + 1 + n, :]
            se0, se1 = se[r : r + n, :], se[r + 1 : r + 1 + n, :]
            east_w = -(d0 + de0) * (s0 * se0)
            ne_w = -0.5 * (d0 + de1) * (s0 * se1)
            nw_e = -0.5 * (de0 + d1) * (se0 * s1)
            w[0, r : r + n, :] = -(d0 + d1) * (s0 * s1)
            w[1, r : r + n, :] = east_w
            w[2, r : r + n, :] = from_west(east_w)
            w[3, r : r + n, :] = ne_w
            w[4, r : r + n, :] = from_west(ne_w)
            w[5, r : r + n, :] = from_west(nw_e)
            w[6, r : r + n, :] = nw_e

    def fold8(x):
        return sum(x[8 * k : 8 * k + 8] for k in range(x.shape[0] // 8))

    lane1 = lanes_of((1, COLS))
    main_lanes = within(lane1, 9, 119)
    strips_p, strips_r = strip_lanes(lane1, 0), strip_lanes(lane1, 64)

    def apply(b, k, w, r, size):
        up, mid, low = (b[k, r + o : r + o + size, :] for o in (1, 0, -1))
        a_u, a_d, e_u, e_c, e_d, f_u, f_c, f_d = w
        east_part = from_east(e_u * up + e_c * mid + e_d * low)
        west_part = from_west(f_u * up + f_c * mid + f_d * low)
        return mid, (a_u * up + a_d * low) + (east_part + west_part)

    def step(n, tasks, first, last):
        total = {}

        def add(key, product, lo, hi):
            value = fold8(product[lo:hi])
            total[key] = total[key] + value if key in total else value

        for kind, r, size, gram_lo, gram_hi in tasks:
            w = kinds[kind][4]
            weights = (
                w[0, r : r + size, :], w[0, r - 1 : r - 1 + size, :],
                w[4, r : r + size, :], w[2, r : r + size, :], w[5, r - 1 : r - 1 + size, :],
                w[6, r : r + size, :], w[1, r : r + size, :], w[3, r - 1 : r - 1 + size, :],
            )
            b, bases = (b_s, (0,)) if kind == "s" else (b_m, (0,) if last else (0, FIRST))
            news, olds = [], []
            for base in bases:
                mid, out = apply(b, base + n - 1, weights, r, size)
                out = 0.5 * out if first else out - b[base + n - 2, r : r + size, :]
                b[base + n, r : r + size, :] = out
                news.append(out)
                olds.append(mid)
            lo, hi = max(r, gram_lo) - r, min(r + size, gram_hi) - r
            if hi <= lo:
                continue
            p1, p0 = news[0], olds[0]
            if kind == "s":
                add("s0", p1 * p1, lo, hi)
                add("s1", p1 * p0, lo, hi)
                add("s4", p1 * shift(p1, 64), lo, hi)
                add("s5", p1 * shift(p0, 64), lo, hi)
                continue
            add("m0", p1 * p1, lo, hi)
            add("m1", p1 * p0, lo, hi)
            if last:
                r0 = b_m[FIRST + STEPS - 1, r : r + size, :]
            else:
                r1, r0 = news[1], olds[1]
                add("m2", r1 * r1, lo, hi)
                add("m3", r1 * r0, lo, hi)
                add("m4", p1 * r1, lo, hi)
            add("m5", p1 * r0, lo, hi)
        gather(n, total)

    def gather(n, total):
        rows = {key: jnp.sum(value, axis=0, keepdims=True) for key, value in total.items()}
        for c in range(6):
            row = jnp.zeros((1, COLS), F32)
            if "m%d" % c in rows:
                row = jnp.where(main_lanes, rows["m%d" % c], row)
            source = "s%d" % (c - 2 if c in (2, 3) else c)
            if source in rows:
                row = row + jnp.where(strips_r if c in (2, 3) else strips_p, rows[source], 0.0)
            at = pl.ds(6 * n + c, 1)
            rows_acc[at, :] = rows_acc[at, :] + row

    def steps(tasks):
        step(1, tasks, True, False)

        @pl.loop(2, STEPS)
        def _(n):
            step(n, tasks, False, False)

        step(STEPS, tasks, False, True)

    def tasks(kind, start, stop, gram_lo, gram_hi):
        return [(kind, r, n, gram_lo, gram_hi) for r, n in chunks(start, stop)]

    own_strips(chunks(16, 176))
    fields("m", chunks(16, 176))
    roots("m", [(17, 7)] + chunks(24, 168) + [(168, 7)])
    links("m", chunks(16, 168))

    @pl.when(jnp.logical_not(top))
    def _():
        next_level(1)

    start = {}
    for r, n in chunks(16, 176):
        p0, r0 = b_m[0, r : r + n, :], b_m[FIRST, r : r + n, :]
        for key, value in (("m0", p0 * p0), ("m2", r0 * r0), ("m4", p0 * r0)):
            start[key] = start[key] + fold8(value) if key in start else fold8(value)
    gather(0, start)
    steps(tasks("m", 16, 168, 32, 160))

    @pl.when(jnp.logical_not(top))
    def _():
        next_level(2)

    to_east.wait()
    to_west.wait()
    for g in range(4):
        at = 32 * g
        far_strips(16 + 40 * g, 40, got_e[...], got_w[...], (at, at + 9, at + 18))
    fields("s", chunks(16, 176))
    start = {}
    for r, n in chunks(16, 176):
        p0 = b_s[0, r : r + n, :]
        for key, value in (("s0", p0 * p0), ("s4", p0 * shift(p0, 64))):
            start[key] = start[key] + fold8(value) if key in start else fold8(value)
    gather(0, start)

    def from_south():
        @pl.when(jnp.logical_not(bottom))
        def _():
            to_se.wait_send()
            to_sw.wait_send()
            to_south.wait_send()
            to_ne.wait_recv()
            to_nw.wait_recv()
            to_north.wait_recv()
            own_strips([(0, 16)])
            far_strips(0, 16, corner[1], corner[0], (96, 105, 114))

        @pl.when(bottom)
        def _():
            for f in range(3):
                raw_m[f, 0:16, :] = jnp.zeros((16, COLS), F32)
            side_depth[0:16, :] = jnp.zeros((16, COLS), F32)
            side_state[0:16, :] = jnp.zeros((16, COLS), F32)

    @pl.when(jnp.logical_not(top))
    def _():
        from_south()
        to_ne.wait_send()
        to_nw.wait_send()
        to_north.wait_send()
        to_se.wait_recv()
        to_sw.wait_recv()
        to_south.wait_recv()
        own_strips([(176, 16)])
        far_strips(176, 16, corner[3], corner[2], (0, 9, 18))
        for kind in ("m", "s"):
            fields(kind, [(LO, 8), (176, 8)])
        roots("m", [(LO, 16), (168, 16)])
        roots("s", chunks(LO, 184))
        links("m", [(LO, 16), (168, 16)])
        links("s", chunks(LO, 184))
        steps([("m", LO, 24, 16, 32), ("m", 160, 24, 160, 176)] + tasks("s", LO, 184, 16, 176))

    @pl.when(top)
    def _():
        from_south()
        for kind in ("m", "s"):
            fields(kind, [(LO, 8)])
        roots("m", [(LO, 16)])
        roots("s", chunks(LO, 168) + [(168, 7)])
        links("m", [(LO, 16)])
        links("s", chunks(LO, 168))
        steps([("m", LO, 24, 16, 32)] + tasks("s", LO, 168, 16, 160))
        for copy in fold_z_copies:
            copy.wait_recv()
        ghost = fold_got[0]
        for k in range(1, NZ):
            ghost = ghost + fold_got[k]
        edges = ghost[32:40]
        lane8 = lanes_of((8, COLS))
        side = []
        for g in range(4):
            edge = pltpu.roll(edges, (COLS - 16 - 32 * g) % COLS, 1)
            side.append(jnp.where((lane8 < 9) | (lane8 >= 119), edge, 0.0))
        side = jnp.concatenate(side, axis=0)
        for f in range(3):
            raw_m[f, 176:192, :] = jnp.zeros((16, COLS), F32)
        raw_m[0, 176:185, :] = ghost[0:9]
        raw_m[1, 176:184, :] = ghost[9:17]
        raw_m[2, 176:184, :] = ghost[17:25]
        own_strips([(176, 16)])
        fold_x[...] = side
        west_p, west_r, east_r = (within(lane1, a, a + 9) for a in (WEST - 9, WEST + 55, 64))
        for ref, p, q, count in ((side_depth, 0, 0, 9), (side_state, 17, 9, 8)):
            one, two = fold_x[p : p + count, :], fold_x[q : q + count, :]
            ref[176 : 176 + count, :] = jnp.where(
                lane1 < 9, one, jnp.where(west_p, shift(one, WEST), jnp.where(
                    east_r, shift(two, 64), jnp.where(
                        west_r, shift(two, WEST + 64), ref[176 : 176 + count, :]))))
        for kind in ("m", "s"):
            fields(kind, [(176, 8)])
            roots(kind, [(168, 16)])
            links(kind, [(168, 16)])
        steps([("m", 160, 24, 160, 176), ("s", 160, 24, 160, 176)])
        for copy in fold_x_copies + fold_z_copies:
            copy.wait_send()

    ones = jnp.ones((8, COLS), F32)
    sums = lax.dot_general(
        ones, rows_acc[...], (((1,), (1,)), ((), ())), precision=HIGHEST, preferred_element_type=F32
    )[0:1]

    def reduce(stage, value, slots, send, recv, count, mine, peer_of, order):
        slots[mine] = value
        part[stage] = value
        copies = [
            remote(part.at[stage], slots.at[mine], send.at[d - 1], recv.at[d - 1], *peer_of(d))
            for d in range(1, count)
        ]
        for d in order:
            copies[d - 1].start()
        for copy in copies:
            copy.wait_recv()
        terms = [slots[k] for k in range(count)]
        while len(terms) > 1:
            terms = [a + b for a, b in zip(terms[::2], terms[1::2])]
        return terms[0], copies

    sums, first_copies = reduce(
        0, sums, red_y, ry_send, ry_recv, LAT, lat,
        lambda d: ((lat + d) % LAT, lon), far_first(LAT))
    next_level(levels)
    sums, second_copies = reduce(
        1, sums, red_p, rp_send, rp_recv, LON, lon,
        lambda d: (lat, (lon + d) % LON), far_first(LON))
    moments_out[...] = sums
    for copy in first_copies + second_copies:
        copy.wait_send()


def held(shape):
    return pltpu.VMEM(shape, F32)


def basis_and_moments(forcing, search, depth, mask, fold_map):
    vm = pltpu.VMEM
    dma = pltpu.SemaphoreType.DMA
    ext = (EXT, COLS)
    return pl.pallas_call(
        basis_kernel,
        out_shape=(held((FIELDS,) + ext), held((STEPS + 1,) + ext), held((1, COLS))),
        in_specs=[pl.BlockSpec(memory_space=pl.ANY)] * 5,
        out_specs=(pl.BlockSpec(memory_space=vm),) * 3,
        scratch_shapes=[
            pltpu.SMEM((1024,), jnp.int32),
            vm((3,) + ext, F32), vm(ext, F32), vm(ext, F32),
            vm((ROWS, COLS), F32), vm((ROWS, COLS), jnp.int32),
            vm((40, COLS), F32), vm((40, COLS), F32), vm((40, COLS), F32), vm((40, COLS), F32),
            vm((4, 16, COLS), F32),
            vm((32, COLS), F32), vm((32, COLS), F32), vm((NX + 1, 32, COLS), F32),
            vm((NZ, 40, COLS), F32), vm((NZ, 40, COLS), F32),
        ]
        + [vm(ext, F32)] * 6
        + [vm((7,) + ext, F32)] * 2
        + [
            vm((COLS, COLS), F32), vm((2, 1, COLS), F32),
            vm((LON, 1, COLS), F32), vm((LAT, 1, COLS), F32),
            pltpu.SemaphoreType.REGULAR((4,)), dma((5,)), dma((8,)), dma((8,)),
            dma((NZ - 1,)), dma((NZ - 1,)), dma((NX - 1,)), dma((NX - 1,)),
            dma((LON - 1,)), dma((LON - 1,)), dma((LAT - 1,)), dma((LAT - 1,)),
        ],
        compiler_params=pltpu.CompilerParams(collective_id=0, has_side_effects=True),
        name="basis",
    )(fold_map, forcing, search, depth, mask)


def combine_kernel(moments_ref, basis_ref, strips_ref, height_ref, residual_ref):
    shape = (24, COLS)
    row = lax.broadcasted_iota(jnp.int32, shape, 0)
    col = lanes_of(shape)

    def power(i):
        return jnp.where(i >= FIRST, i - FIRST, i)

    kind = jnp.where((row >= FIRST) & (col >= FIRST), 1, jnp.where((row >= FIRST) | (col >= FIRST), 2, 0))
    valid = (row < FIELDS) & (col < FIELDS)
    ka, kb = power(row), power(col)
    high, low = ka + kb, jnp.abs(ka - kb)
    odd = high & 1

    def slot(k):
        return jnp.where(valid, 6 * ((k + 1) >> 1) + 2 * kind + odd, 0)

    base = jnp.where(odd == 1, 7 + 2 * kind, 2 * kind)
    raw = jnp.broadcast_to(moments_ref[...], shape)

    def take(index):
        return jnp.take_along_axis(raw, index, axis=1)

    gram = jnp.where(valid, take(slot(high)) + take(slot(low)) - take(jnp.where(valid, base, 0)), 0.0)

    def lower(i):
        return jnp.where((i == 1) | (i == FIRST + 1), 1.0, jnp.where((i >= 1) & (i < FIELDS) & (i != FIRST), 0.5, 0.0))

    def upper(i):
        return jnp.where((i < FIELDS - 2) & (i != FIRST - 2) & (i != FIRST - 1), 0.5, 0.0)

    low_l, up_l = lower(col).astype(F32), upper(col).astype(F32)
    low_s, up_s = lower(row).astype(F32), upper(row).astype(F32)

    def shifted(v, axis):
        length = v.shape[axis]
        low_c, up_c = (low_s, up_s) if axis == 0 else (low_l, up_l)
        return v + low_c * pltpu.roll(v, 1, axis) + up_c * pltpu.roll(v, length - 1, axis)

    below = pltpu.roll(low_l, COLS - 1, 1)
    above = pltpu.roll(up_l, 1, 1)
    ends = (col == FIRST - 1) | (col == FIELDS - 1)
    gram_h = jnp.where(
        ends, 0.0,
        gram + below * pltpu.roll(gram, COLS - 1, 1) + jnp.where(col > 0, above, 0.0) * pltpu.roll(gram, 1, 1),
    )

    def form(matrix, left, right):
        return jnp.sum(matrix * left * right, keepdims=True)

    unit = lambda at: ((row == at).astype(F32), (col == at).astype(F32))
    p_s, p_l = unit(0)
    r_s, r_l = unit(FIRST)
    q_s, q_l = shifted(p_s, 0), shifted(p_l, 1)
    x_s = jnp.zeros(shape, F32)
    norm = form(gram, r_s, r_l)
    curvature = form(gram_h, p_s, p_l)
    for inner in range(STEPS):
        t = norm / curvature
        x_s = x_s + t * p_s
        r_s = r_s - t * q_s
        if inner == STEPS - 1:
            break
        r_l = r_l - t * q_l
        h_s, h_l = shifted(r_s, 0), shifted(r_l, 1)
        fresh = form(gram, r_s, r_l)
        own = form(gram_h, r_s, r_l)
        cross = form(gram_h, r_s, p_l)
        beta = fresh / norm
        curvature = own + beta * (2.0 * cross + beta * curvature)
        norm = fresh
        p_s, p_l = r_s + beta * p_s, r_l + beta * p_l
        q_s, q_l = h_s + beta * q_s, h_l + beta * q_l

    lane1 = lanes_of((1, COLS))
    search_half = within((lane1 + 32) & (COLS - 1), 14, 78)
    size = 32
    for coords, out_ref in ((x_s, height_ref), (r_s, residual_ref)):
        mixed = []
        for n in range(STEPS + 1):
            other = coords[FIRST + n : FIRST + n + 1, :] if n < STEPS else jnp.zeros((1, COLS), F32)
            mixed.append(jnp.where(search_half, coords[n : n + 1, :], other))
        for at in range(0, ROWS, size):
            rows = slice(16 + at, 16 + at + size)
            main = sum(coords[k : k + 1, :] * basis_ref[k, rows, :] for k in range(FIELDS))
            strip = sum(mixed[n] * strips_ref[n, rows, :] for n in range(STEPS + 1))
            strip = strip + shift(strip, 64)
            out_ref[at : at + size, :] = jnp.where(
                lane1 >= 119, strip, jnp.where(lane1 < 9, shift(strip, -WEST), main)
            )


def per_device(forcing, search, depth, mask, fold_map):
    made = basis_and_moments(forcing, search, depth, mask, fold_map)
    basis, strips, moments = (pltpu.with_memory_space_constraint(v, pltpu.VMEM) for v in made)
    block = jax.ShapeDtypeStruct((ROWS, COLS), F32)
    return pl.pallas_call(
        combine_kernel,
        out_shape=(block, block),
        in_specs=[pl.BlockSpec(memory_space=pltpu.VMEM)] * 3,
        name="combine",
    )(moments, basis, strips)


def solution(mesh):
    return jax.shard_map(
        per_device,
        mesh=mesh,
        in_specs=(P("lat", "lon"),) * 4 + (P(),),
        out_specs=(P("lat", "lon"),) * 2,
        check_vma=False,
    )
```

```python
import functools

import jax
import jax.numpy as jnp
from jax import lax
from jax.experimental import pallas as pl
from jax.experimental.pallas import tpu as pltpu
from jax.sharding import PartitionSpec as P

STEPS = 8
REACH = 256
LAT, LON, NX, NZ = 16, 32, 4, 8
ROWS, COLS = 160, 128
EXT = ROWS + 32
LO = 8
FIELDS = 2 * STEPS + 1
FIRST = STEPS + 1
HIGHEST = lax.Precision.HIGHEST
F32 = jnp.float32


def lanes_of(shape):
    return lax.broadcasted_iota(jnp.int32, shape, len(shape) - 1)


def from_east(x):
    return pltpu.roll(x, COLS - 1, 1)


def from_west(x):
    return pltpu.roll(x, 1, 1)


def shift(x, by):
    by %= COLS
    return pltpu.roll(x, by, 1) if by else x


WEST = 28


def strip_lanes(lane, half):
    lane = (lane - half) & (COLS - 1)
    return (lane >= 119) | ((lane >= WEST) & (lane < WEST + 9))


def within(lane, start, stop):
    return (lane >= start) & (lane < stop)


def remote(src, dst, send, recv, lat, lon):
    return pltpu.make_async_remote_copy(
        src_ref=src,
        dst_ref=dst,
        send_sem=send,
        recv_sem=recv,
        device_id={"lat": lat, "lon": lon},
        device_id_type=pl.DeviceIdType.MESH,
    )


CHUNK = 16


def far_first(count):
    return sorted(range(1, count), key=lambda d: (-min(d, count - d), d))


def chunks(start, stop):
    return [(r, min(CHUNK, stop - r)) for r in range(start, stop, CHUNK)]


def basis_kernel(
    fold_ref, forcing_ref, search_ref, depth_ref, mask_ref,
    b_m, b_s, moments_out,
    fold_buf, raw_m, side_depth, side_state, depth_buf, mask_buf, pack_w, pack_e, got_w, got_e, corner,
    fold_x, fold_src, fold_row, fold_send, fold_got,
    s_m, s_s, de_m, de_s, se_m, se_s,
    w_m, w_s, rows_acc, part, red_p, red_y,
    plane_sem, local_sem, halo_send, halo_recv, fz_send, fz_recv, fx_send, fx_recv,
    rp_send, rp_recv, ry_send, ry_recv,
):
    lat = lax.axis_index("lat")
    lon = lax.axis_index("lon")
    zi, xi = lon // NX, lon % NX
    core, yi = lat % 2, lat // 2
    top = lat == LAT - 1
    bottom = lat == 0
    north, south = (lat + 1) % LAT, (lat + LAT - 1) % LAT
    east, west = (lon + 1) % LON, (lon + LON - 1) % LON
    barrier = pltpu.get_barrier_semaphore()

    loads = [
        pltpu.make_async_copy(depth_ref, depth_buf, local_sem.at[0]),
        pltpu.make_async_copy(mask_ref, mask_buf, local_sem.at[1]),
        pltpu.make_async_copy(forcing_ref, raw_m.at[1, pl.ds(16, ROWS), :], local_sem.at[2]),
        pltpu.make_async_copy(search_ref, raw_m.at[2, pl.ds(16, ROWS), :], local_sem.at[3]),
        pltpu.make_async_copy(fold_ref.at[pl.ds(0, 1024)], fold_buf, local_sem.at[4]),
    ]
    for copy in loads:
        copy.start()

    def greet(semaphore, to):
        for a, b in to:
            pl.semaphore_signal(
                semaphore, inc=1, device_id={"lat": a, "lon": b}, device_id_type=pl.DeviceIdType.MESH
            )

    def around(far):
        if 2 * far == NZ:
            return [(lat, (lon + NX * far) % LON)]
        to = [(lat, (lon + NX * far) % LON), (lat, (lon + LON - NX * far) % LON)]
        if 2 * far < LAT:
            to += [((lat + 2 * far) % LAT, lon), ((lat + LAT - 2 * far) % LAT, lon)]
        return to

    beside = [(lat, zi * NX + (xi + d) % NX) for d in far_first(NX)]
    beside += [(north, east), (north, west), (south, east), (south, west)]
    beside += [(lat, east), (lat, west), (north, lon), (south, lon)] + around(1)

    beside += [(lat + 1 - 2 * core, zi * NX + (xi + d) % NX) for d in far_first(NX)]
    greet(barrier, beside)

    levels = 3

    def next_level(level):
        if level > 0:
            pl.semaphore_wait(plane_sem.at[level - 1], len(around(1 << (level - 1))))
        if level < levels:
            greet(plane_sem.at[level], around(1 << level))

    rows_acc[...] = jnp.zeros_like(rows_acc)
    for copy in loads:
        copy.wait()
    raw_m[0, 16 : 16 + ROWS, :] = depth_buf[...] * mask_buf[...].astype(F32)

    pivot = fold_buf[0]
    pivot_block, pivot_lane = lax.shift_right_logical(pivot, 7), pivot & (COLS - 1)

    @pl.when(top)
    def _():
        fold_x[...] = jnp.zeros_like(fold_x)
        for m in range(9):
            fold_x[m : m + 1, :] = raw_m[0, 175 - m : 176 - m, :]
        for m in range(8):
            fold_x[9 + m : 10 + m, :] = raw_m[1, 175 - m : 176 - m, :]
            fold_x[17 + m : 18 + m, :] = raw_m[2, 175 - m : 176 - m, :]
        source = lax.broadcasted_iota(jnp.int32, (COLS, COLS), 0)
        target = lax.broadcasted_iota(jnp.int32, (COLS, COLS), 1)
        choose = (source == ((pivot - target) & (COLS - 1))).astype(F32)
        turned = jnp.dot(fold_x[...], choose, precision=HIGHEST, preferred_element_type=F32)
        fold_src[...] = turned
        fold_row[xi] = turned
        fold_row[NX] = jnp.zeros_like(turned)

    lane40 = lanes_of((40, COLS))
    acc_w = jnp.zeros((40, COLS), F32)
    acc_e = jnp.zeros((40, COLS), F32)
    for g in range(4):
        for f in range(3):
            at = 32 * g + 9 * f
            block = raw_m[f, 16 + 40 * g : 56 + 40 * g, :]
            here = (lane40 >= at) & (lane40 < at + 9)
            acc_w = jnp.where(here, pltpu.roll(block, at, 1) if at else block, acc_w)
            acc_e = jnp.where(here, pltpu.roll(block, (at - 119) % COLS, 1), acc_e)
    pack_w[...] = acc_w
    pack_e[...] = acc_e

    pl.semaphore_wait(barrier, len(beside))

    fold_x_copies = [
        remote(fold_src, fold_row.at[xi], fx_send.at[d - 1], fx_recv.at[d - 1], lat, zi * NX + (xi + d) % NX)
        for d in range(1, NX)
    ]

    @pl.when(top)
    def _():
        for d in far_first(NX):
            fold_x_copies[d - 1].start()

    to_north = remote(raw_m.at[:, pl.ds(160, 16), :], raw_m.at[:, pl.ds(0, 16), :],
                      halo_send.at[0], halo_recv.at[0], north, lon)
    to_south = remote(raw_m.at[:, pl.ds(16, 16), :], raw_m.at[:, pl.ds(176, 16), :],
                      halo_send.at[1], halo_recv.at[1], south, lon)
    to_east = remote(pack_e, got_w, halo_send.at[2], halo_recv.at[2], lat, east)
    to_west = remote(pack_w, got_e, halo_send.at[3], halo_recv.at[3], lat, west)
    to_ne = remote(pack_e.at[pl.ds(24, 16), :], corner.at[0], halo_send.at[4], halo_recv.at[4], north, east)
    to_nw = remote(pack_w.at[pl.ds(24, 16), :], corner.at[1], halo_send.at[5], halo_recv.at[5], north, west)
    to_se = remote(pack_e.at[pl.ds(0, 16), :], corner.at[2], halo_send.at[6], halo_recv.at[6], south, east)
    to_sw = remote(pack_w.at[pl.ds(0, 16), :], corner.at[3], halo_send.at[7], halo_recv.at[7], south, west)

    to_east.start()
    to_west.start()
    next_level(0)

    @pl.when(jnp.logical_not(top))
    def _():
        to_ne.start()
        to_nw.start()
        to_north.start()

    @pl.when(jnp.logical_not(bottom))
    def _():
        to_se.start()
        to_sw.start()
        to_south.start()

    fold_z_copies = [
        remote(fold_send.at[d], fold_got.at[zi], fz_send.at[d - 1], fz_recv.at[d - 1],
               lat, ((zi + d) % NZ) * NX + xi)
        for d in range(1, NZ)
    ]
    lane32 = lanes_of((32, COLS))
    near = lane32 <= pivot_lane

    @pl.when(top)
    def _():
        next_level(1)
        next_level(2)
        for copy in fold_x_copies:
            copy.wait_recv()
        for d in far_first(NZ) + [0]:
            want = pivot_block - ((zi + d) % NZ) * NX - xi

            def block(b):
                mine = (lax.shift_right_logical(b & (LON - 1), 2) == zi)
                return fold_row[jnp.where(mine, b & (NX - 1), NX)]

            ahead, here, behind, beyond = (block(want + o) for o in (1, 0, -1, -2))
            window = jnp.where(near, here, behind)
            edge = jnp.where(
                lane32 < 9, jnp.where(near, behind, beyond),
                jnp.where(lane32 >= 119, jnp.where(near, ahead, here), 0.0),
            )
            edges = sum(pltpu.roll(edge[8 * g : 8 * g + 8], 16 + 32 * g, 1) for g in range(4))
            if d:
                fold_send[d, 0:32, :] = window
                fold_send[d, 32:40, :] = edges
            else:
                fold_got[zi, 0:32, :] = window
                fold_got[zi, 32:40, :] = edges
        for d in far_first(NZ):
            fold_z_copies[d - 1].start()

    def own_strips(spans):
        for r, n in spans:
            depth, residual, search = (raw_m[f, r : r + n, :] for f in range(3))
            lane = lanes_of((n, COLS))
            west_p, east_r, west_r = (within(lane, a, a + 18) for a in (WEST, 46, WEST + 64))
            east_p = lane >= 110
            for ref, p, q in ((side_depth, depth, depth), (side_state, search, residual)):
                ref[r : r + n, :] = jnp.where(
                    east_p, p, jnp.where(west_p, shift(p, WEST), jnp.where(
                        east_r, shift(q, 64), jnp.where(west_r, shift(q, WEST + 64), 0.0))))

    def far_strips(r, n, from_e, from_w, places):
        lane = lanes_of((n, COLS))
        west_p, east_r, west_r = (within(lane, a, a + 9) for a in (WEST - 9, 64, WEST + 55))
        east_p = lane < 9
        at_d, at_r, at_p = places
        for ref, p, q in ((side_depth, at_d, at_d), (side_state, at_p, at_r)):
            ref[r : r + n, :] = jnp.where(
                east_p, shift(from_e, -p), jnp.where(west_p, shift(from_w, WEST - 9 - p), jnp.where(
                    east_r, shift(from_e, 64 - q), jnp.where(
                        west_r, shift(from_w, WEST + 55 - q), ref[r : r + n, :]))))

    kinds = {
        "m": (raw_m.at[0], s_m, de_m, se_m, w_m),
        "s": (side_depth, s_s, de_s, se_s, w_s),
    }

    def fields(kind, spans):
        for r, n in spans:
            wet = (kinds[kind][0][r : r + n, :] > 0.0).astype(F32)
            if kind == "m":
                b_m[0, r : r + n, :] = wet * raw_m[2, r : r + n, :]
                b_m[FIRST, r : r + n, :] = wet * raw_m[1, r : r + n, :]
            else:
                b_s[0, r : r + n, :] = wet * side_state[r : r + n, :]

    def roots(kind, spans):
        depth_ref_, s, de, se, _ = kinds[kind]
        for r, n in spans:
            up, depth, low = (depth_ref_[r + o : r + o + n, :] for o in (1, 0, -1))
            both = up + low
            column = depth + 0.5 * both
            wet_up, wet, wet_low = ((v > 0.0).astype(F32) for v in (up, depth, low))
            both_wet = wet_up + wet_low
            column_wet = wet + 0.5 * both_wet
            all_depth = both + (from_east(column) + from_west(column))
            all_wet = both_wet + (from_east(column_wet) + from_west(column_wet))
            total = 0.5 * (depth * all_wet + all_depth)
            diagonal = wet * (depth * (1.0 / (REACH * REACH)) + total) + (1.0 - wet)
            root = wet * lax.rsqrt(diagonal)
            s[r : r + n, :] = root
            se[r : r + n, :] = from_east(root)
            de[r : r + n, :] = from_east(depth)

    def links(kind, spans):
        depth_ref_, s, de, se, w = kinds[kind]
        for r, n in spans:
            d0, d1 = depth_ref_[r : r + n, :], depth_ref_[r + 1 : r + 1 + n, :]
            s0, s1 = s[r : r + n, :], s[r + 1 : r + 1 + n, :]
            de0, de1 = de[r : r + n, :], de[r + 1 : r + 1 + n, :]
            se0, se1 = se[r : r + n, :], se[r + 1 : r + 1 + n, :]
            east_w = -(d0 + de0) * (s0 * se0)
            ne_w = -0.5 * (d0 + de1) * (s0 * se1)
            nw_e = -0.5 * (de0 + d1) * (se0 * s1)
            w[0, r : r + n, :] = -(d0 + d1) * (s0 * s1)
            w[1, r : r + n, :] = east_w
            w[2, r : r + n, :] = from_west(east_w)
            w[3, r : r + n, :] = ne_w
            w[4, r : r + n, :] = from_west(ne_w)
            w[5, r : r + n, :] = from_west(nw_e)
            w[6, r : r + n, :] = nw_e

    def fold8(x):
        return sum(x[8 * k : 8 * k + 8] for k in range(x.shape[0] // 8))

    lane1 = lanes_of((1, COLS))
    main_lanes = within(lane1, 9, 119)
    strips_p, strips_r = strip_lanes(lane1, 0), strip_lanes(lane1, 64)

    def apply(b, k, w, r, size):
        up, mid, low = (b[k, r + o : r + o + size, :] for o in (1, 0, -1))
        a_u, a_d, e_u, e_c, e_d, f_u, f_c, f_d = w
        east_part = from_east(e_u * up + e_c * mid + e_d * low)
        west_part = from_west(f_u * up + f_c * mid + f_d * low)
        return mid, (a_u * up + a_d * low) + (east_part + west_part)

    def step(n, tasks, first, last):
        total = {}

        def add(key, product, lo, hi):
            value = fold8(product[lo:hi])
            total[key] = total[key] + value if key in total else value

        for kind, r, size, gram_lo, gram_hi in tasks:
            w = kinds[kind][4]
            weights = (
                w[0, r : r + size, :], w[0, r - 1 : r - 1 + size, :],
                w[4, r : r + size, :], w[2, r : r + size, :], w[5, r - 1 : r - 1 + size, :],
                w[6, r : r + size, :], w[1, r : r + size, :], w[3, r - 1 : r - 1 + size, :],
            )
            b, bases = (b_s, (0,)) if kind == "s" else (b_m, (0,) if last else (0, FIRST))
            news, olds = [], []
            for base in bases:
                mid, out = apply(b, base + n - 1, weights, r, size)
                out = 0.5 * out if first else out - b[base + n - 2, r : r + size, :]
                b[base + n, r : r + size, :] = out
                news.append(out)
                olds.append(mid)
            lo, hi = max(r, gram_lo) - r, min(r + size, gram_hi) - r
            if hi <= lo:
                continue
            p1, p0 = news[0], olds[0]
            if kind == "s":
                add("s0", p1 * p1, lo, hi)
                add("s1", p1 * p0, lo, hi)
                add("s4", p1 * shift(p1, 64), lo, hi)
                add("s5", p1 * shift(p0, 64), lo, hi)
                continue
            add("m0", p1 * p1, lo, hi)
            add("m1", p1 * p0, lo, hi)
            if last:
                r0 = b_m[FIRST + STEPS - 1, r : r + size, :]
            else:
                r1, r0 = news[1], olds[1]
                add("m2", r1 * r1, lo, hi)
                add("m3", r1 * r0, lo, hi)
                add("m4", p1 * r1, lo, hi)
            add("m5", p1 * r0, lo, hi)
        gather(n, total)

    def gather(n, total):
        rows = {key: jnp.sum(value, axis=0, keepdims=True) for key, value in total.items()}
        for c in range(6):
            row = jnp.zeros((1, COLS), F32)
            if "m%d" % c in rows:
                row = jnp.where(main_lanes, rows["m%d" % c], row)
            source = "s%d" % (c - 2 if c in (2, 3) else c)
            if source in rows:
                row = row + jnp.where(strips_r if c in (2, 3) else strips_p, rows[source], 0.0)
            at = pl.ds(6 * n + c, 1)
            rows_acc[at, :] = rows_acc[at, :] + row

    def steps(tasks):
        step(1, tasks, True, False)

        @pl.loop(2, STEPS)
        def _(n):
            step(n, tasks, False, False)

        step(STEPS, tasks, False, True)

    def tasks(kind, start, stop, gram_lo, gram_hi):
        return [(kind, r, n, gram_lo, gram_hi) for r, n in chunks(start, stop)]

    own_strips(chunks(16, 176))
    fields("m", chunks(16, 176))
    roots("m", [(17, 7)] + chunks(24, 168) + [(168, 7)])
    links("m", chunks(16, 168))

    @pl.when(jnp.logical_not(top))
    def _():
        next_level(1)

    start = {}
    for r, n in chunks(16, 176):
        p0, r0 = b_m[0, r : r + n, :], b_m[FIRST, r : r + n, :]
        for key, value in (("m0", p0 * p0), ("m2", r0 * r0), ("m4", p0 * r0)):
            start[key] = start[key] + fold8(value) if key in start else fold8(value)
    gather(0, start)
    steps(tasks("m", 16, 168, 32, 160))

    @pl.when(jnp.logical_not(top))
    def _():
        next_level(2)

    to_east.wait()
    to_west.wait()
    for g in range(4):
        at = 32 * g
        far_strips(16 + 40 * g, 40, got_e[...], got_w[...], (at, at + 9, at + 18))
    fields("s", chunks(16, 176))
    start = {}
    for r, n in chunks(16, 176):
        p0 = b_s[0, r : r + n, :]
        for key, value in (("s0", p0 * p0), ("s4", p0 * shift(p0, 64))):
            start[key] = start[key] + fold8(value) if key in start else fold8(value)
    gather(0, start)

    def from_south():
        @pl.when(jnp.logical_not(bottom))
        def _():
            to_se.wait_send()
            to_sw.wait_send()
            to_south.wait_send()
            to_ne.wait_recv()
            to_nw.wait_recv()
            to_north.wait_recv()
            own_strips([(0, 16)])
            far_strips(0, 16, corner[1], corner[0], (96, 105, 114))

        @pl.when(bottom)
        def _():
            for f in range(3):
                raw_m[f, 0:16, :] = jnp.zeros((16, COLS), F32)
            side_depth[0:16, :] = jnp.zeros((16, COLS), F32)
            side_state[0:16, :] = jnp.zeros((16, COLS), F32)

    @pl.when(jnp.logical_not(top))
    def _():
        from_south()
        to_ne.wait_send()
        to_nw.wait_send()
        to_north.wait_send()
        to_se.wait_recv()
        to_sw.wait_recv()
        to_south.wait_recv()
        own_strips([(176, 16)])
        far_strips(176, 16, corner[3], corner[2], (0, 9, 18))
        for kind in ("m", "s"):
            fields(kind, [(LO, 8), (176, 8)])
        roots("m", [(LO, 16), (168, 16)])
        roots("s", chunks(LO, 184))
        links("m", [(LO, 16), (168, 16)])
        links("s", chunks(LO, 184))
        steps([("m", LO, 24, 16, 32), ("m", 160, 24, 160, 176)] + tasks("s", LO, 184, 16, 176))

    @pl.when(top)
    def _():
        from_south()
        for kind in ("m", "s"):
            fields(kind, [(LO, 8)])
        roots("m", [(LO, 16)])
        roots("s", chunks(LO, 168) + [(168, 7)])
        links("m", [(LO, 16)])
        links("s", chunks(LO, 168))
        steps([("m", LO, 24, 16, 32)] + tasks("s", LO, 168, 16, 160))
        for copy in fold_z_copies:
            copy.wait_recv()
        ghost = fold_got[0]
        for k in range(1, NZ):
            ghost = ghost + fold_got[k]
        edges = ghost[32:40]
        lane8 = lanes_of((8, COLS))
        side = []
        for g in range(4):
            edge = pltpu.roll(edges, (COLS - 16 - 32 * g) % COLS, 1)
            side.append(jnp.where((lane8 < 9) | (lane8 >= 119), edge, 0.0))
        side = jnp.concatenate(side, axis=0)
        for f in range(3):
            raw_m[f, 176:192, :] = jnp.zeros((16, COLS), F32)
        raw_m[0, 176:185, :] = ghost[0:9]
        raw_m[1, 176:184, :] = ghost[9:17]
        raw_m[2, 176:184, :] = ghost[17:25]
        own_strips([(176, 16)])
        fold_x[...] = side
        west_p, west_r, east_r = (within(lane1, a, a + 9) for a in (WEST - 9, WEST + 55, 64))
        for ref, p, q, count in ((side_depth, 0, 0, 9), (side_state, 17, 9, 8)):
            one, two = fold_x[p : p + count, :], fold_x[q : q + count, :]
            ref[176 : 176 + count, :] = jnp.where(
                lane1 < 9, one, jnp.where(west_p, shift(one, WEST), jnp.where(
                    east_r, shift(two, 64), jnp.where(
                        west_r, shift(two, WEST + 64), ref[176 : 176 + count, :]))))
        for kind in ("m", "s"):
            fields(kind, [(176, 8)])
            roots(kind, [(168, 16)])
            links(kind, [(168, 16)])
        steps([("m", 160, 24, 160, 176), ("s", 160, 24, 160, 176)])
        for copy in fold_x_copies + fold_z_copies:
            copy.wait_send()

    ones = jnp.ones((8, COLS), F32)
    sums = lax.dot_general(
        ones, rows_acc[...], (((1,), (1,)), ((), ())), precision=HIGHEST, preferred_element_type=F32
    )[0:1]

    def tree(terms):
        while len(terms) > 1:
            terms = [a + b for a, b in zip(terms[::2], terms[1::2])]
        return terms[0]

    second = core == 1
    part[0] = sums
    next_level(levels)
    to_plane = [
        remote(part.at[0], red_p.at[core * LON + lon], rp_send.at[d], rp_recv.at[core * LON + d],
               2 * yi + 1, (lon + d) % LON)
        for d in range(LON)
    ]
    for d in far_first(LON):
        to_plane[d].start()
    count = LAT // 2
    along_y = [(d, c) for d in far_first(count) + [0] for c in (1, 0) if (d, c) != (0, 1)]
    to_lat = [
        remote(part.at[1], red_y.at[yi], ry_send.at[2 * d + c], ry_recv.at[d],
               2 * ((yi + d) % count) + c, lon)
        for d, c in along_y
    ]

    @pl.when(jnp.logical_not(second))
    def _():
        to_plane[0].start()
        to_plane[0].wait_send()

    @pl.when(second)
    def _():
        red_p[LON + lon] = sums
        for c in range(2):
            for d in range(c, LON):
                remote(part.at[0], red_p.at[c * LON + lon], rp_send.at[d], rp_recv.at[c * LON + d],
                       lat, east).wait_recv()
        total = tree([red_p[k] for k in range(2 * LON)])
        part[1] = total
        red_y[yi] = total
        for copy in to_lat:
            copy.start()

    def arrived(d):
        remote(part.at[1], red_y.at[yi], ry_send.at[0], ry_recv.at[d], lat, east).wait_recv()

    @pl.when(jnp.logical_not(second))
    def _():
        arrived(0)

    for d in range(1, count):
        arrived(d)
    moments_out[...] = tree([red_y[k] for k in range(count)])

    @pl.when(second)
    def _():
        for copy in to_lat:
            copy.wait_send()

    for copy in to_plane[1:]:
        copy.wait_send()


def held(shape):
    return pltpu.VMEM(shape, F32)


def basis_and_moments(forcing, search, depth, mask, fold_map):
    vm = pltpu.VMEM
    dma = pltpu.SemaphoreType.DMA
    ext = (EXT, COLS)
    return pl.pallas_call(
        basis_kernel,
        out_shape=(held((FIELDS,) + ext), held((STEPS + 1,) + ext), held((1, COLS))),
        in_specs=[pl.BlockSpec(memory_space=pl.ANY)] * 5,
        out_specs=(pl.BlockSpec(memory_space=vm),) * 3,
        scratch_shapes=[
            pltpu.SMEM((1024,), jnp.int32),
            vm((3,) + ext, F32), vm(ext, F32), vm(ext, F32),
            vm((ROWS, COLS), F32), vm((ROWS, COLS), jnp.int32),
            vm((40, COLS), F32), vm((40, COLS), F32), vm((40, COLS), F32), vm((40, COLS), F32),
            vm((4, 16, COLS), F32),
            vm((32, COLS), F32), vm((32, COLS), F32), vm((NX + 1, 32, COLS), F32),
            vm((NZ, 40, COLS), F32), vm((NZ, 40, COLS), F32),
        ]
        + [vm(ext, F32)] * 6
        + [vm((7,) + ext, F32)] * 2
        + [
            vm((COLS, COLS), F32), vm((2, 1, COLS), F32),
            vm((2 * LON, 1, COLS), F32), vm((LAT // 2, 1, COLS), F32),
            pltpu.SemaphoreType.REGULAR((4,)), dma((5,)), dma((8,)), dma((8,)),
            dma((NZ - 1,)), dma((NZ - 1,)), dma((NX - 1,)), dma((NX - 1,)),
            dma((LON,)), dma((2 * LON,)), dma((LAT,)), dma((LAT // 2,)),
        ],
        compiler_params=pltpu.CompilerParams(collective_id=0, has_side_effects=True),
        name="basis",
    )(fold_map, forcing, search, depth, mask)


def combine_kernel(moments_ref, basis_ref, strips_ref, height_ref, residual_ref):
    shape = (24, COLS)
    row = lax.broadcasted_iota(jnp.int32, shape, 0)
    col = lanes_of(shape)

    def power(i):
        return jnp.where(i >= FIRST, i - FIRST, i)

    kind = jnp.where((row >= FIRST) & (col >= FIRST), 1, jnp.where((row >= FIRST) | (col >= FIRST), 2, 0))
    valid = (row < FIELDS) & (col < FIELDS)
    ka, kb = power(row), power(col)
    high, low = ka + kb, jnp.abs(ka - kb)
    odd = high & 1

    def slot(k):
        return jnp.where(valid, 6 * ((k + 1) >> 1) + 2 * kind + odd, 0)

    base = jnp.where(odd == 1, 7 + 2 * kind, 2 * kind)
    raw = jnp.broadcast_to(moments_ref[...], shape)

    def take(index):
        return jnp.take_along_axis(raw, index, axis=1)

    gram = jnp.where(valid, take(slot(high)) + take(slot(low)) - take(jnp.where(valid, base, 0)), 0.0)

    def lower(i):
        return jnp.where((i == 1) | (i == FIRST + 1), 1.0, jnp.where((i >= 1) & (i < FIELDS) & (i != FIRST), 0.5, 0.0))

    def upper(i):
        return jnp.where((i < FIELDS - 2) & (i != FIRST - 2) & (i != FIRST - 1), 0.5, 0.0)

    low_l, up_l = lower(col).astype(F32), upper(col).astype(F32)
    low_s, up_s = lower(row).astype(F32), upper(row).astype(F32)

    def shifted(v, axis):
        length = v.shape[axis]
        low_c, up_c = (low_s, up_s) if axis == 0 else (low_l, up_l)
        return v + low_c * pltpu.roll(v, 1, axis) + up_c * pltpu.roll(v, length - 1, axis)

    below = pltpu.roll(low_l, COLS - 1, 1)
    above = pltpu.roll(up_l, 1, 1)
    ends = (col == FIRST - 1) | (col == FIELDS - 1)
    gram_h = jnp.where(
        ends, 0.0,
        gram + below * pltpu.roll(gram, COLS - 1, 1) + jnp.where(col > 0, above, 0.0) * pltpu.roll(gram, 1, 1),
    )

    def form(matrix, left, right):
        return jnp.sum(matrix * left * right, keepdims=True)

    unit = lambda at: ((row == at).astype(F32), (col == at).astype(F32))
    p_s, p_l = unit(0)
    r_s, r_l = unit(FIRST)
    q_s, q_l = shifted(p_s, 0), shifted(p_l, 1)
    x_s = jnp.zeros(shape, F32)
    norm = form(gram, r_s, r_l)
    curvature = form(gram_h, p_s, p_l)
    for inner in range(STEPS):
        t = norm / curvature
        x_s = x_s + t * p_s
        r_s = r_s - t * q_s
        if inner == STEPS - 1:
            break
        r_l = r_l - t * q_l
        h_s, h_l = shifted(r_s, 0), shifted(r_l, 1)
        fresh = form(gram, r_s, r_l)
        own = form(gram_h, r_s, r_l)
        cross = form(gram_h, r_s, p_l)
        beta = fresh / norm
        curvature = own + beta * (2.0 * cross + beta * curvature)
        norm = fresh
        p_s, p_l = r_s + beta * p_s, r_l + beta * p_l
        q_s, q_l = h_s + beta * q_s, h_l + beta * q_l

    lane1 = lanes_of((1, COLS))
    search_half = within((lane1 + 32) & (COLS - 1), 14, 78)
    size = 32
    for coords, out_ref in ((x_s, height_ref), (r_s, residual_ref)):
        mixed = []
        for n in range(STEPS + 1):
            other = coords[FIRST + n : FIRST + n + 1, :] if n < STEPS else jnp.zeros((1, COLS), F32)
            mixed.append(jnp.where(search_half, coords[n : n + 1, :], other))
        for at in range(0, ROWS, size):
            rows = slice(16 + at, 16 + at + size)
            main = sum(coords[k : k + 1, :] * basis_ref[k, rows, :] for k in range(FIELDS))
            strip = sum(mixed[n] * strips_ref[n, rows, :] for n in range(STEPS + 1))
            strip = strip + shift(strip, 64)
            out_ref[at : at + size, :] = jnp.where(
                lane1 >= 119, strip, jnp.where(lane1 < 9, shift(strip, -WEST), main)
            )


def per_device(forcing, search, depth, mask, fold_map):
    made = basis_and_moments(forcing, search, depth, mask, fold_map)
    basis, strips, moments = (pltpu.with_memory_space_constraint(v, pltpu.VMEM) for v in made)
    block = jax.ShapeDtypeStruct((ROWS, COLS), F32)
    return pl.pallas_call(
        combine_kernel,
        out_shape=(block, block),
        in_specs=[pl.BlockSpec(memory_space=pltpu.VMEM)] * 3,
        name="combine",
    )(moments, basis, strips)


def solution(mesh):
    return jax.shard_map(
        per_device,
        mesh=mesh,
        in_specs=(P("lat", "lon"),) * 4 + (P(),),
        out_specs=(P("lat", "lon"),) * 2,
        check_vma=False,
    )
```

```python
import functools

import jax
import jax.numpy as jnp
from jax import lax
from jax.experimental import pallas as pl
from jax.experimental.pallas import tpu as pltpu
from jax.sharding import PartitionSpec as P

STEPS = 8
REACH = 256
LAT, LON, NX, NZ = 16, 32, 4, 8
ROWS, COLS = 160, 128
EXT = ROWS + 32
LO = 8
FIELDS = 2 * STEPS + 1
FIRST = STEPS + 1
HIGHEST = lax.Precision.HIGHEST
F32 = jnp.float32


def lanes_of(shape):
    return lax.broadcasted_iota(jnp.int32, shape, len(shape) - 1)


def from_east(x):
    return pltpu.roll(x, COLS - 1, 1)


def from_west(x):
    return pltpu.roll(x, 1, 1)


def shift(x, by):
    by %= COLS
    return pltpu.roll(x, by, 1) if by else x


WEST = 28


def strip_lanes(lane, half):
    lane = (lane - half) & (COLS - 1)
    return (lane >= 119) | ((lane >= WEST) & (lane < WEST + 9))


def within(lane, start, stop):
    return (lane >= start) & (lane < stop)


def remote(src, dst, send, recv, lat, lon):
    return pltpu.make_async_remote_copy(
        src_ref=src,
        dst_ref=dst,
        send_sem=send,
        recv_sem=recv,
        device_id={"lat": lat, "lon": lon},
        device_id_type=pl.DeviceIdType.MESH,
    )


CHUNK = 16


def far_first(count):
    return sorted(range(1, count), key=lambda d: (-min(d, count - d), d))


def chunks(start, stop):
    return [(r, min(CHUNK, stop - r)) for r in range(start, stop, CHUNK)]


def basis_kernel(
    fold_ref, forcing_ref, search_ref, depth_ref, mask_ref,
    b_m, b_s, moments_out,
    fold_buf, raw_m, side_depth, side_state, depth_buf, mask_buf, pack_w, pack_e, got_w, got_e, corner,
    fold_x, fold_src, fold_row, fold_send, fold_got,
    s_m, s_s, de_m, de_s, se_m, se_s,
    w_m, w_s, rows_acc, part, red_p, red_y,
    plane_sem, local_sem, halo_send, halo_recv, fz_send, fz_recv, fx_send, fx_recv,
    rp_send, rp_recv, ry_send, ry_recv,
):
    lat = lax.axis_index("lat")
    lon = lax.axis_index("lon")
    zi, xi = lon // NX, lon % NX
    core, yi = lat % 2, lat // 2
    top = lat == LAT - 1
    bottom = lat == 0
    north, south = (lat + 1) % LAT, (lat + LAT - 1) % LAT
    east, west = (lon + 1) % LON, (lon + LON - 1) % LON
    barrier = pltpu.get_barrier_semaphore()

    loads = [
        pltpu.make_async_copy(depth_ref, depth_buf, local_sem.at[0]),
        pltpu.make_async_copy(mask_ref, mask_buf, local_sem.at[1]),
        pltpu.make_async_copy(forcing_ref, raw_m.at[1, pl.ds(16, ROWS), :], local_sem.at[2]),
        pltpu.make_async_copy(search_ref, raw_m.at[2, pl.ds(16, ROWS), :], local_sem.at[3]),
        pltpu.make_async_copy(fold_ref.at[pl.ds(0, 1024)], fold_buf, local_sem.at[4]),
    ]
    for copy in loads:
        copy.start()

    def greet(semaphore, to):
        for a, b in to:
            pl.semaphore_signal(
                semaphore, inc=1, device_id={"lat": a, "lon": b}, device_id_type=pl.DeviceIdType.MESH
            )

    def around(far):
        if 2 * far == NZ:
            return [(lat, (lon + NX * far) % LON)]
        to = [(lat, (lon + NX * far) % LON), (lat, (lon + LON - NX * far) % LON)]
        if 2 * far < LAT:
            to += [((lat + 2 * far) % LAT, lon), ((lat + LAT - 2 * far) % LAT, lon)]
        return to

    beside = [(lat, zi * NX + (xi + d) % NX) for d in far_first(NX)]
    beside += [(north, east), (north, west), (south, east), (south, west)]
    beside += [(lat, east), (lat, west), (north, lon), (south, lon)] + around(1)

    beside += [(lat + 1 - 2 * core, zi * NX + (xi + d) % NX) for d in far_first(NX)]
    greet(barrier, beside)

    levels = 3

    def next_level(level):
        if level > 0:
            pl.semaphore_wait(plane_sem.at[level - 1], len(around(1 << (level - 1))))
        if level < levels:
            greet(plane_sem.at[level], around(1 << level))

    rows_acc[...] = jnp.zeros_like(rows_acc)
    for copy in loads:
        copy.wait()
    raw_m[0, 16 : 16 + ROWS, :] = depth_buf[...] * mask_buf[...].astype(F32)

    pivot = fold_buf[0]
    pivot_block, pivot_lane = lax.shift_right_logical(pivot, 7), pivot & (COLS - 1)

    @pl.when(top)
    def _():
        fold_x[...] = jnp.zeros_like(fold_x)
        for m in range(9):
            fold_x[m : m + 1, :] = raw_m[0, 175 - m : 176 - m, :]
        for m in range(8):
            fold_x[9 + m : 10 + m, :] = raw_m[1, 175 - m : 176 - m, :]
            fold_x[17 + m : 18 + m, :] = raw_m[2, 175 - m : 176 - m, :]
        source = lax.broadcasted_iota(jnp.int32, (COLS, COLS), 0)
        target = lax.broadcasted_iota(jnp.int32, (COLS, COLS), 1)
        choose = (source == ((pivot - target) & (COLS - 1))).astype(F32)
        turned = jnp.dot(fold_x[...], choose, precision=HIGHEST, preferred_element_type=F32)
        fold_src[...] = turned
        fold_row[xi] = turned
        fold_row[NX] = jnp.zeros_like(turned)

    lane40 = lanes_of((40, COLS))
    acc_w = jnp.zeros((40, COLS), F32)
    acc_e = jnp.zeros((40, COLS), F32)
    for g in range(4):
        for f in range(3):
            at = 32 * g + 9 * f
            block = raw_m[f, 16 + 40 * g : 56 + 40 * g, :]
            here = (lane40 >= at) & (lane40 < at + 9)
            acc_w = jnp.where(here, pltpu.roll(block, at, 1) if at else block, acc_w)
            acc_e = jnp.where(here, pltpu.roll(block, (at - 119) % COLS, 1), acc_e)
    pack_w[...] = acc_w
    pack_e[...] = acc_e

    pl.semaphore_wait(barrier, len(beside))

    fold_x_copies = [
        remote(fold_src, fold_row.at[xi], fx_send.at[d - 1], fx_recv.at[d - 1], lat, zi * NX + (xi + d) % NX)
        for d in range(1, NX)
    ]

    @pl.when(top)
    def _():
        for d in far_first(NX):
            fold_x_copies[d - 1].start()

    to_north = remote(raw_m.at[:, pl.ds(160, 16), :], raw_m.at[:, pl.ds(0, 16), :],
                      halo_send.at[0], halo_recv.at[0], north, lon)
    to_south = remote(raw_m.at[:, pl.ds(16, 16), :], raw_m.at[:, pl.ds(176, 16), :],
                      halo_send.at[1], halo_recv.at[1], south, lon)
    to_east = remote(pack_e, got_w, halo_send.at[2], halo_recv.at[2], lat, east)
    to_west = remote(pack_w, got_e, halo_send.at[3], halo_recv.at[3], lat, west)
    to_ne = remote(pack_e.at[pl.ds(24, 16), :], corner.at[0], halo_send.at[4], halo_recv.at[4], north, east)
    to_nw = remote(pack_w.at[pl.ds(24, 16), :], corner.at[1], halo_send.at[5], halo_recv.at[5], north, west)
    to_se = remote(pack_e.at[pl.ds(0, 16), :], corner.at[2], halo_send.at[6], halo_recv.at[6], south, east)
    to_sw = remote(pack_w.at[pl.ds(0, 16), :], corner.at[3], halo_send.at[7], halo_recv.at[7], south, west)

    to_east.start()
    to_west.start()
    next_level(0)

    @pl.when(jnp.logical_not(top))
    def _():
        to_ne.start()
        to_nw.start()
        to_north.start()

    @pl.when(jnp.logical_not(bottom))
    def _():
        to_se.start()
        to_sw.start()
        to_south.start()

    fold_z_copies = [
        remote(fold_send.at[d], fold_got.at[zi], fz_send.at[d - 1], fz_recv.at[d - 1],
               lat, ((zi + d) % NZ) * NX + xi)
        for d in range(1, NZ)
    ]
    lane32 = lanes_of((32, COLS))
    near = lane32 <= pivot_lane

    @pl.when(top)
    def _():
        next_level(1)
        next_level(2)
        for copy in fold_x_copies:
            copy.wait_recv()
        for d in far_first(NZ) + [0]:
            want = pivot_block - ((zi + d) % NZ) * NX - xi

            def block(b):
                mine = (lax.shift_right_logical(b & (LON - 1), 2) == zi)
                return fold_row[jnp.where(mine, b & (NX - 1), NX)]

            ahead, here, behind, beyond = (block(want + o) for o in (1, 0, -1, -2))
            window = jnp.where(near, here, behind)
            edge = jnp.where(
                lane32 < 9, jnp.where(near, behind, beyond),
                jnp.where(lane32 >= 119, jnp.where(near, ahead, here), 0.0),
            )
            edges = sum(pltpu.roll(edge[8 * g : 8 * g + 8], 16 + 32 * g, 1) for g in range(4))
            if d:
                fold_send[d, 0:32, :] = window
                fold_send[d, 32:40, :] = edges
            else:
                fold_got[zi, 0:32, :] = window
                fold_got[zi, 32:40, :] = edges
        for d in far_first(NZ):
            fold_z_copies[d - 1].start()

    def own_strips(spans):
        for r, n in spans:
            depth, residual, search = (raw_m[f, r : r + n, :] for f in range(3))
            lane = lanes_of((n, COLS))
            west_p, east_r, west_r = (within(lane, a, a + 18) for a in (WEST, 46, WEST + 64))
            east_p = lane >= 110
            for ref, p, q in ((side_depth, depth, depth), (side_state, search, residual)):
                ref[r : r + n, :] = jnp.where(
                    east_p, p, jnp.where(west_p, shift(p, WEST), jnp.where(
                        east_r, shift(q, 64), jnp.where(west_r, shift(q, WEST + 64), 0.0))))

    def far_strips(r, n, from_e, from_w, places):
        lane = lanes_of((n, COLS))
        west_p, east_r, west_r = (within(lane, a, a + 9) for a in (WEST - 9, 64, WEST + 55))
        east_p = lane < 9
        at_d, at_r, at_p = places
        for ref, p, q in ((side_depth, at_d, at_d), (side_state, at_p, at_r)):
            ref[r : r + n, :] = jnp.where(
                east_p, shift(from_e, -p), jnp.where(west_p, shift(from_w, WEST - 9 - p), jnp.where(
                    east_r, shift(from_e, 64 - q), jnp.where(
                        west_r, shift(from_w, WEST + 55 - q), ref[r : r + n, :]))))

    kinds = {
        "m": (raw_m.at[0], s_m, de_m, se_m, w_m),
        "s": (side_depth, s_s, de_s, se_s, w_s),
    }

    def fields(kind, spans):
        for r, n in spans:
            wet = (kinds[kind][0][r : r + n, :] > 0.0).astype(F32)
            if kind == "m":
                b_m[0, r : r + n, :] = wet * raw_m[2, r : r + n, :]
                b_m[FIRST, r : r + n, :] = wet * raw_m[1, r : r + n, :]
            else:
                b_s[0, r : r + n, :] = wet * side_state[r : r + n, :]

    def roots(kind, spans):
        depth_ref_, s, de, se, _ = kinds[kind]
        for r, n in spans:
            up, depth, low = (depth_ref_[r + o : r + o + n, :] for o in (1, 0, -1))
            both = up + low
            column = depth + 0.5 * both
            wet_up, wet, wet_low = ((v > 0.0).astype(F32) for v in (up, depth, low))
            both_wet = wet_up + wet_low
            column_wet = wet + 0.5 * both_wet
            all_depth = both + (from_east(column) + from_west(column))
            all_wet = both_wet + (from_east(column_wet) + from_west(column_wet))
            total = 0.5 * (depth * all_wet + all_depth)
            diagonal = wet * (depth * (1.0 / (REACH * REACH)) + total) + (1.0 - wet)
            root = wet * lax.rsqrt(diagonal)
            s[r : r + n, :] = root
            se[r : r + n, :] = from_east(root)
            de[r : r + n, :] = from_east(depth)

    def links(kind, spans):
        depth_ref_, s, de, se, w = kinds[kind]
        for r, n in spans:
            d0, d1 = depth_ref_[r : r + n, :], depth_ref_[r + 1 : r + 1 + n, :]
            s0, s1 = s[r : r + n, :], s[r + 1 : r + 1 + n, :]
            de0, de1 = de[r : r + n, :], de[r + 1 : r + 1 + n, :]
            se0, se1 = se[r : r + n, :], se[r + 1 : r + 1 + n, :]
            east_w = -(d0 + de0) * (s0 * se0)
            ne_w = -0.5 * (d0 + de1) * (s0 * se1)
            nw_e = -0.5 * (de0 + d1) * (se0 * s1)
            w[0, r : r + n, :] = -(d0 + d1) * (s0 * s1)
            w[1, r : r + n, :] = east_w
            w[2, r : r + n, :] = from_west(east_w)
            w[3, r : r + n, :] = ne_w
            w[4, r : r + n, :] = from_west(ne_w)
            w[5, r : r + n, :] = from_west(nw_e)
            w[6, r : r + n, :] = nw_e

    def fold8(x):
        return sum(x[8 * k : 8 * k + 8] for k in range(x.shape[0] // 8))

    lane1 = lanes_of((1, COLS))
    main_lanes = within(lane1, 9, 119)
    strips_p, strips_r = strip_lanes(lane1, 0), strip_lanes(lane1, 64)

    def apply(b, k, w, r, size):
        up, mid, low = (b[k, r + o : r + o + size, :] for o in (1, 0, -1))
        a_u, a_d, e_u, e_c, e_d, f_u, f_c, f_d = w
        east_part = from_east(e_u * up + e_c * mid + e_d * low)
        west_part = from_west(f_u * up + f_c * mid + f_d * low)
        return mid, (a_u * up + a_d * low) + (east_part + west_part)

    def step(n, tasks, first, last):
        total = {}

        def add(key, product, lo, hi):
            value = fold8(product[lo:hi])
            total[key] = total[key] + value if key in total else value

        for kind, r, size, gram_lo, gram_hi in tasks:
            w = kinds[kind][4]
            weights = (
                w[0, r : r + size, :], w[0, r - 1 : r - 1 + size, :],
                w[4, r : r + size, :], w[2, r : r + size, :], w[5, r - 1 : r - 1 + size, :],
                w[6, r : r + size, :], w[1, r : r + size, :], w[3, r - 1 : r - 1 + size, :],
            )
            b, bases = (b_s, (0,)) if kind == "s" else (b_m, (0,) if last else (0, FIRST))
            news, olds = [], []
            for base in bases:
                mid, out = apply(b, base + n - 1, weights, r, size)
                out = 0.5 * out if first else out - b[base + n - 2, r : r + size, :]
                b[base + n, r : r + size, :] = out
                news.append(out)
                olds.append(mid)
            lo, hi = max(r, gram_lo) - r, min(r + size, gram_hi) - r
            if hi <= lo:
                continue
            p1, p0 = news[0], olds[0]
            if kind == "s":
                add("s0", p1 * p1, lo, hi)
                add("s1", p1 * p0, lo, hi)
                add("s4", p1 * shift(p1, 64), lo, hi)
                add("s5", p1 * shift(p0, 64), lo, hi)
                continue
            add("m0", p1 * p1, lo, hi)
            add("m1", p1 * p0, lo, hi)
            if last:
                r0 = b_m[FIRST + STEPS - 1, r : r + size, :]
            else:
                r1, r0 = news[1], olds[1]
                add("m2", r1 * r1, lo, hi)
                add("m3", r1 * r0, lo, hi)
                add("m4", p1 * r1, lo, hi)
            add("m5", p1 * r0, lo, hi)
        gather(n, total)

    def gather(n, total):
        rows = {key: jnp.sum(value, axis=0, keepdims=True) for key, value in total.items()}
        for c in range(6):
            row = jnp.zeros((1, COLS), F32)
            if "m%d" % c in rows:
                row = jnp.where(main_lanes, rows["m%d" % c], row)
            source = "s%d" % (c - 2 if c in (2, 3) else c)
            if source in rows:
                row = row + jnp.where(strips_r if c in (2, 3) else strips_p, rows[source], 0.0)
            at = pl.ds(6 * n + c, 1)
            rows_acc[at, :] = rows_acc[at, :] + row

    def steps(tasks):
        step(1, tasks, True, False)

        @pl.loop(2, STEPS)
        def _(n):
            step(n, tasks, False, False)

        step(STEPS, tasks, False, True)

    def tasks(kind, start, stop, gram_lo, gram_hi):
        return [(kind, r, n, gram_lo, gram_hi) for r, n in chunks(start, stop)]

    own_strips(chunks(16, 176))
    fields("m", chunks(16, 176))
    roots("m", [(17, 7)] + chunks(24, 168) + [(168, 7)])
    links("m", chunks(16, 168))

    @pl.when(jnp.logical_not(top))
    def _():
        next_level(1)

    start = {}
    for r, n in chunks(16, 176):
        p0, r0 = b_m[0, r : r + n, :], b_m[FIRST, r : r + n, :]
        for key, value in (("m0", p0 * p0), ("m2", r0 * r0), ("m4", p0 * r0)):
            start[key] = start[key] + fold8(value) if key in start else fold8(value)
    gather(0, start)

    @pl.when(jnp.logical_not(top))
    def _():
        next_level(2)

    steps(tasks("m", 16, 168, 32, 160))

    to_east.wait()
    to_west.wait()
    for g in range(4):
        at = 32 * g
        far_strips(16 + 40 * g, 40, got_e[...], got_w[...], (at, at + 9, at + 18))
    fields("s", chunks(16, 176))
    start = {}
    for r, n in chunks(16, 176):
        p0 = b_s[0, r : r + n, :]
        for key, value in (("s0", p0 * p0), ("s4", p0 * shift(p0, 64))):
            start[key] = start[key] + fold8(value) if key in start else fold8(value)
    gather(0, start)

    roots("s", [(17, 7)] + chunks(24, 168) + [(168, 7)])
    links("s", chunks(16, 168))
    steps(tasks("s", 16, 168, 32, 160))

    @pl.when(jnp.logical_not(bottom))
    def _():
        to_se.wait_send()
        to_sw.wait_send()
        to_south.wait_send()
        to_ne.wait_recv()
        to_nw.wait_recv()
        to_north.wait_recv()
        own_strips([(0, 16)])
        far_strips(0, 16, corner[1], corner[0], (96, 105, 114))

    @pl.when(bottom)
    def _():
        for f in range(3):
            raw_m[f, 0:16, :] = jnp.zeros((16, COLS), F32)
        side_depth[0:16, :] = jnp.zeros((16, COLS), F32)
        side_state[0:16, :] = jnp.zeros((16, COLS), F32)

    @pl.when(jnp.logical_not(top))
    def _():
        to_ne.wait_send()
        to_nw.wait_send()
        to_north.wait_send()
        to_se.wait_recv()
        to_sw.wait_recv()
        to_south.wait_recv()
        own_strips([(176, 16)])
        far_strips(176, 16, corner[3], corner[2], (0, 9, 18))

    @pl.when(top)
    def _():
        for copy in fold_z_copies:
            copy.wait_recv()
        ghost = fold_got[0]
        for k in range(1, NZ):
            ghost = ghost + fold_got[k]
        edges = ghost[32:40]
        lane8 = lanes_of((8, COLS))
        side = []
        for g in range(4):
            edge = pltpu.roll(edges, (COLS - 16 - 32 * g) % COLS, 1)
            side.append(jnp.where((lane8 < 9) | (lane8 >= 119), edge, 0.0))
        side = jnp.concatenate(side, axis=0)
        for f in range(3):
            raw_m[f, 176:192, :] = jnp.zeros((16, COLS), F32)
        raw_m[0, 176:185, :] = ghost[0:9]
        raw_m[1, 176:184, :] = ghost[9:17]
        raw_m[2, 176:184, :] = ghost[17:25]
        own_strips([(176, 16)])
        fold_x[...] = side
        west_p, west_r, east_r = (within(lane1, a, a + 9) for a in (WEST - 9, WEST + 55, 64))
        for ref, p, q, count in ((side_depth, 0, 0, 9), (side_state, 17, 9, 8)):
            one, two = fold_x[p : p + count, :], fold_x[q : q + count, :]
            ref[176 : 176 + count, :] = jnp.where(
                lane1 < 9, one, jnp.where(west_p, shift(one, WEST), jnp.where(
                    east_r, shift(two, 64), jnp.where(
                        west_r, shift(two, WEST + 64), ref[176 : 176 + count, :]))))
        for copy in fold_x_copies + fold_z_copies:
            copy.wait_send()

    for kind in ("m", "s"):
        fields(kind, [(LO, 8), (176, 8)])
        roots(kind, [(LO, 16), (168, 16)])
        links(kind, [(LO, 16), (168, 16)])
    steps([(kind, r, 24, lo, lo + 16) for kind in ("m", "s") for r, lo in ((LO, 16), (160, 160))])

    ones = jnp.ones((8, COLS), F32)
    sums = lax.dot_general(
        ones, rows_acc[...], (((1,), (1,)), ((), ())), precision=HIGHEST, preferred_element_type=F32
    )[0:1]

    def tree(terms):
        while len(terms) > 1:
            terms = [a + b for a, b in zip(terms[::2], terms[1::2])]
        return terms[0]

    second = core == 1
    part[0] = sums
    next_level(levels)
    to_plane = [
        remote(part.at[0], red_p.at[core * LON + lon], rp_send.at[d], rp_recv.at[core * LON + d],
               2 * yi + 1, (lon + d) % LON)
        for d in range(LON)
    ]
    for d in far_first(LON):
        to_plane[d].start()
    count = LAT // 2
    along_y = [(d, c) for d in far_first(count) + [0] for c in (1, 0) if (d, c) != (0, 1)]
    to_lat = [
        remote(part.at[1], red_y.at[yi], ry_send.at[2 * d + c], ry_recv.at[d],
               2 * ((yi + d) % count) + c, lon)
        for d, c in along_y
    ]

    @pl.when(jnp.logical_not(second))
    def _():
        to_plane[0].start()
        to_plane[0].wait_send()

    @pl.when(second)
    def _():
        red_p[LON + lon] = sums
        for c in range(2):
            for d in range(c, LON):
                remote(part.at[0], red_p.at[c * LON + lon], rp_send.at[d], rp_recv.at[c * LON + d],
                       lat, east).wait_recv()
        total = tree([red_p[k] for k in range(2 * LON)])
        part[1] = total
        red_y[yi] = total
        for copy in to_lat:
            copy.start()

    def arrived(d):
        remote(part.at[1], red_y.at[yi], ry_send.at[0], ry_recv.at[d], lat, east).wait_recv()

    @pl.when(jnp.logical_not(second))
    def _():
        arrived(0)

    for d in range(1, count):
        arrived(d)
    moments_out[...] = tree([red_y[k] for k in range(count)])

    @pl.when(second)
    def _():
        for copy in to_lat:
            copy.wait_send()

    for copy in to_plane[1:]:
        copy.wait_send()


def held(shape):
    return pltpu.VMEM(shape, F32)


def basis_and_moments(forcing, search, depth, mask, fold_map):
    vm = pltpu.VMEM
    dma = pltpu.SemaphoreType.DMA
    ext = (EXT, COLS)
    return pl.pallas_call(
        basis_kernel,
        out_shape=(held((FIELDS,) + ext), held((STEPS + 1,) + ext), held((1, COLS))),
        in_specs=[pl.BlockSpec(memory_space=pl.ANY)] * 5,
        out_specs=(pl.BlockSpec(memory_space=vm),) * 3,
        scratch_shapes=[
            pltpu.SMEM((1024,), jnp.int32),
            vm((3,) + ext, F32), vm(ext, F32), vm(ext, F32),
            vm((ROWS, COLS), F32), vm((ROWS, COLS), jnp.int32),
            vm((40, COLS), F32), vm((40, COLS), F32), vm((40, COLS), F32), vm((40, COLS), F32),
            vm((4, 16, COLS), F32),
            vm((32, COLS), F32), vm((32, COLS), F32), vm((NX + 1, 32, COLS), F32),
            vm((NZ, 40, COLS), F32), vm((NZ, 40, COLS), F32),
        ]
        + [vm(ext, F32)] * 6
        + [vm((7,) + ext, F32)] * 2
        + [
            vm((COLS, COLS), F32), vm((2, 1, COLS), F32),
            vm((2 * LON, 1, COLS), F32), vm((LAT // 2, 1, COLS), F32),
            pltpu.SemaphoreType.REGULAR((4,)), dma((5,)), dma((8,)), dma((8,)),
            dma((NZ - 1,)), dma((NZ - 1,)), dma((NX - 1,)), dma((NX - 1,)),
            dma((LON,)), dma((2 * LON,)), dma((LAT,)), dma((LAT // 2,)),
        ],
        compiler_params=pltpu.CompilerParams(collective_id=0, has_side_effects=True),
        name="basis",
    )(fold_map, forcing, search, depth, mask)


def combine_kernel(moments_ref, basis_ref, strips_ref, height_ref, residual_ref):
    shape = (24, COLS)
    row = lax.broadcasted_iota(jnp.int32, shape, 0)
    col = lanes_of(shape)

    def power(i):
        return jnp.where(i >= FIRST, i - FIRST, i)

    kind = jnp.where((row >= FIRST) & (col >= FIRST), 1, jnp.where((row >= FIRST) | (col >= FIRST), 2, 0))
    valid = (row < FIELDS) & (col < FIELDS)
    ka, kb = power(row), power(col)
    high, low = ka + kb, jnp.abs(ka - kb)
    odd = high & 1

    def slot(k):
        return jnp.where(valid, 6 * ((k + 1) >> 1) + 2 * kind + odd, 0)

    base = jnp.where(odd == 1, 7 + 2 * kind, 2 * kind)
    raw = jnp.broadcast_to(moments_ref[...], shape)

    def take(index):
        return jnp.take_along_axis(raw, index, axis=1)

    gram = jnp.where(valid, take(slot(high)) + take(slot(low)) - take(jnp.where(valid, base, 0)), 0.0)

    def lower(i):
        return jnp.where((i == 1) | (i == FIRST + 1), 1.0, jnp.where((i >= 1) & (i < FIELDS) & (i != FIRST), 0.5, 0.0))

    def upper(i):
        return jnp.where((i < FIELDS - 2) & (i != FIRST - 2) & (i != FIRST - 1), 0.5, 0.0)

    low_l, up_l = lower(col).astype(F32), upper(col).astype(F32)
    low_s, up_s = lower(row).astype(F32), upper(row).astype(F32)

    def shifted(v, axis):
        length = v.shape[axis]
        low_c, up_c = (low_s, up_s) if axis == 0 else (low_l, up_l)
        return v + low_c * pltpu.roll(v, 1, axis) + up_c * pltpu.roll(v, length - 1, axis)

    below = pltpu.roll(low_l, COLS - 1, 1)
    above = pltpu.roll(up_l, 1, 1)
    ends = (col == FIRST - 1) | (col == FIELDS - 1)
    gram_h = jnp.where(
        ends, 0.0,
        gram + below * pltpu.roll(gram, COLS - 1, 1) + jnp.where(col > 0, above, 0.0) * pltpu.roll(gram, 1, 1),
    )

    def form(matrix, left, right):
        return jnp.sum(matrix * left * right, keepdims=True)

    unit = lambda at: ((row == at).astype(F32), (col == at).astype(F32))
    p_s, p_l = unit(0)
    r_s, r_l = unit(FIRST)
    q_s, q_l = shifted(p_s, 0), shifted(p_l, 1)
    x_s = jnp.zeros(shape, F32)
    norm = form(gram, r_s, r_l)
    curvature = form(gram_h, p_s, p_l)
    for inner in range(STEPS):
        t = norm / curvature
        x_s = x_s + t * p_s
        r_s = r_s - t * q_s
        if inner == STEPS - 1:
            break
        r_l = r_l - t * q_l
        h_s, h_l = shifted(r_s, 0), shifted(r_l, 1)
        fresh = form(gram, r_s, r_l)
        own = form(gram_h, r_s, r_l)
        cross = form(gram_h, r_s, p_l)
        beta = fresh / norm
        curvature = own + beta * (2.0 * cross + beta * curvature)
        norm = fresh
        p_s, p_l = r_s + beta * p_s, r_l + beta * p_l
        q_s, q_l = h_s + beta * q_s, h_l + beta * q_l

    lane1 = lanes_of((1, COLS))
    search_half = within((lane1 + 32) & (COLS - 1), 14, 78)
    size = 32
    for coords, out_ref in ((x_s, height_ref), (r_s, residual_ref)):
        mixed = []
        for n in range(STEPS + 1):
            other = coords[FIRST + n : FIRST + n + 1, :] if n < STEPS else jnp.zeros((1, COLS), F32)
            mixed.append(jnp.where(search_half, coords[n : n + 1, :], other))
        for at in range(0, ROWS, size):
            rows = slice(16 + at, 16 + at + size)
            main = sum(coords[k : k + 1, :] * basis_ref[k, rows, :] for k in range(FIELDS))
            strip = sum(mixed[n] * strips_ref[n, rows, :] for n in range(STEPS + 1))
            strip = strip + shift(strip, 64)
            out_ref[at : at + size, :] = jnp.where(
                lane1 >= 119, strip, jnp.where(lane1 < 9, shift(strip, -WEST), main)
            )


def per_device(forcing, search, depth, mask, fold_map):
    made = basis_and_moments(forcing, search, depth, mask, fold_map)
    basis, strips, moments = (pltpu.with_memory_space_constraint(v, pltpu.VMEM) for v in made)
    block = jax.ShapeDtypeStruct((ROWS, COLS), F32)
    return pl.pallas_call(
        combine_kernel,
        out_shape=(block, block),
        in_specs=[pl.BlockSpec(memory_space=pltpu.VMEM)] * 3,
        name="combine",
    )(moments, basis, strips)


def solution(mesh):
    return jax.shard_map(
        per_device,
        mesh=mesh,
        in_specs=(P("lat", "lon"),) * 4 + (P(),),
        out_specs=(P("lat", "lon"),) * 2,
        check_vma=False,
    )
```

```python
import functools

import jax
import jax.numpy as jnp
from jax import lax
from jax.experimental import pallas as pl
from jax.experimental.pallas import tpu as pltpu
from jax.sharding import PartitionSpec as P

STEPS = 8
REACH = 256
LAT, LON, NX, NZ = 16, 32, 4, 8
ROWS, COLS = 160, 128
EXT = ROWS + 32
LO = 8
FIELDS = 2 * STEPS + 1
FIRST = STEPS + 1
HIGHEST = lax.Precision.HIGHEST
F32 = jnp.float32


def lanes_of(shape):
    return lax.broadcasted_iota(jnp.int32, shape, len(shape) - 1)


def from_east(x):
    return pltpu.roll(x, COLS - 1, 1)


def from_west(x):
    return pltpu.roll(x, 1, 1)


def shift(x, by):
    by %= COLS
    return pltpu.roll(x, by, 1) if by else x


WEST = 28


def strip_lanes(lane, half):
    lane = (lane - half) & (COLS - 1)
    return (lane >= 119) | ((lane >= WEST) & (lane < WEST + 9))


def within(lane, start, stop):
    return (lane >= start) & (lane < stop)


def remote(src, dst, send, recv, lat, lon):
    return pltpu.make_async_remote_copy(
        src_ref=src,
        dst_ref=dst,
        send_sem=send,
        recv_sem=recv,
        device_id={"lat": lat, "lon": lon},
        device_id_type=pl.DeviceIdType.MESH,
    )


CHUNK = 16


def far_first(count):
    return sorted(range(1, count), key=lambda d: (-min(d, count - d), d))


def chunks(start, stop):
    return [(r, min(CHUNK, stop - r)) for r in range(start, stop, CHUNK)]


def basis_kernel(
    fold_ref, forcing_ref, search_ref, depth_ref, mask_ref,
    b_m, b_s, moments_out,
    fold_buf, raw_m, side_depth, side_state, depth_buf, mask_buf, pack_w, pack_e, got_w, got_e, corner,
    fold_x, fold_src, fold_row, fold_send, fold_got,
    s_m, s_s, de_m, de_s, se_m, se_s,
    w_m, w_s, rows_acc, part, red_p, red_y,
    plane_sem, local_sem, halo_send, halo_recv, fz_send, fz_recv, fx_send, fx_recv,
    rp_send, rp_recv, ry_send, ry_recv,
):
    lat = lax.axis_index("lat")
    lon = lax.axis_index("lon")
    zi, xi = lon // NX, lon % NX
    core, yi = lat % 2, lat // 2
    top = lat == LAT - 1
    bottom = lat == 0
    north, south = (lat + 1) % LAT, (lat + LAT - 1) % LAT
    east, west = (lon + 1) % LON, (lon + LON - 1) % LON
    barrier = pltpu.get_barrier_semaphore()

    loads = [
        pltpu.make_async_copy(depth_ref, depth_buf, local_sem.at[0]),
        pltpu.make_async_copy(mask_ref, mask_buf, local_sem.at[1]),
        pltpu.make_async_copy(forcing_ref, raw_m.at[1, pl.ds(16, ROWS), :], local_sem.at[2]),
        pltpu.make_async_copy(search_ref, raw_m.at[2, pl.ds(16, ROWS), :], local_sem.at[3]),
        pltpu.make_async_copy(fold_ref.at[pl.ds(0, 1024)], fold_buf, local_sem.at[4]),
    ]
    for copy in loads:
        copy.start()

    def greet(semaphore, to):
        for a, b in to:
            pl.semaphore_signal(
                semaphore, inc=1, device_id={"lat": a, "lon": b}, device_id_type=pl.DeviceIdType.MESH
            )

    def around(far):
        if 2 * far == NZ:
            return [(lat, (lon + NX * far) % LON)]
        to = [(lat, (lon + NX * far) % LON), (lat, (lon + LON - NX * far) % LON)]
        if 2 * far < LAT:
            to += [((lat + 2 * far) % LAT, lon), ((lat + LAT - 2 * far) % LAT, lon)]
        return to

    beside = [(lat, zi * NX + (xi + d) % NX) for d in far_first(NX)]
    beside += [(north, east), (north, west), (south, east), (south, west)]
    beside += [(lat, east), (lat, west), (north, lon), (south, lon)] + around(1)

    beside += [(lat + 1 - 2 * core, zi * NX + (xi + d) % NX) for d in far_first(NX)]
    greet(barrier, beside)

    levels = 3

    def next_level(level):
        if level > 0:
            pl.semaphore_wait(plane_sem.at[level - 1], len(around(1 << (level - 1))))
        if level < levels:
            greet(plane_sem.at[level], around(1 << level))

    rows_acc[...] = jnp.zeros_like(rows_acc)
    for copy in loads:
        copy.wait()
    raw_m[0, 16 : 16 + ROWS, :] = depth_buf[...] * mask_buf[...].astype(F32)

    pivot = fold_buf[0]
    pivot_block, pivot_lane = lax.shift_right_logical(pivot, 7), pivot & (COLS - 1)

    @pl.when(top)
    def _():
        fold_x[...] = jnp.zeros_like(fold_x)
        for m in range(9):
            fold_x[m : m + 1, :] = raw_m[0, 175 - m : 176 - m, :]
        for m in range(8):
            fold_x[9 + m : 10 + m, :] = raw_m[1, 175 - m : 176 - m, :]
            fold_x[17 + m : 18 + m, :] = raw_m[2, 175 - m : 176 - m, :]
        source = lax.broadcasted_iota(jnp.int32, (COLS, COLS), 0)
        target = lax.broadcasted_iota(jnp.int32, (COLS, COLS), 1)
        choose = (source == ((pivot - target) & (COLS - 1))).astype(F32)
        turned = jnp.dot(fold_x[...], choose, precision=HIGHEST, preferred_element_type=F32)
        fold_src[...] = turned
        fold_row[xi] = turned
        fold_row[NX] = jnp.zeros_like(turned)

    lane40 = lanes_of((40, COLS))
    acc_w = jnp.zeros((40, COLS), F32)
    acc_e = jnp.zeros((40, COLS), F32)
    for g in range(4):
        for f in range(3):
            at = 32 * g + 9 * f
            block = raw_m[f, 16 + 40 * g : 56 + 40 * g, :]
            here = (lane40 >= at) & (lane40 < at + 9)
            acc_w = jnp.where(here, pltpu.roll(block, at, 1) if at else block, acc_w)
            acc_e = jnp.where(here, pltpu.roll(block, (at - 119) % COLS, 1), acc_e)
    pack_w[...] = acc_w
    pack_e[...] = acc_e

    pl.semaphore_wait(barrier, len(beside))

    fold_x_copies = [
        remote(fold_src, fold_row.at[xi], fx_send.at[d - 1], fx_recv.at[d - 1], lat, zi * NX + (xi + d) % NX)
        for d in range(1, NX)
    ]

    @pl.when(top)
    def _():
        for d in far_first(NX):
            fold_x_copies[d - 1].start()

    to_north = remote(raw_m.at[:, pl.ds(160, 16), :], raw_m.at[:, pl.ds(0, 16), :],
                      halo_send.at[0], halo_recv.at[0], north, lon)
    to_south = remote(raw_m.at[:, pl.ds(16, 16), :], raw_m.at[:, pl.ds(176, 16), :],
                      halo_send.at[1], halo_recv.at[1], south, lon)
    to_east = remote(pack_e, got_w, halo_send.at[2], halo_recv.at[2], lat, east)
    to_west = remote(pack_w, got_e, halo_send.at[3], halo_recv.at[3], lat, west)
    to_ne = remote(pack_e.at[pl.ds(24, 16), :], corner.at[0], halo_send.at[4], halo_recv.at[4], north, east)
    to_nw = remote(pack_w.at[pl.ds(24, 16), :], corner.at[1], halo_send.at[5], halo_recv.at[5], north, west)
    to_se = remote(pack_e.at[pl.ds(0, 16), :], corner.at[2], halo_send.at[6], halo_recv.at[6], south, east)
    to_sw = remote(pack_w.at[pl.ds(0, 16), :], corner.at[3], halo_send.at[7], halo_recv.at[7], south, west)

    to_east.start()
    to_west.start()
    next_level(0)

    @pl.when(jnp.logical_not(top))
    def _():
        to_ne.start()
        to_nw.start()
        to_north.start()

    @pl.when(jnp.logical_not(bottom))
    def _():
        to_se.start()
        to_sw.start()
        to_south.start()

    fold_z_copies = [
        remote(fold_send.at[d], fold_got.at[zi], fz_send.at[d - 1], fz_recv.at[d - 1],
               lat, ((zi + d) % NZ) * NX + xi)
        for d in range(1, NZ)
    ]
    lane32 = lanes_of((32, COLS))
    near = lane32 <= pivot_lane

    @pl.when(top)
    def _():
        next_level(1)
        next_level(2)
        for copy in fold_x_copies:
            copy.wait_recv()
        for d in far_first(NZ) + [0]:
            want = pivot_block - ((zi + d) % NZ) * NX - xi

            def block(b):
                mine = (lax.shift_right_logical(b & (LON - 1), 2) == zi)
                return fold_row[jnp.where(mine, b & (NX - 1), NX)]

            ahead, here, behind, beyond = (block(want + o) for o in (1, 0, -1, -2))
            window = jnp.where(near, here, behind)
            edge = jnp.where(
                lane32 < 9, jnp.where(near, behind, beyond),
                jnp.where(lane32 >= 119, jnp.where(near, ahead, here), 0.0),
            )
            edges = sum(pltpu.roll(edge[8 * g : 8 * g + 8], 16 + 32 * g, 1) for g in range(4))
            if d:
                fold_send[d, 0:32, :] = window
                fold_send[d, 32:40, :] = edges
            else:
                fold_got[zi, 0:32, :] = window
                fold_got[zi, 32:40, :] = edges
        for d in far_first(NZ):
            fold_z_copies[d - 1].start()

    def own_strips(spans):
        for r, n in spans:
            depth, residual, search = (raw_m[f, r : r + n, :] for f in range(3))
            lane = lanes_of((n, COLS))
            west_p, east_r, west_r = (within(lane, a, a + 18) for a in (WEST, 46, WEST + 64))
            east_p = lane >= 110
            for ref, p, q in ((side_depth, depth, depth), (side_state, search, residual)):
                ref[r : r + n, :] = jnp.where(
                    east_p, p, jnp.where(west_p, shift(p, WEST), jnp.where(
                        east_r, shift(q, 64), jnp.where(west_r, shift(q, WEST + 64), 0.0))))

    def far_strips(r, n, from_e, from_w, places):
        lane = lanes_of((n, COLS))
        west_p, east_r, west_r = (within(lane, a, a + 9) for a in (WEST - 9, 64, WEST + 55))
        east_p = lane < 9
        at_d, at_r, at_p = places
        for ref, p, q in ((side_depth, at_d, at_d), (side_state, at_p, at_r)):
            ref[r : r + n, :] = jnp.where(
                east_p, shift(from_e, -p), jnp.where(west_p, shift(from_w, WEST - 9 - p), jnp.where(
                    east_r, shift(from_e, 64 - q), jnp.where(
                        west_r, shift(from_w, WEST + 55 - q), ref[r : r + n, :]))))

    kinds = {
        "m": (raw_m.at[0], s_m, de_m, se_m, w_m),
        "s": (side_depth, s_s, de_s, se_s, w_s),
    }

    def fields(kind, spans):
        for r, n in spans:
            wet = (kinds[kind][0][r : r + n, :] > 0.0).astype(F32)
            if kind == "m":
                b_m[0, r : r + n, :] = wet * raw_m[2, r : r + n, :]
                b_m[FIRST, r : r + n, :] = wet * raw_m[1, r : r + n, :]
            else:
                b_s[0, r : r + n, :] = wet * side_state[r : r + n, :]

    def roots(kind, spans):
        depth_ref_, s, de, se, _ = kinds[kind]
        for r, n in spans:
            up, depth, low = (depth_ref_[r + o : r + o + n, :] for o in (1, 0, -1))
            both = up + low
            column = depth + 0.5 * both
            wet_up, wet, wet_low = ((v > 0.0).astype(F32) for v in (up, depth, low))
            both_wet = wet_up + wet_low
            column_wet = wet + 0.5 * both_wet
            all_depth = both + (from_east(column) + from_west(column))
            all_wet = both_wet + (from_east(column_wet) + from_west(column_wet))
            total = 0.5 * (depth * all_wet + all_depth)
            diagonal = wet * (depth * (1.0 / (REACH * REACH)) + total) + (1.0 - wet)
            root = wet * lax.rsqrt(diagonal)
            s[r : r + n, :] = root
            se[r : r + n, :] = from_east(root)
            de[r : r + n, :] = from_east(depth)

    def links(kind, spans):
        depth_ref_, s, de, se, w = kinds[kind]
        for r, n in spans:
            d0, d1 = depth_ref_[r : r + n, :], depth_ref_[r + 1 : r + 1 + n, :]
            s0, s1 = s[r : r + n, :], s[r + 1 : r + 1 + n, :]
            de0, de1 = de[r : r + n, :], de[r + 1 : r + 1 + n, :]
            se0, se1 = se[r : r + n, :], se[r + 1 : r + 1 + n, :]
            east_w = -(d0 + de0) * (s0 * se0)
            ne_w = -0.5 * (d0 + de1) * (s0 * se1)
            nw_e = -0.5 * (de0 + d1) * (se0 * s1)
            w[0, r : r + n, :] = -(d0 + d1) * (s0 * s1)
            w[1, r : r + n, :] = east_w
            w[2, r : r + n, :] = from_west(east_w)
            w[3, r : r + n, :] = ne_w
            w[4, r : r + n, :] = from_west(ne_w)
            w[5, r : r + n, :] = from_west(nw_e)
            w[6, r : r + n, :] = nw_e

    def fold8(x):
        return sum(x[8 * k : 8 * k + 8] for k in range(x.shape[0] // 8))

    lane1 = lanes_of((1, COLS))
    main_lanes = within(lane1, 9, 119)
    strips_p, strips_r = strip_lanes(lane1, 0), strip_lanes(lane1, 64)

    def apply(b, k, w, r, size):
        up, mid, low = (b[k, r + o : r + o + size, :] for o in (1, 0, -1))
        a_u, a_d, e_u, e_c, e_d, f_u, f_c, f_d = w
        east_part = from_east(e_u * up + e_c * mid + e_d * low)
        west_part = from_west(f_u * up + f_c * mid + f_d * low)
        return mid, (a_u * up + a_d * low) + (east_part + west_part)

    def step(n, tasks, first, last):
        total = {}

        def add(key, product, lo, hi):
            value = fold8(product[lo:hi])
            total[key] = total[key] + value if key in total else value

        for kind, r, size, gram_lo, gram_hi in tasks:
            w = kinds[kind][4]
            weights = (
                w[0, r : r + size, :], w[0, r - 1 : r - 1 + size, :],
                w[4, r : r + size, :], w[2, r : r + size, :], w[5, r - 1 : r - 1 + size, :],
                w[6, r : r + size, :], w[1, r : r + size, :], w[3, r - 1 : r - 1 + size, :],
            )
            b, bases = (b_s, (0,)) if kind == "s" else (b_m, (0,) if last else (0, FIRST))
            news, olds = [], []
            for base in bases:
                mid, out = apply(b, base + n - 1, weights, r, size)
                out = 0.5 * out if first else out - b[base + n - 2, r : r + size, :]
                b[base + n, r : r + size, :] = out
                news.append(out)
                olds.append(mid)
            lo, hi = max(r, gram_lo) - r, min(r + size, gram_hi) - r
            if hi <= lo:
                continue
            p1, p0 = news[0], olds[0]
            if kind == "s":
                add("s0", p1 * p1, lo, hi)
                add("s1", p1 * p0, lo, hi)
                add("s4", p1 * shift(p1, 64), lo, hi)
                add("s5", p1 * shift(p0, 64), lo, hi)
                continue
            add("m0", p1 * p1, lo, hi)
            add("m1", p1 * p0, lo, hi)
            if last:
                r0 = b_m[FIRST + STEPS - 1, r : r + size, :]
            else:
                r1, r0 = news[1], olds[1]
                add("m2", r1 * r1, lo, hi)
                add("m3", r1 * r0, lo, hi)
                add("m4", p1 * r1, lo, hi)
            add("m5", p1 * r0, lo, hi)
        gather(n, total)

    def gather(n, total):
        rows = {key: jnp.sum(value, axis=0, keepdims=True) for key, value in total.items()}
        for c in range(6):
            row = jnp.zeros((1, COLS), F32)
            if "m%d" % c in rows:
                row = jnp.where(main_lanes, rows["m%d" % c], row)
            source = "s%d" % (c - 2 if c in (2, 3) else c)
            if source in rows:
                row = row + jnp.where(strips_r if c in (2, 3) else strips_p, rows[source], 0.0)
            at = pl.ds(6 * n + c, 1)
            rows_acc[at, :] = rows_acc[at, :] + row

    def steps(tasks):
        step(1, tasks, True, False)

        @pl.loop(2, STEPS)
        def _(n):
            step(n, tasks, False, False)

        step(STEPS, tasks, False, True)

    def tasks(kind, start, stop, gram_lo, gram_hi):
        return [(kind, r, n, gram_lo, gram_hi) for r, n in chunks(start, stop)]

    own_strips(chunks(16, 176))
    fields("m", chunks(16, 176))
    roots("m", [(17, 7)] + chunks(24, 168) + [(168, 7)])
    links("m", chunks(16, 168))

    @pl.when(jnp.logical_not(top))
    def _():
        next_level(1)

    start = {}
    for r, n in chunks(16, 176):
        p0, r0 = b_m[0, r : r + n, :], b_m[FIRST, r : r + n, :]
        for key, value in (("m0", p0 * p0), ("m2", r0 * r0), ("m4", p0 * r0)):
            start[key] = start[key] + fold8(value) if key in start else fold8(value)
    gather(0, start)

    @pl.when(jnp.logical_not(top))
    def _():
        next_level(2)

    steps(tasks("m", 16, 168, 32, 160))

    to_east.wait()
    to_west.wait()
    for g in range(4):
        at = 32 * g
        far_strips(16 + 40 * g, 40, got_e[...], got_w[...], (at, at + 9, at + 18))
    fields("s", chunks(16, 176))
    start = {}
    for r, n in chunks(16, 176):
        p0 = b_s[0, r : r + n, :]
        for key, value in (("s0", p0 * p0), ("s4", p0 * shift(p0, 64))):
            start[key] = start[key] + fold8(value) if key in start else fold8(value)
    gather(0, start)

    roots("s", [(17, 7)] + chunks(24, 168) + [(168, 7)])
    links("s", chunks(16, 168))
    steps(tasks("s", 16, 168, 32, 160))

    @pl.when(jnp.logical_not(bottom))
    def _():
        to_se.wait_send()
        to_sw.wait_send()
        to_south.wait_send()
        to_ne.wait_recv()
        to_nw.wait_recv()
        to_north.wait_recv()
        own_strips([(0, 16)])
        far_strips(0, 16, corner[1], corner[0], (96, 105, 114))

    @pl.when(bottom)
    def _():
        for f in range(3):
            raw_m[f, 0:16, :] = jnp.zeros((16, COLS), F32)
        side_depth[0:16, :] = jnp.zeros((16, COLS), F32)
        side_state[0:16, :] = jnp.zeros((16, COLS), F32)

    @pl.when(jnp.logical_not(top))
    def _():
        to_ne.wait_send()
        to_nw.wait_send()
        to_north.wait_send()
        to_se.wait_recv()
        to_sw.wait_recv()
        to_south.wait_recv()
        own_strips([(176, 16)])
        far_strips(176, 16, corner[3], corner[2], (0, 9, 18))

    @pl.when(top)
    def _():
        for copy in fold_z_copies:
            copy.wait_recv()
        ghost = fold_got[0]
        for k in range(1, NZ):
            ghost = ghost + fold_got[k]
        edges = ghost[32:40]
        lane8 = lanes_of((8, COLS))
        side = []
        for g in range(4):
            edge = pltpu.roll(edges, (COLS - 16 - 32 * g) % COLS, 1)
            side.append(jnp.where((lane8 < 9) | (lane8 >= 119), edge, 0.0))
        side = jnp.concatenate(side, axis=0)
        for f in range(3):
            raw_m[f, 176:192, :] = jnp.zeros((16, COLS), F32)
        raw_m[0, 176:185, :] = ghost[0:9]
        raw_m[1, 176:184, :] = ghost[9:17]
        raw_m[2, 176:184, :] = ghost[17:25]
        own_strips([(176, 16)])
        fold_x[...] = side
        west_p, west_r, east_r = (within(lane1, a, a + 9) for a in (WEST - 9, WEST + 55, 64))
        for ref, p, q, count in ((side_depth, 0, 0, 9), (side_state, 17, 9, 8)):
            one, two = fold_x[p : p + count, :], fold_x[q : q + count, :]
            ref[176 : 176 + count, :] = jnp.where(
                lane1 < 9, one, jnp.where(west_p, shift(one, WEST), jnp.where(
                    east_r, shift(two, 64), jnp.where(
                        west_r, shift(two, WEST + 64), ref[176 : 176 + count, :]))))
        for copy in fold_x_copies + fold_z_copies:
            copy.wait_send()

    for kind in ("m", "s"):
        fields(kind, [(LO, 8), (176, 8)])
        roots(kind, [(LO, 16), (168, 16)])
        links(kind, [(LO, 16), (168, 16)])
    steps([(kind, r, 24, lo, lo + 16) for kind in ("m", "s") for r, lo in ((LO, 16), (160, 160))])

    ones = jnp.ones((8, COLS), F32)
    sums = lax.dot_general(
        ones, rows_acc[...], (((1,), (1,)), ((), ())), precision=HIGHEST, preferred_element_type=F32
    )[0:1]

    def tree(terms):
        while len(terms) > 1:
            terms = [a + b for a, b in zip(terms[::2], terms[1::2])]
        return terms[0]

    second = core == 1
    part[0] = sums
    next_level(levels)
    to_plane = [
        remote(part.at[0], red_p.at[core * LON + lon], rp_send.at[d], rp_recv.at[core * LON + d],
               2 * yi + 1, (lon + d) % LON)
        for d in range(LON)
    ]
    for d in far_first(LON):
        to_plane[d].start()
    count = LAT // 2
    along_y = [(d, c) for d in far_first(count) + [0] for c in (1, 0) if (d, c) != (0, 1)]
    to_lat = [
        remote(part.at[1], red_y.at[yi], ry_send.at[2 * d + c], ry_recv.at[d],
               2 * ((yi + d) % count) + c, lon)
        for d, c in along_y
    ]

    @pl.when(jnp.logical_not(second))
    def _():
        to_plane[0].start()
        to_plane[0].wait_send()

    @pl.when(second)
    def _():
        red_p[LON + lon] = sums
        for c in range(2):
            for d in range(c, LON):
                remote(part.at[0], red_p.at[c * LON + lon], rp_send.at[d], rp_recv.at[c * LON + d],
                       lat, east).wait_recv()
        total = tree([red_p[k] for k in range(2 * LON)])
        part[1] = total
        red_y[yi] = total
        for copy in to_lat:
            copy.start()

    def arrived(d):
        remote(part.at[1], red_y.at[yi], ry_send.at[0], ry_recv.at[d], lat, east).wait_recv()

    @pl.when(jnp.logical_not(second))
    def _():
        arrived(0)

    for d in range(1, count):
        arrived(d)
    moments_out[...] = tree([red_y[k] for k in range(count)])

    @pl.when(second)
    def _():
        for copy in to_lat:
            copy.wait_send()

    for copy in to_plane[1:]:
        copy.wait_send()


def held(shape):
    return pltpu.VMEM(shape, F32)


def basis_and_moments(forcing, search, depth, mask, fold_map):
    vm = pltpu.VMEM
    dma = pltpu.SemaphoreType.DMA
    ext = (EXT, COLS)
    return pl.pallas_call(
        basis_kernel,
        out_shape=(held((FIELDS,) + ext), held((STEPS + 1,) + ext), held((1, COLS))),
        in_specs=[pl.BlockSpec(memory_space=pl.ANY)] * 5,
        out_specs=(pl.BlockSpec(memory_space=vm),) * 3,
        scratch_shapes=[
            pltpu.SMEM((1024,), jnp.int32),
            vm((3,) + ext, F32), vm(ext, F32), vm(ext, F32),
            vm((ROWS, COLS), F32), vm((ROWS, COLS), jnp.int32),
            vm((40, COLS), F32), vm((40, COLS), F32), vm((40, COLS), F32), vm((40, COLS), F32),
            vm((4, 16, COLS), F32),
            vm((32, COLS), F32), vm((32, COLS), F32), vm((NX + 1, 32, COLS), F32),
            vm((NZ, 40, COLS), F32), vm((NZ, 40, COLS), F32),
        ]
        + [vm(ext, F32)] * 6
        + [vm((7,) + ext, F32)] * 2
        + [
            vm((COLS, COLS), F32), vm((2, 1, COLS), F32),
            vm((2 * LON, 1, COLS), F32), vm((LAT // 2, 1, COLS), F32),
            pltpu.SemaphoreType.REGULAR((4,)), dma((5,)), dma((8,)), dma((8,)),
            dma((NZ - 1,)), dma((NZ - 1,)), dma((NX - 1,)), dma((NX - 1,)),
            dma((LON,)), dma((2 * LON,)), dma((LAT,)), dma((LAT // 2,)),
        ],
        compiler_params=pltpu.CompilerParams(collective_id=0, has_side_effects=True),
        name="basis",
    )(fold_map, forcing, search, depth, mask)


def rows_of(shape):
    return lax.broadcasted_iota(jnp.int32, shape, 0)


def applied_to_coords(c):
    row = rows_of(c.shape)
    below = jnp.where(row == 0, 0.0, jnp.where(row == 1, 1.0, 0.5)).astype(F32)
    above = jnp.where(row == c.shape[0] - 1, 0.0, 0.5).astype(F32)
    return c + below * pltpu.roll(c, 1, 0) + above * pltpu.roll(c, c.shape[0] - 1, 0)


def applied_to_moments(m):
    row = rows_of(m.shape)
    up, down = pltpu.roll(m, m.shape[0] - 1, 0), pltpu.roll(m, 1, 0)
    return m + 0.5 * (up + jnp.where(row == 0, up, down))


def moment_rows(raw, kind, count):
    k = rows_of((count, COLS))
    odd = k & 1
    high = jnp.minimum(6 * ((k + 1) >> 1) + 2 * kind + odd, COLS - 1)
    spread = jnp.broadcast_to(raw, (count, COLS))
    base = jnp.where(odd == 1, 7 + 2 * kind, 2 * kind)
    return 2.0 * jnp.take_along_axis(spread, high, axis=1) - jnp.take_along_axis(spread, base, axis=1)


def dot_rows(coords, moments):
    (cp, cr), (mp, mr) = coords, moments
    products = cp * mp[0:16]
    return jnp.sum(products[0:8] + products[8:16] + cr * mr[0:8], axis=0, keepdims=True)


def pair(function, one, two):
    return tuple(function(a, b) for a, b in zip(one, two))


def coordinates(raw):
    search_search = moment_rows(raw, 0, 24)
    residual_residual = moment_rows(raw, 1, 16)
    mixed_long, mixed = moment_rows(raw, 2, 24), moment_rows(raw, 2, 16)
    first16 = (rows_of((16, COLS)) == 0).astype(F32)
    first8 = (rows_of((8, COLS)) == 0).astype(F32)
    p, pm = (first16, jnp.zeros((8, COLS), F32)), (search_search, mixed)
    r, rm = (jnp.zeros((16, COLS), F32), first8), (mixed_long, residual_residual)
    x = (jnp.zeros((16, COLS), F32), jnp.zeros((8, COLS), F32))
    q, qm = tuple(map(applied_to_coords, p)), tuple(map(applied_to_moments, pm))
    norm, curvature = dot_rows(r, rm), dot_rows(p, qm)
    for inner in range(STEPS):
        t = norm / curvature
        x = pair(lambda a, b: a + t * b, x, p)
        r = pair(lambda a, b: a - t * b, r, q)
        if inner == STEPS - 1:
            break
        rm = pair(lambda a, b: a - t * b, rm, qm)
        am = tuple(map(applied_to_moments, rm))
        fresh, own, cross = dot_rows(r, rm), dot_rows(r, am), dot_rows(p, am)
        beta = fresh / norm
        curvature = own + beta * (2.0 * cross + beta * curvature)
        norm = fresh
        p = pair(lambda a, b: a + beta * b, r, p)
        q = tuple(map(applied_to_coords, p))
        qm = pair(lambda a, b: a + beta * b, am, qm)
    return x, r


def combine_kernel(moments_ref, basis_ref, strips_ref, height_ref, residual_ref):
    found = coordinates(moments_ref[...])
    lane1 = lanes_of((1, COLS))
    search_half = within((lane1 + 32) & (COLS - 1), 14, 78)
    size = 32
    for (of_p, of_r), out_ref in zip(found, (height_ref, residual_ref)):
        coords = [of_p[k : k + 1, :] for k in range(FIRST)] + [of_r[k : k + 1, :] for k in range(STEPS)]
        mixed = []
        for n in range(STEPS + 1):
            other = coords[FIRST + n] if n < STEPS else jnp.zeros((1, COLS), F32)
            mixed.append(jnp.where(search_half, coords[n], other))
        for at in range(0, ROWS, size):
            rows = slice(16 + at, 16 + at + size)
            main = sum(coords[k] * basis_ref[k, rows, :] for k in range(FIELDS))
            strip = sum(mixed[n] * strips_ref[n, rows, :] for n in range(STEPS + 1))
            strip = strip + shift(strip, 64)
            out_ref[at : at + size, :] = jnp.where(
                lane1 >= 119, strip, jnp.where(lane1 < 9, shift(strip, -WEST), main)
            )


def per_device(forcing, search, depth, mask, fold_map):
    made = basis_and_moments(forcing, search, depth, mask, fold_map)
    basis, strips, moments = (pltpu.with_memory_space_constraint(v, pltpu.VMEM) for v in made)
    block = jax.ShapeDtypeStruct((ROWS, COLS), F32)
    return pl.pallas_call(
        combine_kernel,
        out_shape=(block, block),
        in_specs=[pl.BlockSpec(memory_space=pltpu.VMEM)] * 3,
        name="combine",
    )(moments, basis, strips)


def solution(mesh):
    return jax.shard_map(
        per_device,
        mesh=mesh,
        in_specs=(P("lat", "lon"),) * 4 + (P(),),
        out_specs=(P("lat", "lon"),) * 2,
        check_vma=False,
    )
```

```python
import functools

import jax
import jax.numpy as jnp
from jax import lax
from jax.experimental import pallas as pl
from jax.experimental.pallas import tpu as pltpu
from jax.sharding import PartitionSpec as P

STEPS = 8
REACH = 256
LAT, LON, NX, NZ = 16, 32, 4, 8
ROWS, COLS = 160, 128
EXT = ROWS + 32
LO = 8
FIELDS = 2 * STEPS + 1
FIRST = STEPS + 1
HIGHEST = lax.Precision.HIGHEST
F32 = jnp.float32


def lanes_of(shape):
    return lax.broadcasted_iota(jnp.int32, shape, len(shape) - 1)


def from_east(x):
    return pltpu.roll(x, COLS - 1, 1)


def from_west(x):
    return pltpu.roll(x, 1, 1)


def shift(x, by):
    by %= COLS
    return pltpu.roll(x, by, 1) if by else x


WEST = 28


def strip_lanes(lane, half):
    lane = (lane - half) & (COLS - 1)
    return (lane >= 119) | ((lane >= WEST) & (lane < WEST + 9))


def within(lane, start, stop):
    return (lane >= start) & (lane < stop)


def remote(src, dst, send, recv, lat, lon):
    return pltpu.make_async_remote_copy(
        src_ref=src,
        dst_ref=dst,
        send_sem=send,
        recv_sem=recv,
        device_id={"lat": lat, "lon": lon},
        device_id_type=pl.DeviceIdType.MESH,
    )


CHUNK = 16


def far_first(count):
    return sorted(range(1, count), key=lambda d: (-min(d, count - d), d))


def chunks(start, stop):
    return [(r, min(CHUNK, stop - r)) for r in range(start, stop, CHUNK)]


def basis_kernel(
    fold_ref, forcing_ref, search_ref, depth_ref, mask_ref,
    b_m, b_s, moments_out,
    fold_buf, raw_m, side_depth, side_state, depth_buf, mask_buf, pack_w, pack_e, got_w, got_e, corner,
    fold_x, fold_src, fold_row, fold_send, fold_got,
    s_m, s_s, de_m, de_s, se_m, se_s,
    w_m, w_s, rows_acc, part, red_p, red_y,
    plane_sem, local_sem, halo_send, halo_recv, fz_send, fz_recv, fx_send, fx_recv,
    rp_send, rp_recv, ry_send, ry_recv,
):
    lat = lax.axis_index("lat")
    lon = lax.axis_index("lon")
    zi, xi = lon // NX, lon % NX
    core, yi = lat % 2, lat // 2
    top = lat == LAT - 1
    bottom = lat == 0
    north, south = (lat + 1) % LAT, (lat + LAT - 1) % LAT
    east, west = (lon + 1) % LON, (lon + LON - 1) % LON
    barrier = pltpu.get_barrier_semaphore()

    loads = [
        pltpu.make_async_copy(depth_ref, depth_buf, local_sem.at[0]),
        pltpu.make_async_copy(mask_ref, mask_buf, local_sem.at[1]),
        pltpu.make_async_copy(forcing_ref, raw_m.at[1, pl.ds(16, ROWS), :], local_sem.at[2]),
        pltpu.make_async_copy(search_ref, raw_m.at[2, pl.ds(16, ROWS), :], local_sem.at[3]),
        pltpu.make_async_copy(fold_ref.at[pl.ds(0, 1024)], fold_buf, local_sem.at[4]),
    ]
    for copy in loads:
        copy.start()

    def greet(semaphore, to):
        for a, b in to:
            pl.semaphore_signal(
                semaphore, inc=1, device_id={"lat": a, "lon": b}, device_id_type=pl.DeviceIdType.MESH
            )

    def around(far):
        if 2 * far == NZ:
            return [(lat, (lon + NX * far) % LON)]
        to = [(lat, (lon + NX * far) % LON), (lat, (lon + LON - NX * far) % LON)]
        if 2 * far < LAT:
            to += [((lat + 2 * far) % LAT, lon), ((lat + LAT - 2 * far) % LAT, lon)]
        return to

    beside = [(lat, zi * NX + (xi + d) % NX) for d in far_first(NX)]
    beside += [(north, east), (north, west), (south, east), (south, west)]
    beside += [(lat, east), (lat, west), (north, lon), (south, lon)] + around(1)

    beside += [(lat + 1 - 2 * core, zi * NX + (xi + d) % NX) for d in far_first(NX)]
    greet(barrier, beside)

    levels = 3

    def next_level(level):
        if level > 0:
            pl.semaphore_wait(plane_sem.at[level - 1], len(around(1 << (level - 1))))
        if level < levels:
            greet(plane_sem.at[level], around(1 << level))

    rows_acc[...] = jnp.zeros_like(rows_acc)
    for copy in loads:
        copy.wait()
    raw_m[0, 16 : 16 + ROWS, :] = depth_buf[...] * mask_buf[...].astype(F32)

    pivot = fold_buf[0]
    pivot_block, pivot_lane = lax.shift_right_logical(pivot, 7), pivot & (COLS - 1)

    @pl.when(top)
    def _():
        fold_x[...] = jnp.zeros_like(fold_x)
        for m in range(9):
            fold_x[m : m + 1, :] = raw_m[0, 175 - m : 176 - m, :]
        for m in range(8):
            fold_x[9 + m : 10 + m, :] = raw_m[1, 175 - m : 176 - m, :]
            fold_x[17 + m : 18 + m, :] = raw_m[2, 175 - m : 176 - m, :]
        source = lax.broadcasted_iota(jnp.int32, (COLS, COLS), 0)
        target = lax.broadcasted_iota(jnp.int32, (COLS, COLS), 1)
        choose = (source == ((pivot - target) & (COLS - 1))).astype(F32)
        turned = jnp.dot(fold_x[...], choose, precision=HIGHEST, preferred_element_type=F32)
        fold_src[...] = turned
        fold_row[xi] = turned
        fold_row[NX] = jnp.zeros_like(turned)

    lane40 = lanes_of((40, COLS))
    acc_w = jnp.zeros((40, COLS), F32)
    acc_e = jnp.zeros((40, COLS), F32)
    for g in range(4):
        for f in range(3):
            at = 32 * g + 9 * f
            block = raw_m[f, 16 + 40 * g : 56 + 40 * g, :]
            here = (lane40 >= at) & (lane40 < at + 9)
            acc_w = jnp.where(here, pltpu.roll(block, at, 1) if at else block, acc_w)
            acc_e = jnp.where(here, pltpu.roll(block, (at - 119) % COLS, 1), acc_e)
    pack_w[...] = acc_w
    pack_e[...] = acc_e

    pl.semaphore_wait(barrier, len(beside))

    fold_x_copies = [
        remote(fold_src, fold_row.at[xi], fx_send.at[d - 1], fx_recv.at[d - 1], lat, zi * NX + (xi + d) % NX)
        for d in range(1, NX)
    ]

    @pl.when(top)
    def _():
        for d in far_first(NX):
            fold_x_copies[d - 1].start()

    to_north = remote(raw_m.at[:, pl.ds(160, 16), :], raw_m.at[:, pl.ds(0, 16), :],
                      halo_send.at[0], halo_recv.at[0], north, lon)
    to_south = remote(raw_m.at[:, pl.ds(16, 16), :], raw_m.at[:, pl.ds(176, 16), :],
                      halo_send.at[1], halo_recv.at[1], south, lon)
    to_east = remote(pack_e, got_w, halo_send.at[2], halo_recv.at[2], lat, east)
    to_west = remote(pack_w, got_e, halo_send.at[3], halo_recv.at[3], lat, west)
    to_ne = remote(pack_e.at[pl.ds(24, 16), :], corner.at[0], halo_send.at[4], halo_recv.at[4], north, east)
    to_nw = remote(pack_w.at[pl.ds(24, 16), :], corner.at[1], halo_send.at[5], halo_recv.at[5], north, west)
    to_se = remote(pack_e.at[pl.ds(0, 16), :], corner.at[2], halo_send.at[6], halo_recv.at[6], south, east)
    to_sw = remote(pack_w.at[pl.ds(0, 16), :], corner.at[3], halo_send.at[7], halo_recv.at[7], south, west)

    to_east.start()
    to_west.start()
    next_level(0)

    @pl.when(jnp.logical_not(top))
    def _():
        to_ne.start()
        to_nw.start()
        to_north.start()

    @pl.when(jnp.logical_not(bottom))
    def _():
        to_se.start()
        to_sw.start()
        to_south.start()

    fold_z_copies = [
        remote(fold_send.at[d], fold_got.at[zi], fz_send.at[d - 1], fz_recv.at[d - 1],
               lat, ((zi + d) % NZ) * NX + xi)
        for d in range(1, NZ)
    ]
    lane32 = lanes_of((32, COLS))
    near = lane32 <= pivot_lane

    @pl.when(top)
    def _():
        next_level(1)
        next_level(2)
        for copy in fold_x_copies:
            copy.wait_recv()
        for d in far_first(NZ) + [0]:
            want = pivot_block - ((zi + d) % NZ) * NX - xi

            def block(b):
                mine = (lax.shift_right_logical(b & (LON - 1), 2) == zi)
                return fold_row[jnp.where(mine, b & (NX - 1), NX)]

            ahead, here, behind, beyond = (block(want + o) for o in (1, 0, -1, -2))
            window = jnp.where(near, here, behind)
            edge = jnp.where(
                lane32 < 9, jnp.where(near, behind, beyond),
                jnp.where(lane32 >= 119, jnp.where(near, ahead, here), 0.0),
            )
            edges = sum(pltpu.roll(edge[8 * g : 8 * g + 8], 16 + 32 * g, 1) for g in range(4))
            if d:
                fold_send[d, 0:32, :] = window
                fold_send[d, 32:40, :] = edges
            else:
                fold_got[zi, 0:32, :] = window
                fold_got[zi, 32:40, :] = edges
        for d in far_first(NZ):
            fold_z_copies[d - 1].start()

    def own_strips(spans):
        for r, n in spans:
            depth, residual, search = (raw_m[f, r : r + n, :] for f in range(3))
            lane = lanes_of((n, COLS))
            west_p, east_r, west_r = (within(lane, a, a + 18) for a in (WEST, 46, WEST + 64))
            east_p = lane >= 110
            for ref, p, q in ((side_depth, depth, depth), (side_state, search, residual)):
                ref[r : r + n, :] = jnp.where(
                    east_p, p, jnp.where(west_p, shift(p, WEST), jnp.where(
                        east_r, shift(q, 64), jnp.where(west_r, shift(q, WEST + 64), 0.0))))

    def far_strips(r, n, from_e, from_w, places):
        lane = lanes_of((n, COLS))
        west_p, east_r, west_r = (within(lane, a, a + 9) for a in (WEST - 9, 64, WEST + 55))
        east_p = lane < 9
        at_d, at_r, at_p = places
        for ref, p, q in ((side_depth, at_d, at_d), (side_state, at_p, at_r)):
            ref[r : r + n, :] = jnp.where(
                east_p, shift(from_e, -p), jnp.where(west_p, shift(from_w, WEST - 9 - p), jnp.where(
                    east_r, shift(from_e, 64 - q), jnp.where(
                        west_r, shift(from_w, WEST + 55 - q), ref[r : r + n, :]))))

    kinds = {
        "m": (raw_m.at[0], s_m, de_m, se_m, w_m),
        "s": (side_depth, s_s, de_s, se_s, w_s),
    }

    def fields(kind, spans):
        for r, n in spans:
            wet = (kinds[kind][0][r : r + n, :] > 0.0).astype(F32)
            if kind == "m":
                b_m[0, r : r + n, :] = wet * raw_m[2, r : r + n, :]
                b_m[FIRST, r : r + n, :] = wet * raw_m[1, r : r + n, :]
            else:
                b_s[0, r : r + n, :] = wet * side_state[r : r + n, :]

    def roots(kind, spans):
        depth_ref_, s, de, se, _ = kinds[kind]
        for r, n in spans:
            up, depth, low = (depth_ref_[r + o : r + o + n, :] for o in (1, 0, -1))
            both = up + low
            column = depth + 0.5 * both
            wet_up, wet, wet_low = ((v > 0.0).astype(F32) for v in (up, depth, low))
            both_wet = wet_up + wet_low
            column_wet = wet + 0.5 * both_wet
            all_depth = both + (from_east(column) + from_west(column))
            all_wet = both_wet + (from_east(column_wet) + from_west(column_wet))
            total = 0.5 * (depth * all_wet + all_depth)
            diagonal = wet * (depth * (1.0 / (REACH * REACH)) + total) + (1.0 - wet)
            root = wet * lax.rsqrt(diagonal)
            s[r : r + n, :] = root
            se[r : r + n, :] = from_east(root)
            de[r : r + n, :] = from_east(depth)

    def links(kind, spans):
        depth_ref_, s, de, se, w = kinds[kind]
        for r, n in spans:
            d0, d1 = depth_ref_[r : r + n, :], depth_ref_[r + 1 : r + 1 + n, :]
            s0, s1 = s[r : r + n, :], s[r + 1 : r + 1 + n, :]
            de0, de1 = de[r : r + n, :], de[r + 1 : r + 1 + n, :]
            se0, se1 = se[r : r + n, :], se[r + 1 : r + 1 + n, :]
            east_w = -(d0 + de0) * (s0 * se0)
            ne_w = -0.5 * (d0 + de1) * (s0 * se1)
            nw_e = -0.5 * (de0 + d1) * (se0 * s1)
            w[0, r : r + n, :] = -(d0 + d1) * (s0 * s1)
            w[1, r : r + n, :] = east_w
            w[2, r : r + n, :] = from_west(east_w)
            w[3, r : r + n, :] = ne_w
            w[4, r : r + n, :] = from_west(ne_w)
            w[5, r : r + n, :] = from_west(nw_e)
            w[6, r : r + n, :] = nw_e

    def fold8(x):
        return sum(x[8 * k : 8 * k + 8] for k in range(x.shape[0] // 8))

    lane1 = lanes_of((1, COLS))
    main_lanes = within(lane1, 9, 119)
    strips_p, strips_r = strip_lanes(lane1, 0), strip_lanes(lane1, 64)

    def apply(b, k, w, r, size):
        up, mid, low = (b[k, r + o : r + o + size, :] for o in (1, 0, -1))
        a_u, a_d, e_u, e_c, e_d, f_u, f_c, f_d = w
        east_part = from_east(e_u * up + e_c * mid + e_d * low)
        west_part = from_west(f_u * up + f_c * mid + f_d * low)
        return mid, (a_u * up + a_d * low) + (east_part + west_part)

    def step(n, tasks, first, last):
        total = {}

        def add(key, product, lo, hi):
            value = fold8(product[lo:hi])
            total[key] = total[key] + value if key in total else value

        for kind, r, size, gram_lo, gram_hi in tasks:
            w = kinds[kind][4]
            weights = (
                w[0, r : r + size, :], w[0, r - 1 : r - 1 + size, :],
                w[4, r : r + size, :], w[2, r : r + size, :], w[5, r - 1 : r - 1 + size, :],
                w[6, r : r + size, :], w[1, r : r + size, :], w[3, r - 1 : r - 1 + size, :],
            )
            b, bases = (b_s, (0,)) if kind == "s" else (b_m, (0,) if last else (0, FIRST))
            news, olds = [], []
            for base in bases:
                mid, out = apply(b, base + n - 1, weights, r, size)
                out = 0.5 * out if first else out - b[base + n - 2, r : r + size, :]
                b[base + n, r : r + size, :] = out
                news.append(out)
                olds.append(mid)
            lo, hi = max(r, gram_lo) - r, min(r + size, gram_hi) - r
            if hi <= lo:
                continue
            p1, p0 = news[0], olds[0]
            if kind == "s":
                add("s0", p1 * p1, lo, hi)
                add("s1", p1 * p0, lo, hi)
                add("s4", p1 * shift(p1, 64), lo, hi)
                add("s5", p1 * shift(p0, 64), lo, hi)
                continue
            add("m0", p1 * p1, lo, hi)
            add("m1", p1 * p0, lo, hi)
            if last:
                r0 = b_m[FIRST + STEPS - 1, r : r + size, :]
            else:
                r1, r0 = news[1], olds[1]
                add("m2", r1 * r1, lo, hi)
                add("m3", r1 * r0, lo, hi)
                add("m4", p1 * r1, lo, hi)
            add("m5", p1 * r0, lo, hi)
        gather(n, total)

    def gather(n, total):
        rows = {key: jnp.sum(value, axis=0, keepdims=True) for key, value in total.items()}
        for c in range(6):
            row = jnp.zeros((1, COLS), F32)
            if "m%d" % c in rows:
                row = jnp.where(main_lanes, rows["m%d" % c], row)
            source = "s%d" % (c - 2 if c in (2, 3) else c)
            if source in rows:
                row = row + jnp.where(strips_r if c in (2, 3) else strips_p, rows[source], 0.0)
            at = pl.ds(6 * n + c, 1)
            rows_acc[at, :] = rows_acc[at, :] + row

    def steps(tasks, unrolled):
        step(1, tasks, True, False)
        if unrolled:
            for n in range(2, STEPS):
                step(n, tasks, False, False)
        else:

            @pl.loop(2, STEPS)
            def _(n):
                step(n, tasks, False, False)

        step(STEPS, tasks, False, True)

    def tasks(kind, start, stop, gram_lo, gram_hi):
        return [(kind, r, n, gram_lo, gram_hi) for r, n in chunks(start, stop)]

    own_strips(chunks(16, 176))
    fields("m", chunks(16, 176))
    roots("m", [(17, 7)] + chunks(24, 168) + [(168, 7)])
    links("m", chunks(16, 168))

    @pl.when(jnp.logical_not(top))
    def _():
        next_level(1)

    start = {}
    for r, n in chunks(16, 176):
        p0, r0 = b_m[0, r : r + n, :], b_m[FIRST, r : r + n, :]
        for key, value in (("m0", p0 * p0), ("m2", r0 * r0), ("m4", p0 * r0)):
            start[key] = start[key] + fold8(value) if key in start else fold8(value)
    gather(0, start)

    @pl.when(jnp.logical_not(top))
    def _():
        next_level(2)

    steps(tasks("m", 16, 168, 32, 160), False)

    to_east.wait()
    to_west.wait()
    for g in range(4):
        at = 32 * g
        far_strips(16 + 40 * g, 40, got_e[...], got_w[...], (at, at + 9, at + 18))
    fields("s", chunks(16, 176))
    start = {}
    for r, n in chunks(16, 176):
        p0 = b_s[0, r : r + n, :]
        for key, value in (("s0", p0 * p0), ("s4", p0 * shift(p0, 64))):
            start[key] = start[key] + fold8(value) if key in start else fold8(value)
    gather(0, start)

    roots("s", [(17, 7)] + chunks(24, 168) + [(168, 7)])
    links("s", chunks(16, 168))
    steps(tasks("s", 16, 168, 32, 160), True)

    @pl.when(jnp.logical_not(bottom))
    def _():
        to_se.wait_send()
        to_sw.wait_send()
        to_south.wait_send()
        to_ne.wait_recv()
        to_nw.wait_recv()
        to_north.wait_recv()
        own_strips([(0, 16)])
        far_strips(0, 16, corner[1], corner[0], (96, 105, 114))

    @pl.when(bottom)
    def _():
        for f in range(3):
            raw_m[f, 0:16, :] = jnp.zeros((16, COLS), F32)
        side_depth[0:16, :] = jnp.zeros((16, COLS), F32)
        side_state[0:16, :] = jnp.zeros((16, COLS), F32)

    @pl.when(jnp.logical_not(top))
    def _():
        to_ne.wait_send()
        to_nw.wait_send()
        to_north.wait_send()
        to_se.wait_recv()
        to_sw.wait_recv()
        to_south.wait_recv()
        own_strips([(176, 16)])
        far_strips(176, 16, corner[3], corner[2], (0, 9, 18))

    @pl.when(top)
    def _():
        for copy in fold_z_copies:
            copy.wait_recv()
        ghost = fold_got[0]
        for k in range(1, NZ):
            ghost = ghost + fold_got[k]
        edges = ghost[32:40]
        lane8 = lanes_of((8, COLS))
        side = []
        for g in range(4):
            edge = pltpu.roll(edges, (COLS - 16 - 32 * g) % COLS, 1)
            side.append(jnp.where((lane8 < 9) | (lane8 >= 119), edge, 0.0))
        side = jnp.concatenate(side, axis=0)
        for f in range(3):
            raw_m[f, 176:192, :] = jnp.zeros((16, COLS), F32)
        raw_m[0, 176:185, :] = ghost[0:9]
        raw_m[1, 176:184, :] = ghost[9:17]
        raw_m[2, 176:184, :] = ghost[17:25]
        own_strips([(176, 16)])
        fold_x[...] = side
        west_p, west_r, east_r = (within(lane1, a, a + 9) for a in (WEST - 9, WEST + 55, 64))
        for ref, p, q, count in ((side_depth, 0, 0, 9), (side_state, 17, 9, 8)):
            one, two = fold_x[p : p + count, :], fold_x[q : q + count, :]
            ref[176 : 176 + count, :] = jnp.where(
                lane1 < 9, one, jnp.where(west_p, shift(one, WEST), jnp.where(
                    east_r, shift(two, 64), jnp.where(
                        west_r, shift(two, WEST + 64), ref[176 : 176 + count, :]))))
        for copy in fold_x_copies + fold_z_copies:
            copy.wait_send()

    for kind in ("m", "s"):
        fields(kind, [(LO, 8), (176, 8)])
        roots(kind, [(LO, 16), (168, 16)])
        links(kind, [(LO, 16), (168, 16)])
    steps([(kind, r, 24, lo, lo + 16) for kind in ("m", "s") for r, lo in ((LO, 16), (160, 160))], True)

    ones = jnp.ones((8, COLS), F32)
    sums = lax.dot_general(
        ones, rows_acc[...], (((1,), (1,)), ((), ())), precision=HIGHEST, preferred_element_type=F32
    )[0:1]

    def tree(terms):
        while len(terms) > 1:
            terms = [a + b for a, b in zip(terms[::2], terms[1::2])]
        return terms[0]

    second = core == 1
    part[0] = sums
    next_level(levels)
    to_plane = [
        remote(part.at[0], red_p.at[core * LON + lon], rp_send.at[d], rp_recv.at[core * LON + d],
               2 * yi + 1, (lon + d) % LON)
        for d in range(LON)
    ]
    for d in far_first(LON):
        to_plane[d].start()
    count = LAT // 2
    along_y = [(d, c) for d in far_first(count) + [0] for c in (1, 0) if (d, c) != (0, 1)]
    to_lat = [
        remote(part.at[1], red_y.at[yi], ry_send.at[2 * d + c], ry_recv.at[d],
               2 * ((yi + d) % count) + c, lon)
        for d, c in along_y
    ]

    @pl.when(jnp.logical_not(second))
    def _():
        to_plane[0].start()
        to_plane[0].wait_send()

    @pl.when(second)
    def _():
        red_p[LON + lon] = sums
        for c in range(2):
            for d in range(c, LON):
                remote(part.at[0], red_p.at[c * LON + lon], rp_send.at[d], rp_recv.at[c * LON + d],
                       lat, east).wait_recv()
        total = tree([red_p[k] for k in range(2 * LON)])
        part[1] = total
        red_y[yi] = total
        for copy in to_lat:
            copy.start()

    def arrived(d):
        remote(part.at[1], red_y.at[yi], ry_send.at[0], ry_recv.at[d], lat, east).wait_recv()

    @pl.when(jnp.logical_not(second))
    def _():
        arrived(0)

    for d in range(1, count):
        arrived(d)
    moments_out[...] = tree([red_y[k] for k in range(count)])

    @pl.when(second)
    def _():
        for copy in to_lat:
            copy.wait_send()

    for copy in to_plane[1:]:
        copy.wait_send()


def held(shape):
    return pltpu.VMEM(shape, F32)


def basis_and_moments(forcing, search, depth, mask, fold_map):
    vm = pltpu.VMEM
    dma = pltpu.SemaphoreType.DMA
    ext = (EXT, COLS)
    return pl.pallas_call(
        basis_kernel,
        out_shape=(held((FIELDS,) + ext), held((STEPS + 1,) + ext), held((1, COLS))),
        in_specs=[pl.BlockSpec(memory_space=pl.ANY)] * 5,
        out_specs=(pl.BlockSpec(memory_space=vm),) * 3,
        scratch_shapes=[
            pltpu.SMEM((1024,), jnp.int32),
            vm((3,) + ext, F32), vm(ext, F32), vm(ext, F32),
            vm((ROWS, COLS), F32), vm((ROWS, COLS), jnp.int32),
            vm((40, COLS), F32), vm((40, COLS), F32), vm((40, COLS), F32), vm((40, COLS), F32),
            vm((4, 16, COLS), F32),
            vm((32, COLS), F32), vm((32, COLS), F32), vm((NX + 1, 32, COLS), F32),
            vm((NZ, 40, COLS), F32), vm((NZ, 40, COLS), F32),
        ]
        + [vm(ext, F32)] * 6
        + [vm((7,) + ext, F32)] * 2
        + [
            vm((COLS, COLS), F32), vm((2, 1, COLS), F32),
            vm((2 * LON, 1, COLS), F32), vm((LAT // 2, 1, COLS), F32),
            pltpu.SemaphoreType.REGULAR((4,)), dma((5,)), dma((8,)), dma((8,)),
            dma((NZ - 1,)), dma((NZ - 1,)), dma((NX - 1,)), dma((NX - 1,)),
            dma((LON,)), dma((2 * LON,)), dma((LAT,)), dma((LAT // 2,)),
        ],
        compiler_params=pltpu.CompilerParams(collective_id=0, has_side_effects=True),
        name="basis",
    )(fold_map, forcing, search, depth, mask)


def rows_of(shape):
    return lax.broadcasted_iota(jnp.int32, shape, 0)


def applied_to_coords(c):
    row = rows_of(c.shape)
    below = jnp.where(row == 0, 0.0, jnp.where(row == 1, 1.0, 0.5)).astype(F32)
    above = jnp.where(row == c.shape[0] - 1, 0.0, 0.5).astype(F32)
    return c + below * pltpu.roll(c, 1, 0) + above * pltpu.roll(c, c.shape[0] - 1, 0)


def applied_to_moments(m):
    row = rows_of(m.shape)
    up, down = pltpu.roll(m, m.shape[0] - 1, 0), pltpu.roll(m, 1, 0)
    return m + 0.5 * (up + jnp.where(row == 0, up, down))


def moment_rows(raw, kind, count):
    k = rows_of((count, COLS))
    odd = k & 1
    high = jnp.minimum(6 * ((k + 1) >> 1) + 2 * kind + odd, COLS - 1)
    spread = jnp.broadcast_to(raw, (count, COLS))
    base = jnp.where(odd == 1, 7 + 2 * kind, 2 * kind)
    return 2.0 * jnp.take_along_axis(spread, high, axis=1) - jnp.take_along_axis(spread, base, axis=1)


def dot_rows(coords, moments):
    (cp, cr), (mp, mr) = coords, moments
    products = cp * mp[0:16]
    return jnp.sum(products[0:8] + products[8:16] + cr * mr[0:8], axis=0, keepdims=True)


def pair(function, one, two):
    return tuple(function(a, b) for a, b in zip(one, two))


def coordinates(raw):
    search_search = moment_rows(raw, 0, 24)
    residual_residual = moment_rows(raw, 1, 16)
    mixed_long, mixed = moment_rows(raw, 2, 24), moment_rows(raw, 2, 16)
    first16 = (rows_of((16, COLS)) == 0).astype(F32)
    first8 = (rows_of((8, COLS)) == 0).astype(F32)
    p, pm = (first16, jnp.zeros((8, COLS), F32)), (search_search, mixed)
    r, rm = (jnp.zeros((16, COLS), F32), first8), (mixed_long, residual_residual)
    x = (jnp.zeros((16, COLS), F32), jnp.zeros((8, COLS), F32))
    q, qm = tuple(map(applied_to_coords, p)), tuple(map(applied_to_moments, pm))
    norm, curvature = dot_rows(r, rm), dot_rows(p, qm)
    for inner in range(STEPS):
        t = norm / curvature
        x = pair(lambda a, b: a + t * b, x, p)
        r = pair(lambda a, b: a - t * b, r, q)
        if inner == STEPS - 1:
            break
        rm = pair(lambda a, b: a - t * b, rm, qm)
        am = tuple(map(applied_to_moments, rm))
        fresh, own, cross = dot_rows(r, rm), dot_rows(r, am), dot_rows(p, am)
        beta = fresh / norm
        curvature = own + beta * (2.0 * cross + beta * curvature)
        norm = fresh
        p = pair(lambda a, b: a + beta * b, r, p)
        q = tuple(map(applied_to_coords, p))
        qm = pair(lambda a, b: a + beta * b, am, qm)
    return x, r


def combine_kernel(moments_ref, basis_ref, strips_ref, height_ref, residual_ref):
    found = coordinates(moments_ref[...])
    lane1 = lanes_of((1, COLS))
    search_half = within((lane1 + 32) & (COLS - 1), 14, 78)
    size = 32
    for (of_p, of_r), out_ref in zip(found, (height_ref, residual_ref)):
        coords = [of_p[k : k + 1, :] for k in range(FIRST)] + [of_r[k : k + 1, :] for k in range(STEPS)]
        mixed = []
        for n in range(STEPS + 1):
            other = coords[FIRST + n] if n < STEPS else jnp.zeros((1, COLS), F32)
            mixed.append(jnp.where(search_half, coords[n], other))
        for at in range(0, ROWS, size):
            rows = slice(16 + at, 16 + at + size)
            main = sum(coords[k] * basis_ref[k, rows, :] for k in range(FIELDS))
            strip = sum(mixed[n] * strips_ref[n, rows, :] for n in range(STEPS + 1))
            strip = strip + shift(strip, 64)
            out_ref[at : at + size, :] = jnp.where(
                lane1 >= 119, strip, jnp.where(lane1 < 9, shift(strip, -WEST), main)
            )


def per_device(forcing, search, depth, mask, fold_map):
    made = basis_and_moments(forcing, search, depth, mask, fold_map)
    basis, strips, moments = (pltpu.with_memory_space_constraint(v, pltpu.VMEM) for v in made)
    block = jax.ShapeDtypeStruct((ROWS, COLS), F32)
    return pl.pallas_call(
        combine_kernel,
        out_shape=(block, block),
        in_specs=[pl.BlockSpec(memory_space=pltpu.VMEM)] * 3,
        name="combine",
    )(moments, basis, strips)


def solution(mesh):
    return jax.shard_map(
        per_device,
        mesh=mesh,
        in_specs=(P("lat", "lon"),) * 4 + (P(),),
        out_specs=(P("lat", "lon"),) * 2,
        check_vma=False,
    )
```

```python
import functools

import jax
import jax.numpy as jnp
from jax import lax
from jax.experimental import pallas as pl
from jax.experimental.pallas import tpu as pltpu
from jax.sharding import PartitionSpec as P

STEPS = 8
REACH = 256
LAT, LON, NX, NZ = 16, 32, 4, 8
ROWS, COLS = 160, 128
EXT = ROWS + 32
LO = 8
FIELDS = 2 * STEPS + 1
FIRST = STEPS + 1
HALF = FIELDS + 1
HIGHEST = lax.Precision.HIGHEST
F32 = jnp.float32


def lanes_of(shape):
    return lax.broadcasted_iota(jnp.int32, shape, len(shape) - 1)


def from_east(x):
    return pltpu.roll(x, COLS - 1, 1)


def from_west(x):
    return pltpu.roll(x, 1, 1)


def shift(x, by):
    by %= COLS
    return pltpu.roll(x, by, 1) if by else x


WEST = 28


def strip_lanes(lane, half):
    lane = (lane - half) & (COLS - 1)
    return (lane >= 119) | ((lane >= WEST) & (lane < WEST + 9))


def within(lane, start, stop):
    return (lane >= start) & (lane < stop)


def remote(src, dst, send, recv, lat, lon):
    return pltpu.make_async_remote_copy(
        src_ref=src,
        dst_ref=dst,
        send_sem=send,
        recv_sem=recv,
        device_id={"lat": lat, "lon": lon},
        device_id_type=pl.DeviceIdType.MESH,
    )


CHUNK = 16


def far_first(count):
    return sorted(range(1, count), key=lambda d: (-min(d, count - d), d))


def chunks(start, stop):
    return [(r, min(CHUNK, stop - r)) for r in range(start, stop, CHUNK)]


def basis_kernel(
    fold_ref, forcing_ref, search_ref, depth_ref, mask_ref,
    b_m, b_s, moments_out,
    fold_buf, raw_m, side_depth, side_state, depth_buf, mask_buf, pack_w, pack_e, got_w, got_e, corner,
    fold_x, fold_src, fold_row, fold_send, fold_got,
    s_m, s_s, de_m, de_s, se_m, se_s,
    w_m, w_s, rows_acc, part, red_p, red_y,
    plane_sem, local_sem, halo_send, halo_recv, fz_send, fz_recv, fx_send, fx_recv,
    rp_send, rp_recv, ry_send, ry_recv,
):
    lat = lax.axis_index("lat")
    lon = lax.axis_index("lon")
    zi, xi = lon // NX, lon % NX
    core, yi = lat % 2, lat // 2
    top = lat == LAT - 1
    bottom = lat == 0
    north, south = (lat + 1) % LAT, (lat + LAT - 1) % LAT
    east, west = (lon + 1) % LON, (lon + LON - 1) % LON
    barrier = pltpu.get_barrier_semaphore()

    loads = [
        pltpu.make_async_copy(depth_ref, depth_buf, local_sem.at[0]),
        pltpu.make_async_copy(mask_ref, mask_buf, local_sem.at[1]),
        pltpu.make_async_copy(forcing_ref, raw_m.at[1, pl.ds(16, ROWS), :], local_sem.at[2]),
        pltpu.make_async_copy(search_ref, raw_m.at[2, pl.ds(16, ROWS), :], local_sem.at[3]),
        pltpu.make_async_copy(fold_ref.at[pl.ds(0, 1024)], fold_buf, local_sem.at[4]),
    ]
    for copy in loads:
        copy.start()

    def greet(semaphore, to):
        for a, b in to:
            pl.semaphore_signal(
                semaphore, inc=1, device_id={"lat": a, "lon": b}, device_id_type=pl.DeviceIdType.MESH
            )

    def around(far):
        if 2 * far == NZ:
            return [(lat, (lon + NX * far) % LON)]
        to = [(lat, (lon + NX * far) % LON), (lat, (lon + LON - NX * far) % LON)]
        if 2 * far < LAT:
            to += [((lat + 2 * far) % LAT, lon), ((lat + LAT - 2 * far) % LAT, lon)]
        return to

    beside = [(lat, zi * NX + (xi + d) % NX) for d in far_first(NX)]
    beside += [(north, east), (north, west), (south, east), (south, west)]
    beside += [(lat, east), (lat, west), (north, lon), (south, lon)] + around(1)

    beside += [(lat + 1 - 2 * core, zi * NX + (xi + d) % NX) for d in far_first(NX)]
    greet(barrier, beside)

    levels = 3

    def next_level(level):
        if level > 0:
            pl.semaphore_wait(plane_sem.at[level - 1], len(around(1 << (level - 1))))
        if level < levels:
            greet(plane_sem.at[level], around(1 << level))

    rows_acc[...] = jnp.zeros_like(rows_acc)
    b_m[HALF + 2] = jnp.zeros((EXT, COLS), F32)
    b_s[STEPS + 2] = jnp.zeros((EXT, COLS), F32)
    for copy in loads:
        copy.wait()
    raw_m[0, 16 : 16 + ROWS, :] = depth_buf[...] * mask_buf[...].astype(F32)

    pivot = fold_buf[0]
    pivot_block, pivot_lane = lax.shift_right_logical(pivot, 7), pivot & (COLS - 1)

    @pl.when(top)
    def _():
        fold_x[...] = jnp.zeros_like(fold_x)
        for m in range(9):
            fold_x[m : m + 1, :] = raw_m[0, 175 - m : 176 - m, :]
        for m in range(8):
            fold_x[9 + m : 10 + m, :] = raw_m[1, 175 - m : 176 - m, :]
            fold_x[17 + m : 18 + m, :] = raw_m[2, 175 - m : 176 - m, :]
        source = lax.broadcasted_iota(jnp.int32, (COLS, COLS), 0)
        target = lax.broadcasted_iota(jnp.int32, (COLS, COLS), 1)
        choose = (source == ((pivot - target) & (COLS - 1))).astype(F32)
        turned = jnp.dot(fold_x[...], choose, precision=HIGHEST, preferred_element_type=F32)
        fold_src[...] = turned
        fold_row[xi] = turned
        fold_row[NX] = jnp.zeros_like(turned)

    lane40 = lanes_of((40, COLS))
    acc_w = jnp.zeros((40, COLS), F32)
    acc_e = jnp.zeros((40, COLS), F32)
    for g in range(4):
        for f in range(3):
            at = 32 * g + 9 * f
            block = raw_m[f, 16 + 40 * g : 56 + 40 * g, :]
            here = (lane40 >= at) & (lane40 < at + 9)
            acc_w = jnp.where(here, pltpu.roll(block, at, 1) if at else block, acc_w)
            acc_e = jnp.where(here, pltpu.roll(block, (at - 119) % COLS, 1), acc_e)
    pack_w[...] = acc_w
    pack_e[...] = acc_e

    pl.semaphore_wait(barrier, len(beside))

    fold_x_copies = [
        remote(fold_src, fold_row.at[xi], fx_send.at[d - 1], fx_recv.at[d - 1], lat, zi * NX + (xi + d) % NX)
        for d in range(1, NX)
    ]

    @pl.when(top)
    def _():
        for d in far_first(NX):
            fold_x_copies[d - 1].start()

    to_north = remote(raw_m.at[:, pl.ds(160, 16), :], raw_m.at[:, pl.ds(0, 16), :],
                      halo_send.at[0], halo_recv.at[0], north, lon)
    to_south = remote(raw_m.at[:, pl.ds(16, 16), :], raw_m.at[:, pl.ds(176, 16), :],
                      halo_send.at[1], halo_recv.at[1], south, lon)
    to_east = remote(pack_e, got_w, halo_send.at[2], halo_recv.at[2], lat, east)
    to_west = remote(pack_w, got_e, halo_send.at[3], halo_recv.at[3], lat, west)
    to_ne = remote(pack_e.at[pl.ds(24, 16), :], corner.at[0], halo_send.at[4], halo_recv.at[4], north, east)
    to_nw = remote(pack_w.at[pl.ds(24, 16), :], corner.at[1], halo_send.at[5], halo_recv.at[5], north, west)
    to_se = remote(pack_e.at[pl.ds(0, 16), :], corner.at[2], halo_send.at[6], halo_recv.at[6], south, east)
    to_sw = remote(pack_w.at[pl.ds(0, 16), :], corner.at[3], halo_send.at[7], halo_recv.at[7], south, west)

    to_east.start()
    to_west.start()
    next_level(0)

    @pl.when(jnp.logical_not(top))
    def _():
        to_ne.start()
        to_nw.start()
        to_north.start()

    @pl.when(jnp.logical_not(bottom))
    def _():
        to_se.start()
        to_sw.start()
        to_south.start()

    fold_z_copies = [
        remote(fold_send.at[d], fold_got.at[zi], fz_send.at[d - 1], fz_recv.at[d - 1],
               lat, ((zi + d) % NZ) * NX + xi)
        for d in range(1, NZ)
    ]
    lane32 = lanes_of((32, COLS))
    near = lane32 <= pivot_lane

    @pl.when(top)
    def _():
        next_level(1)
        next_level(2)
        for copy in fold_x_copies:
            copy.wait_recv()
        for d in far_first(NZ) + [0]:
            want = pivot_block - ((zi + d) % NZ) * NX - xi

            def block(b):
                mine = (lax.shift_right_logical(b & (LON - 1), 2) == zi)
                return fold_row[jnp.where(mine, b & (NX - 1), NX)]

            ahead, here, behind, beyond = (block(want + o) for o in (1, 0, -1, -2))
            window = jnp.where(near, here, behind)
            edge = jnp.where(
                lane32 < 9, jnp.where(near, behind, beyond),
                jnp.where(lane32 >= 119, jnp.where(near, ahead, here), 0.0),
            )
            edges = sum(pltpu.roll(edge[8 * g : 8 * g + 8], 16 + 32 * g, 1) for g in range(4))
            if d:
                fold_send[d, 0:32, :] = window
                fold_send[d, 32:40, :] = edges
            else:
                fold_got[zi, 0:32, :] = window
                fold_got[zi, 32:40, :] = edges
        for d in far_first(NZ):
            fold_z_copies[d - 1].start()

    def own_strips(spans):
        for r, n in spans:
            depth, residual, search = (raw_m[f, r : r + n, :] for f in range(3))
            lane = lanes_of((n, COLS))
            west_p, east_r, west_r = (within(lane, a, a + 18) for a in (WEST, 46, WEST + 64))
            east_p = lane >= 110
            for ref, p, q in ((side_depth, depth, depth), (side_state, search, residual)):
                ref[r : r + n, :] = jnp.where(
                    east_p, p, jnp.where(west_p, shift(p, WEST), jnp.where(
                        east_r, shift(q, 64), jnp.where(west_r, shift(q, WEST + 64), 0.0))))

    def far_strips(r, n, from_e, from_w, places):
        lane = lanes_of((n, COLS))
        west_p, east_r, west_r = (within(lane, a, a + 9) for a in (WEST - 9, 64, WEST + 55))
        east_p = lane < 9
        at_d, at_r, at_p = places
        for ref, p, q in ((side_depth, at_d, at_d), (side_state, at_p, at_r)):
            ref[r : r + n, :] = jnp.where(
                east_p, shift(from_e, -p), jnp.where(west_p, shift(from_w, WEST - 9 - p), jnp.where(
                    east_r, shift(from_e, 64 - q), jnp.where(
                        west_r, shift(from_w, WEST + 55 - q), ref[r : r + n, :]))))

    kinds = {
        "m": (raw_m.at[0], s_m, de_m, se_m, w_m),
        "s": (side_depth, s_s, de_s, se_s, w_s),
    }

    def fields(kind, spans):
        for r, n in spans:
            wet = (kinds[kind][0][r : r + n, :] > 0.0).astype(F32)
            if kind == "m":
                for slot, half, source in ((0, HALF, 2), (FIRST, HALF + 1, 1)):
                    value = wet * raw_m[source, r : r + n, :]
                    b_m[slot, r : r + n, :] = value
                    b_m[half, r : r + n, :] = 0.5 * value
            else:
                value = wet * side_state[r : r + n, :]
                b_s[0, r : r + n, :] = value
                b_s[STEPS + 1, r : r + n, :] = 0.5 * value

    def roots(kind, spans):
        depth_ref_, s, de, se, _ = kinds[kind]
        for r, n in spans:
            up, depth, low = (depth_ref_[r + o : r + o + n, :] for o in (1, 0, -1))
            both = up + low
            column = depth + 0.5 * both
            wet_up, wet, wet_low = ((v > 0.0).astype(F32) for v in (up, depth, low))
            both_wet = wet_up + wet_low
            column_wet = wet + 0.5 * both_wet
            all_depth = both + (from_east(column) + from_west(column))
            all_wet = both_wet + (from_east(column_wet) + from_west(column_wet))
            total = 0.5 * (depth * all_wet + all_depth)
            diagonal = wet * (depth * (1.0 / (REACH * REACH)) + total) + (1.0 - wet)
            root = wet * lax.rsqrt(diagonal)
            s[r : r + n, :] = root
            se[r : r + n, :] = from_east(root)
            de[r : r + n, :] = from_east(depth)

    def links(kind, spans):
        depth_ref_, s, de, se, w = kinds[kind]
        for r, n in spans:
            d0, d1 = depth_ref_[r : r + n, :], depth_ref_[r + 1 : r + 1 + n, :]
            s0, s1 = s[r : r + n, :], s[r + 1 : r + 1 + n, :]
            de0, de1 = de[r : r + n, :], de[r + 1 : r + 1 + n, :]
            se0, se1 = se[r : r + n, :], se[r + 1 : r + 1 + n, :]
            east_w = -(d0 + de0) * (s0 * se0)
            ne_w = -0.5 * (d0 + de1) * (s0 * se1)
            nw_e = -0.5 * (de0 + d1) * (se0 * s1)
            w[0, r : r + n, :] = -(d0 + d1) * (s0 * s1)
            w[1, r : r + n, :] = east_w
            w[2, r : r + n, :] = from_west(east_w)
            w[3, r : r + n, :] = ne_w
            w[4, r : r + n, :] = from_west(ne_w)
            w[5, r : r + n, :] = from_west(nw_e)
            w[6, r : r + n, :] = nw_e

    def fold8(x):
        return sum(x[8 * k : 8 * k + 8] for k in range(x.shape[0] // 8))

    lane1 = lanes_of((1, COLS))
    main_lanes = within(lane1, 9, 119)
    strips_p, strips_r = strip_lanes(lane1, 0), strip_lanes(lane1, 64)

    def apply(b, k, w, r, size):
        up, mid, low = (b[k, r + o : r + o + size, :] for o in (1, 0, -1))
        a_u, a_d, e_u, e_c, e_d, f_u, f_c, f_d = w
        east_part = from_east(e_u * up + e_c * mid + e_d * low)
        west_part = from_west(f_u * up + f_c * mid + f_d * low)
        return mid, (a_u * up + a_d * low) + (east_part + west_part)

    def step(n, tasks):
        first = n == 1
        total = {}

        def add(key, product, lo, hi):
            value = fold8(product[lo:hi])
            total[key] = total[key] + value if key in total else value

        for kind, r, size, gram_lo, gram_hi in tasks:
            w = kinds[kind][4]
            weights = (
                w[0, r : r + size, :], w[0, r - 1 : r - 1 + size, :],
                w[4, r : r + size, :], w[2, r : r + size, :], w[5, r - 1 : r - 1 + size, :],
                w[6, r : r + size, :], w[1, r : r + size, :], w[3, r - 1 : r - 1 + size, :],
            )
            if kind == "s":
                b, starts, zero = b_s, ((0, STEPS + 1),), STEPS + 2
            else:
                b, starts, zero = b_m, ((0, HALF), (FIRST, HALF + 1)), HALF + 2
            news, olds = [], []
            for base, half in starts:
                mid, out = apply(b, jnp.where(first, half, base + n - 1), weights, r, size)
                out = out - b[jnp.where(first, zero, base + n - 2), r : r + size, :]
                b[base + n, r : r + size, :] = out
                news.append(out)
                olds.append(mid)
            lo, hi = max(r, gram_lo) - r, min(r + size, gram_hi) - r
            if hi <= lo:
                continue
            p1, p0 = news[0], olds[0]
            if kind == "s":
                add("s0", p1 * p1, lo, hi)
                add("s1", p1 * p0, lo, hi)
                add("s4", p1 * shift(p1, 64), lo, hi)
                add("s5", p1 * shift(p0, 64), lo, hi)
                continue
            r1, r0 = news[1], olds[1]
            for c, product in enumerate((p1 * p1, p1 * p0, r1 * r1, r1 * r0, p1 * r1, p1 * r0)):
                add("m%d" % c, product, lo, hi)
        gather(n, total, jnp.where(first, 2.0, 1.0))

    def gather(n, total, scale):
        rows = {key: jnp.sum(value, axis=0, keepdims=True) for key, value in total.items()}
        for c in range(6):
            row = jnp.zeros((1, COLS), F32)
            if "m%d" % c in rows:
                row = jnp.where(main_lanes, rows["m%d" % c], row)
            source = "s%d" % (c - 2 if c in (2, 3) else c)
            if source in rows:
                row = row + jnp.where(strips_r if c in (2, 3) else strips_p, rows[source], 0.0)
            if c % 2:
                row = row * scale
            at = pl.ds(6 * n + c, 1)
            rows_acc[at, :] = rows_acc[at, :] + row

    def steps(tasks):
        @pl.loop(1, STEPS + 1)
        def _(n):
            step(n, tasks)

    def tasks(kind, start, stop, gram_lo, gram_hi):
        return [(kind, r, n, gram_lo, gram_hi) for r, n in chunks(start, stop)]

    own_strips(chunks(16, 176))
    fields("m", chunks(16, 176))
    roots("m", [(17, 7)] + chunks(24, 168) + [(168, 7)])
    links("m", chunks(16, 168))

    @pl.when(jnp.logical_not(top))
    def _():
        next_level(1)

    start = {}
    for r, n in chunks(16, 176):
        p0, r0 = b_m[0, r : r + n, :], b_m[FIRST, r : r + n, :]
        for key, value in (("m0", p0 * p0), ("m2", r0 * r0), ("m4", p0 * r0)):
            start[key] = start[key] + fold8(value) if key in start else fold8(value)
    gather(0, start, 1.0)

    @pl.when(jnp.logical_not(top))
    def _():
        next_level(2)

    steps(tasks("m", 16, 168, 32, 160))

    to_east.wait()
    to_west.wait()
    for g in range(4):
        at = 32 * g
        far_strips(16 + 40 * g, 40, got_e[...], got_w[...], (at, at + 9, at + 18))
    fields("s", chunks(16, 176))
    start = {}
    for r, n in chunks(16, 176):
        p0 = b_s[0, r : r + n, :]
        for key, value in (("s0", p0 * p0), ("s4", p0 * shift(p0, 64))):
            start[key] = start[key] + fold8(value) if key in start else fold8(value)
    gather(0, start, 1.0)

    roots("s", [(17, 7)] + chunks(24, 168) + [(168, 7)])
    links("s", chunks(16, 168))
    steps(tasks("s", 16, 168, 32, 160))

    @pl.when(jnp.logical_not(bottom))
    def _():
        to_se.wait_send()
        to_sw.wait_send()
        to_south.wait_send()
        to_ne.wait_recv()
        to_nw.wait_recv()
        to_north.wait_recv()
        own_strips([(0, 16)])
        far_strips(0, 16, corner[1], corner[0], (96, 105, 114))

    @pl.when(bottom)
    def _():
        for f in range(3):
            raw_m[f, 0:16, :] = jnp.zeros((16, COLS), F32)
        side_depth[0:16, :] = jnp.zeros((16, COLS), F32)
        side_state[0:16, :] = jnp.zeros((16, COLS), F32)

    @pl.when(jnp.logical_not(top))
    def _():
        to_ne.wait_send()
        to_nw.wait_send()
        to_north.wait_send()
        to_se.wait_recv()
        to_sw.wait_recv()
        to_south.wait_recv()
        own_strips([(176, 16)])
        far_strips(176, 16, corner[3], corner[2], (0, 9, 18))

    @pl.when(top)
    def _():
        for copy in fold_z_copies:
            copy.wait_recv()
        ghost = fold_got[0]
        for k in range(1, NZ):
            ghost = ghost + fold_got[k]
        edges = ghost[32:40]
        lane8 = lanes_of((8, COLS))
        side = []
        for g in range(4):
            edge = pltpu.roll(edges, (COLS - 16 - 32 * g) % COLS, 1)
            side.append(jnp.where((lane8 < 9) | (lane8 >= 119), edge, 0.0))
        side = jnp.concatenate(side, axis=0)
        for f in range(3):
            raw_m[f, 176:192, :] = jnp.zeros((16, COLS), F32)
        raw_m[0, 176:185, :] = ghost[0:9]
        raw_m[1, 176:184, :] = ghost[9:17]
        raw_m[2, 176:184, :] = ghost[17:25]
        own_strips([(176, 16)])
        fold_x[...] = side
        west_p, west_r, east_r = (within(lane1, a, a + 9) for a in (WEST - 9, WEST + 55, 64))
        for ref, p, q, count in ((side_depth, 0, 0, 9), (side_state, 17, 9, 8)):
            one, two = fold_x[p : p + count, :], fold_x[q : q + count, :]
            ref[176 : 176 + count, :] = jnp.where(
                lane1 < 9, one, jnp.where(west_p, shift(one, WEST), jnp.where(
                    east_r, shift(two, 64), jnp.where(
                        west_r, shift(two, WEST + 64), ref[176 : 176 + count, :]))))
        for copy in fold_x_copies + fold_z_copies:
            copy.wait_send()

    for kind in ("m", "s"):
        fields(kind, [(LO, 8), (176, 8)])
        roots(kind, [(LO, 16), (168, 16)])
        links(kind, [(LO, 16), (168, 16)])
    steps([(kind, r, 24, lo, lo + 16) for kind in ("m", "s") for r, lo in ((LO, 16), (160, 160))])

    ones = jnp.ones((8, COLS), F32)
    sums = lax.dot_general(
        ones, rows_acc[...], (((1,), (1,)), ((), ())), precision=HIGHEST, preferred_element_type=F32
    )[0:1]

    def tree(terms):
        while len(terms) > 1:
            terms = [a + b for a, b in zip(terms[::2], terms[1::2])]
        return terms[0]

    second = core == 1
    part[0] = sums
    next_level(levels)
    to_plane = [
        remote(part.at[0], red_p.at[core * LON + lon], rp_send.at[d], rp_recv.at[core * LON + d],
               2 * yi + 1, (lon + d) % LON)
        for d in range(LON)
    ]
    for d in far_first(LON):
        to_plane[d].start()
    count = LAT // 2
    along_y = [(d, c) for d in far_first(count) + [0] for c in (1, 0) if (d, c) != (0, 1)]
    to_lat = [
        remote(part.at[1], red_y.at[yi], ry_send.at[2 * d + c], ry_recv.at[d],
               2 * ((yi + d) % count) + c, lon)
        for d, c in along_y
    ]

    @pl.when(jnp.logical_not(second))
    def _():
        to_plane[0].start()
        to_plane[0].wait_send()

    @pl.when(second)
    def _():
        red_p[LON + lon] = sums
        for c in range(2):
            for d in range(c, LON):
                remote(part.at[0], red_p.at[c * LON + lon], rp_send.at[d], rp_recv.at[c * LON + d],
                       lat, east).wait_recv()
        total = tree([red_p[k] for k in range(2 * LON)])
        part[1] = total
        red_y[yi] = total
        for copy in to_lat:
            copy.start()

    def arrived(d):
        remote(part.at[1], red_y.at[yi], ry_send.at[0], ry_recv.at[d], lat, east).wait_recv()

    @pl.when(jnp.logical_not(second))
    def _():
        arrived(0)

    for d in range(1, count):
        arrived(d)
    moments_out[...] = tree([red_y[k] for k in range(count)])

    @pl.when(second)
    def _():
        for copy in to_lat:
            copy.wait_send()

    for copy in to_plane[1:]:
        copy.wait_send()


def held(shape):
    return pltpu.VMEM(shape, F32)


def basis_and_moments(forcing, search, depth, mask, fold_map):
    vm = pltpu.VMEM
    dma = pltpu.SemaphoreType.DMA
    ext = (EXT, COLS)
    return pl.pallas_call(
        basis_kernel,
        out_shape=(held((HALF + 3,) + ext), held((STEPS + 3,) + ext), held((1, COLS))),
        in_specs=[pl.BlockSpec(memory_space=pl.ANY)] * 5,
        out_specs=(pl.BlockSpec(memory_space=vm),) * 3,
        scratch_shapes=[
            pltpu.SMEM((1024,), jnp.int32),
            vm((3,) + ext, F32), vm(ext, F32), vm(ext, F32),
            vm((ROWS, COLS), F32), vm((ROWS, COLS), jnp.int32),
            vm((40, COLS), F32), vm((40, COLS), F32), vm((40, COLS), F32), vm((40, COLS), F32),
            vm((4, 16, COLS), F32),
            vm((32, COLS), F32), vm((32, COLS), F32), vm((NX + 1, 32, COLS), F32),
            vm((NZ, 40, COLS), F32), vm((NZ, 40, COLS), F32),
        ]
        + [vm(ext, F32)] * 6
        + [vm((7,) + ext, F32)] * 2
        + [
            vm((COLS, COLS), F32), vm((2, 1, COLS), F32),
            vm((2 * LON, 1, COLS), F32), vm((LAT // 2, 1, COLS), F32),
            pltpu.SemaphoreType.REGULAR((4,)), dma((5,)), dma((8,)), dma((8,)),
            dma((NZ - 1,)), dma((NZ - 1,)), dma((NX - 1,)), dma((NX - 1,)),
            dma((LON,)), dma((2 * LON,)), dma((LAT,)), dma((LAT // 2,)),
        ],
        compiler_params=pltpu.CompilerParams(collective_id=0, has_side_effects=True),
        name="basis",
    )(fold_map, forcing, search, depth, mask)


def rows_of(shape):
    return lax.broadcasted_iota(jnp.int32, shape, 0)


def applied_to_coords(c):
    row = rows_of(c.shape)
    below = jnp.where(row == 0, 0.0, jnp.where(row == 1, 1.0, 0.5)).astype(F32)
    above = jnp.where(row == c.shape[0] - 1, 0.0, 0.5).astype(F32)
    return c + below * pltpu.roll(c, 1, 0) + above * pltpu.roll(c, c.shape[0] - 1, 0)


def applied_to_moments(m):
    row = rows_of(m.shape)
    up, down = pltpu.roll(m, m.shape[0] - 1, 0), pltpu.roll(m, 1, 0)
    return m + 0.5 * (up + jnp.where(row == 0, up, down))


def moment_rows(raw, kind, count):
    k = rows_of((count, COLS))
    odd = k & 1
    high = jnp.minimum(6 * ((k + 1) >> 1) + 2 * kind + odd, COLS - 1)
    spread = jnp.broadcast_to(raw, (count, COLS))
    base = jnp.where(odd == 1, 7 + 2 * kind, 2 * kind)
    return 2.0 * jnp.take_along_axis(spread, high, axis=1) - jnp.take_along_axis(spread, base, axis=1)


def dot_rows(coords, moments):
    (cp, cr), (mp, mr) = coords, moments
    products = cp * mp[0:16]
    return jnp.sum(products[0:8] + products[8:16] + cr * mr[0:8], axis=0, keepdims=True)


def pair(function, one, two):
    return tuple(function(a, b) for a, b in zip(one, two))


def coordinates(raw):
    search_search = moment_rows(raw, 0, 24)
    residual_residual = moment_rows(raw, 1, 16)
    mixed_long, mixed = moment_rows(raw, 2, 24), moment_rows(raw, 2, 16)
    first16 = (rows_of((16, COLS)) == 0).astype(F32)
    first8 = (rows_of((8, COLS)) == 0).astype(F32)
    p, pm = (first16, jnp.zeros((8, COLS), F32)), (search_search, mixed)
    r, rm = (jnp.zeros((16, COLS), F32), first8), (mixed_long, residual_residual)
    x = (jnp.zeros((16, COLS), F32), jnp.zeros((8, COLS), F32))
    q, qm = tuple(map(applied_to_coords, p)), tuple(map(applied_to_moments, pm))
    norm, curvature = dot_rows(r, rm), dot_rows(p, qm)
    for inner in range(STEPS):
        t = norm / curvature
        x = pair(lambda a, b: a + t * b, x, p)
        r = pair(lambda a, b: a - t * b, r, q)
        if inner == STEPS - 1:
            break
        rm = pair(lambda a, b: a - t * b, rm, qm)
        am = tuple(map(applied_to_moments, rm))
        fresh, own, cross = dot_rows(r, rm), dot_rows(r, am), dot_rows(p, am)
        beta = fresh / norm
        curvature = own + beta * (2.0 * cross + beta * curvature)
        norm = fresh
        p = pair(lambda a, b: a + beta * b, r, p)
        q = tuple(map(applied_to_coords, p))
        qm = pair(lambda a, b: a + beta * b, am, qm)
    return x, r


def combine_kernel(moments_ref, basis_ref, strips_ref, height_ref, residual_ref):
    found = coordinates(moments_ref[...])
    lane1 = lanes_of((1, COLS))
    search_half = within((lane1 + 32) & (COLS - 1), 14, 78)
    size = 32
    for (of_p, of_r), out_ref in zip(found, (height_ref, residual_ref)):
        coords = [of_p[k : k + 1, :] for k in range(FIRST)] + [of_r[k : k + 1, :] for k in range(STEPS)]
        mixed = []
        for n in range(STEPS + 1):
            other = coords[FIRST + n] if n < STEPS else jnp.zeros((1, COLS), F32)
            mixed.append(jnp.where(search_half, coords[n], other))
        for at in range(0, ROWS, size):
            rows = slice(16 + at, 16 + at + size)
            main = sum(coords[k] * basis_ref[k, rows, :] for k in range(FIELDS))
            strip = sum(mixed[n] * strips_ref[n, rows, :] for n in range(STEPS + 1))
            strip = strip + shift(strip, 64)
            out_ref[at : at + size, :] = jnp.where(
                lane1 >= 119, strip, jnp.where(lane1 < 9, shift(strip, -WEST), main)
            )


def per_device(forcing, search, depth, mask, fold_map):
    made = basis_and_moments(forcing, search, depth, mask, fold_map)
    basis, strips, moments = (pltpu.with_memory_space_constraint(v, pltpu.VMEM) for v in made)
    block = jax.ShapeDtypeStruct((ROWS, COLS), F32)
    return pl.pallas_call(
        combine_kernel,
        out_shape=(block, block),
        in_specs=[pl.BlockSpec(memory_space=pltpu.VMEM)] * 3,
        name="combine",
    )(moments, basis, strips)


def solution(mesh):
    return jax.shard_map(
        per_device,
        mesh=mesh,
        in_specs=(P("lat", "lon"),) * 4 + (P(),),
        out_specs=(P("lat", "lon"),) * 2,
        check_vma=False,
    )
```

```python
import functools

import jax
import jax.numpy as jnp
from jax import lax
from jax.experimental import pallas as pl
from jax.experimental.pallas import tpu as pltpu
from jax.sharding import PartitionSpec as P

STEPS = 8
REACH = 256
LAT, LON, NX, NZ = 16, 32, 4, 8
ROWS, COLS = 160, 128
EXT = ROWS + 32
LO = 8
FIELDS = 2 * STEPS + 1
FIRST = STEPS + 1
HIGHEST = lax.Precision.HIGHEST
F32 = jnp.float32


def lanes_of(shape):
    return lax.broadcasted_iota(jnp.int32, shape, len(shape) - 1)


def from_east(x):
    return pltpu.roll(x, COLS - 1, 1)


def from_west(x):
    return pltpu.roll(x, 1, 1)


def shift(x, by):
    by %= COLS
    return pltpu.roll(x, by, 1) if by else x


WEST = 28


def strip_lanes(lane, half):
    lane = (lane - half) & (COLS - 1)
    return (lane >= 119) | ((lane >= WEST) & (lane < WEST + 9))


def within(lane, start, stop):
    return (lane >= start) & (lane < stop)


def remote(src, dst, send, recv, lat, lon):
    return pltpu.make_async_remote_copy(
        src_ref=src,
        dst_ref=dst,
        send_sem=send,
        recv_sem=recv,
        device_id={"lat": lat, "lon": lon},
        device_id_type=pl.DeviceIdType.MESH,
    )


CHUNK = 16


def far_first(count):
    return sorted(range(1, count), key=lambda d: (-min(d, count - d), d))


def chunks(start, stop):
    return [(r, min(CHUNK, stop - r)) for r in range(start, stop, CHUNK)]


def basis_kernel(
    fold_ref, forcing_ref, search_ref, depth_ref, mask_ref,
    b_m, b_s, moments_out,
    fold_buf, raw_m, side_depth, side_state, depth_buf, mask_buf, pack_w, pack_e, got_w, got_e, corner,
    fold_x, fold_src, fold_row, fold_send, fold_got,
    s_m, s_s, de_m, de_s, se_m, se_s,
    w_m, w_s, rows_acc, part, red_p, red_y,
    plane_sem, local_sem, halo_send, halo_recv, fz_send, fz_recv, fx_send, fx_recv,
    rp_send, rp_recv, ry_send, ry_recv,
):
    lat = lax.axis_index("lat")
    lon = lax.axis_index("lon")
    zi, xi = lon // NX, lon % NX
    core, yi = lat % 2, lat // 2
    top = lat == LAT - 1
    bottom = lat == 0
    north, south = (lat + 1) % LAT, (lat + LAT - 1) % LAT
    east, west = (lon + 1) % LON, (lon + LON - 1) % LON
    barrier = pltpu.get_barrier_semaphore()

    loads = [
        pltpu.make_async_copy(depth_ref, depth_buf, local_sem.at[0]),
        pltpu.make_async_copy(mask_ref, mask_buf, local_sem.at[1]),
        pltpu.make_async_copy(forcing_ref, raw_m.at[1, pl.ds(16, ROWS), :], local_sem.at[2]),
        pltpu.make_async_copy(search_ref, raw_m.at[2, pl.ds(16, ROWS), :], local_sem.at[3]),
        pltpu.make_async_copy(fold_ref.at[pl.ds(0, 1024)], fold_buf, local_sem.at[4]),
    ]
    for copy in loads:
        copy.start()

    def greet(semaphore, to):
        for a, b in to:
            pl.semaphore_signal(
                semaphore, inc=1, device_id={"lat": a, "lon": b}, device_id_type=pl.DeviceIdType.MESH
            )

    def around(far):
        if 2 * far == NZ:
            return [(lat, (lon + NX * far) % LON)]
        to = [(lat, (lon + NX * far) % LON), (lat, (lon + LON - NX * far) % LON)]
        if 2 * far < LAT:
            to += [((lat + 2 * far) % LAT, lon), ((lat + LAT - 2 * far) % LAT, lon)]
        return to

    beside = [(lat, zi * NX + (xi + d) % NX) for d in far_first(NX)]
    beside += [(north, east), (north, west), (south, east), (south, west)]
    beside += [(lat, east), (lat, west), (north, lon), (south, lon)] + around(1)

    beside += [(lat + 1 - 2 * core, zi * NX + (xi + d) % NX) for d in far_first(NX)]
    greet(barrier, beside)

    levels = 3

    def next_level(level):
        if level > 0:
            pl.semaphore_wait(plane_sem.at[level - 1], len(around(1 << (level - 1))))
        if level < levels:
            greet(plane_sem.at[level], around(1 << level))

    rows_acc[...] = jnp.zeros_like(rows_acc)
    for copy in loads:
        copy.wait()
    raw_m[0, 16 : 16 + ROWS, :] = depth_buf[...] * mask_buf[...].astype(F32)

    pivot = fold_buf[0]
    pivot_block, pivot_lane = lax.shift_right_logical(pivot, 7), pivot & (COLS - 1)

    @pl.when(top)
    def _():
        fold_x[...] = jnp.zeros_like(fold_x)
        for m in range(9):
            fold_x[m : m + 1, :] = raw_m[0, 175 - m : 176 - m, :]
        for m in range(8):
            fold_x[9 + m : 10 + m, :] = raw_m[1, 175 - m : 176 - m, :]
            fold_x[17 + m : 18 + m, :] = raw_m[2, 175 - m : 176 - m, :]
        source = lax.broadcasted_iota(jnp.int32, (COLS, COLS), 0)
        target = lax.broadcasted_iota(jnp.int32, (COLS, COLS), 1)
        choose = (source == ((pivot - target) & (COLS - 1))).astype(F32)
        turned = jnp.dot(fold_x[...], choose, precision=HIGHEST, preferred_element_type=F32)
        fold_src[...] = turned
        fold_row[xi] = turned
        fold_row[NX] = jnp.zeros_like(turned)

    lane40 = lanes_of((40, COLS))
    acc_w = jnp.zeros((40, COLS), F32)
    acc_e = jnp.zeros((40, COLS), F32)
    for g in range(4):
        for f in range(3):
            at = 32 * g + 9 * f
            block = raw_m[f, 16 + 40 * g : 56 + 40 * g, :]
            here = (lane40 >= at) & (lane40 < at + 9)
            acc_w = jnp.where(here, pltpu.roll(block, at, 1) if at else block, acc_w)
            acc_e = jnp.where(here, pltpu.roll(block, (at - 119) % COLS, 1), acc_e)
    pack_w[...] = acc_w
    pack_e[...] = acc_e

    pl.semaphore_wait(barrier, len(beside))

    fold_x_copies = [
        remote(fold_src, fold_row.at[xi], fx_send.at[d - 1], fx_recv.at[d - 1], lat, zi * NX + (xi + d) % NX)
        for d in range(1, NX)
    ]

    @pl.when(top)
    def _():
        for d in far_first(NX):
            fold_x_copies[d - 1].start()

    to_north = remote(raw_m.at[:, pl.ds(160, 16), :], raw_m.at[:, pl.ds(0, 16), :],
                      halo_send.at[0], halo_recv.at[0], north, lon)
    to_south = remote(raw_m.at[:, pl.ds(16, 16), :], raw_m.at[:, pl.ds(176, 16), :],
                      halo_send.at[1], halo_recv.at[1], south, lon)
    to_east = remote(pack_e, got_w, halo_send.at[2], halo_recv.at[2], lat, east)
    to_west = remote(pack_w, got_e, halo_send.at[3], halo_recv.at[3], lat, west)
    to_ne = remote(pack_e.at[pl.ds(24, 16), :], corner.at[0], halo_send.at[4], halo_recv.at[4], north, east)
    to_nw = remote(pack_w.at[pl.ds(24, 16), :], corner.at[1], halo_send.at[5], halo_recv.at[5], north, west)
    to_se = remote(pack_e.at[pl.ds(0, 16), :], corner.at[2], halo_send.at[6], halo_recv.at[6], south, east)
    to_sw = remote(pack_w.at[pl.ds(0, 16), :], corner.at[3], halo_send.at[7], halo_recv.at[7], south, west)

    to_east.start()
    to_west.start()
    next_level(0)

    @pl.when(jnp.logical_not(top))
    def _():
        to_ne.start()
        to_nw.start()
        to_north.start()

    @pl.when(jnp.logical_not(bottom))
    def _():
        to_se.start()
        to_sw.start()
        to_south.start()

    fold_z_copies = [
        remote(fold_send.at[d], fold_got.at[zi], fz_send.at[d - 1], fz_recv.at[d - 1],
               lat, ((zi + d) % NZ) * NX + xi)
        for d in range(1, NZ)
    ]
    lane32 = lanes_of((32, COLS))
    near = lane32 <= pivot_lane

    @pl.when(top)
    def _():
        next_level(1)
        next_level(2)
        for copy in fold_x_copies:
            copy.wait_recv()
        for d in far_first(NZ) + [0]:
            want = pivot_block - ((zi + d) % NZ) * NX - xi

            def block(b):
                mine = (lax.shift_right_logical(b & (LON - 1), 2) == zi)
                return fold_row[jnp.where(mine, b & (NX - 1), NX)]

            ahead, here, behind, beyond = (block(want + o) for o in (1, 0, -1, -2))
            window = jnp.where(near, here, behind)
            edge = jnp.where(
                lane32 < 9, jnp.where(near, behind, beyond),
                jnp.where(lane32 >= 119, jnp.where(near, ahead, here), 0.0),
            )
            edges = sum(pltpu.roll(edge[8 * g : 8 * g + 8], 16 + 32 * g, 1) for g in range(4))
            if d:
                fold_send[d, 0:32, :] = window
                fold_send[d, 32:40, :] = edges
            else:
                fold_got[zi, 0:32, :] = window
                fold_got[zi, 32:40, :] = edges
        for d in far_first(NZ):
            fold_z_copies[d - 1].start()

    def own_strips(spans):
        for r, n in spans:
            depth, residual, search = (raw_m[f, r : r + n, :] for f in range(3))
            lane = lanes_of((n, COLS))
            west_p, east_r, west_r = (within(lane, a, a + 18) for a in (WEST, 46, WEST + 64))
            east_p = lane >= 110
            for ref, p, q in ((side_depth, depth, depth), (side_state, search, residual)):
                ref[r : r + n, :] = jnp.where(
                    east_p, p, jnp.where(west_p, shift(p, WEST), jnp.where(
                        east_r, shift(q, 64), jnp.where(west_r, shift(q, WEST + 64), 0.0))))

    def far_strips(r, n, from_e, from_w, places):
        lane = lanes_of((n, COLS))
        west_p, east_r, west_r = (within(lane, a, a + 9) for a in (WEST - 9, 64, WEST + 55))
        east_p = lane < 9
        at_d, at_r, at_p = places
        for ref, p, q in ((side_depth, at_d, at_d), (side_state, at_p, at_r)):
            ref[r : r + n, :] = jnp.where(
                east_p, shift(from_e, -p), jnp.where(west_p, shift(from_w, WEST - 9 - p), jnp.where(
                    east_r, shift(from_e, 64 - q), jnp.where(
                        west_r, shift(from_w, WEST + 55 - q), ref[r : r + n, :]))))

    kinds = {
        "m": (raw_m.at[0], s_m, de_m, se_m, w_m),
        "s": (side_depth, s_s, de_s, se_s, w_s),
    }

    def fields(kind, spans):
        for r, n in spans:
            wet = (kinds[kind][0][r : r + n, :] > 0.0).astype(F32)
            if kind == "m":
                b_m[0, r : r + n, :] = wet * raw_m[2, r : r + n, :]
                b_m[FIRST, r : r + n, :] = wet * raw_m[1, r : r + n, :]
            else:
                b_s[0, r : r + n, :] = wet * side_state[r : r + n, :]

    def roots(kind, spans):
        depth_ref_, s, de, se, _ = kinds[kind]
        for r, n in spans:
            up, depth, low = (depth_ref_[r + o : r + o + n, :] for o in (1, 0, -1))
            both = up + low
            column = depth + 0.5 * both
            wet_up, wet, wet_low = ((v > 0.0).astype(F32) for v in (up, depth, low))
            both_wet = wet_up + wet_low
            column_wet = wet + 0.5 * both_wet
            all_depth = both + (from_east(column) + from_west(column))
            all_wet = both_wet + (from_east(column_wet) + from_west(column_wet))
            total = 0.5 * (depth * all_wet + all_depth)
            diagonal = wet * (depth * (1.0 / (REACH * REACH)) + total) + (1.0 - wet)
            root = wet * lax.rsqrt(diagonal)
            s[r : r + n, :] = root
            se[r : r + n, :] = from_east(root)
            de[r : r + n, :] = from_east(depth)

    def links(kind, spans):
        depth_ref_, s, de, se, w = kinds[kind]
        for r, n in spans:
            d0, d1 = depth_ref_[r : r + n, :], depth_ref_[r + 1 : r + 1 + n, :]
            s0, s1 = s[r : r + n, :], s[r + 1 : r + 1 + n, :]
            de0, de1 = de[r : r + n, :], de[r + 1 : r + 1 + n, :]
            se0, se1 = se[r : r + n, :], se[r + 1 : r + 1 + n, :]
            east_w = -(d0 + de0) * (s0 * se0)
            ne_w = -0.5 * (d0 + de1) * (s0 * se1)
            nw_e = -0.5 * (de0 + d1) * (se0 * s1)
            w[0, r : r + n, :] = -(d0 + d1) * (s0 * s1)
            w[1, r : r + n, :] = east_w
            w[2, r : r + n, :] = from_west(east_w)
            w[3, r : r + n, :] = ne_w
            w[4, r : r + n, :] = from_west(ne_w)
            w[5, r : r + n, :] = from_west(nw_e)
            w[6, r : r + n, :] = nw_e

    def fold8(x):
        return sum(x[8 * k : 8 * k + 8] for k in range(x.shape[0] // 8))

    lane1 = lanes_of((1, COLS))
    main_lanes = within(lane1, 9, 119)
    strips_p, strips_r = strip_lanes(lane1, 0), strip_lanes(lane1, 64)

    def apply(b, k, w, r, size):
        up, mid, low = (b[k, r + o : r + o + size, :] for o in (1, 0, -1))
        a_u, a_d, e_u, e_c, e_d, f_u, f_c, f_d = w
        east_part = from_east(e_u * up + e_c * mid + e_d * low)
        west_part = from_west(f_u * up + f_c * mid + f_d * low)
        return mid, (a_u * up + a_d * low) + (east_part + west_part)

    def step(n, tasks, first):
        total = {}

        def add(key, product, lo, hi):
            value = fold8(product[lo:hi])
            total[key] = total[key] + value if key in total else value

        for kind, r, size, gram_lo, gram_hi in tasks:
            w = kinds[kind][4]
            weights = (
                w[0, r : r + size, :], w[0, r - 1 : r - 1 + size, :],
                w[4, r : r + size, :], w[2, r : r + size, :], w[5, r - 1 : r - 1 + size, :],
                w[6, r : r + size, :], w[1, r : r + size, :], w[3, r - 1 : r - 1 + size, :],
            )
            b, bases = (b_s, (0,)) if kind == "s" else (b_m, (0, FIRST))
            news, olds = [], []
            for base in bases:
                mid, out = apply(b, base + n - 1, weights, r, size)
                out = 0.5 * out if first else out - b[base + n - 2, r : r + size, :]
                b[base + n, r : r + size, :] = out
                news.append(out)
                olds.append(mid)
            lo, hi = max(r, gram_lo) - r, min(r + size, gram_hi) - r
            if hi <= lo:
                continue
            p1, p0 = news[0], olds[0]
            if kind == "s":
                add("s0", p1 * p1, lo, hi)
                add("s1", p1 * p0, lo, hi)
                add("s4", p1 * shift(p1, 64), lo, hi)
                add("s5", p1 * shift(p0, 64), lo, hi)
                continue
            r1, r0 = news[1], olds[1]
            for c, product in enumerate((p1 * p1, p1 * p0, r1 * r1, r1 * r0, p1 * r1, p1 * r0)):
                add("m%d" % c, product, lo, hi)
        gather(n, total)

    def gather(n, total):
        rows = {key: jnp.sum(value, axis=0, keepdims=True) for key, value in total.items()}
        for c in range(6):
            row = jnp.zeros((1, COLS), F32)
            if "m%d" % c in rows:
                row = jnp.where(main_lanes, rows["m%d" % c], row)
            source = "s%d" % (c - 2 if c in (2, 3) else c)
            if source in rows:
                row = row + jnp.where(strips_r if c in (2, 3) else strips_p, rows[source], 0.0)
            at = pl.ds(6 * n + c, 1)
            rows_acc[at, :] = rows_acc[at, :] + row

    def steps(tasks):
        step(1, tasks, True)

        @pl.loop(2, STEPS + 1)
        def _(n):
            step(n, tasks, False)

    def tasks(kind, start, stop, gram_lo, gram_hi):
        return [(kind, r, n, gram_lo, gram_hi) for r, n in chunks(start, stop)]

    own_strips(chunks(16, 176))
    fields("m", chunks(16, 176))
    roots("m", [(17, 7)] + chunks(24, 168) + [(168, 7)])
    links("m", chunks(16, 168))

    @pl.when(jnp.logical_not(top))
    def _():
        next_level(1)

    start = {}
    for r, n in chunks(16, 176):
        p0, r0 = b_m[0, r : r + n, :], b_m[FIRST, r : r + n, :]
        for key, value in (("m0", p0 * p0), ("m2", r0 * r0), ("m4", p0 * r0)):
            start[key] = start[key] + fold8(value) if key in start else fold8(value)
    gather(0, start)

    @pl.when(jnp.logical_not(top))
    def _():
        next_level(2)

    steps(tasks("m", 16, 168, 32, 160))

    to_east.wait()
    to_west.wait()
    for g in range(4):
        at = 32 * g
        far_strips(16 + 40 * g, 40, got_e[...], got_w[...], (at, at + 9, at + 18))
    fields("s", chunks(16, 176))
    start = {}
    for r, n in chunks(16, 176):
        p0 = b_s[0, r : r + n, :]
        for key, value in (("s0", p0 * p0), ("s4", p0 * shift(p0, 64))):
            start[key] = start[key] + fold8(value) if key in start else fold8(value)
    gather(0, start)

    roots("s", [(17, 7)] + chunks(24, 168) + [(168, 7)])
    links("s", chunks(16, 168))
    steps(tasks("s", 16, 168, 32, 160))

    @pl.when(jnp.logical_not(bottom))
    def _():
        to_se.wait_send()
        to_sw.wait_send()
        to_south.wait_send()
        to_ne.wait_recv()
        to_nw.wait_recv()
        to_north.wait_recv()
        own_strips([(0, 16)])
        far_strips(0, 16, corner[1], corner[0], (96, 105, 114))

    @pl.when(bottom)
    def _():
        for f in range(3):
            raw_m[f, 0:16, :] = jnp.zeros((16, COLS), F32)
        side_depth[0:16, :] = jnp.zeros((16, COLS), F32)
        side_state[0:16, :] = jnp.zeros((16, COLS), F32)

    @pl.when(jnp.logical_not(top))
    def _():
        to_ne.wait_send()
        to_nw.wait_send()
        to_north.wait_send()
        to_se.wait_recv()
        to_sw.wait_recv()
        to_south.wait_recv()
        own_strips([(176, 16)])
        far_strips(176, 16, corner[3], corner[2], (0, 9, 18))

    @pl.when(top)
    def _():
        for copy in fold_z_copies:
            copy.wait_recv()
        ghost = fold_got[0]
        for k in range(1, NZ):
            ghost = ghost + fold_got[k]
        edges = ghost[32:40]
        lane8 = lanes_of((8, COLS))
        side = []
        for g in range(4):
            edge = pltpu.roll(edges, (COLS - 16 - 32 * g) % COLS, 1)
            side.append(jnp.where((lane8 < 9) | (lane8 >= 119), edge, 0.0))
        side = jnp.concatenate(side, axis=0)
        for f in range(3):
            raw_m[f, 176:192, :] = jnp.zeros((16, COLS), F32)
        raw_m[0, 176:185, :] = ghost[0:9]
        raw_m[1, 176:184, :] = ghost[9:17]
        raw_m[2, 176:184, :] = ghost[17:25]
        own_strips([(176, 16)])
        fold_x[...] = side
        west_p, west_r, east_r = (within(lane1, a, a + 9) for a in (WEST - 9, WEST + 55, 64))
        for ref, p, q, count in ((side_depth, 0, 0, 9), (side_state, 17, 9, 8)):
            one, two = fold_x[p : p + count, :], fold_x[q : q + count, :]
            ref[176 : 176 + count, :] = jnp.where(
                lane1 < 9, one, jnp.where(west_p, shift(one, WEST), jnp.where(
                    east_r, shift(two, 64), jnp.where(
                        west_r, shift(two, WEST + 64), ref[176 : 176 + count, :]))))
        for copy in fold_x_copies + fold_z_copies:
            copy.wait_send()

    for kind in ("m", "s"):
        fields(kind, [(LO, 8), (176, 8)])
        roots(kind, [(LO, 16), (168, 16)])
        links(kind, [(LO, 16), (168, 16)])
    steps([(kind, r, 24, lo, lo + 16) for kind in ("m", "s") for r, lo in ((LO, 16), (160, 160))])

    ones = jnp.ones((8, COLS), F32)
    sums = lax.dot_general(
        ones, rows_acc[...], (((1,), (1,)), ((), ())), precision=HIGHEST, preferred_element_type=F32
    )[0:1]

    def tree(terms):
        while len(terms) > 1:
            terms = [a + b for a, b in zip(terms[::2], terms[1::2])]
        return terms[0]

    second = core == 1
    part[0] = sums
    next_level(levels)
    to_plane = [
        remote(part.at[0], red_p.at[core * LON + lon], rp_send.at[d], rp_recv.at[core * LON + d],
               2 * yi + 1, (lon + d) % LON)
        for d in range(LON)
    ]
    for d in far_first(LON):
        to_plane[d].start()
    count = LAT // 2
    along_y = [(d, c) for d in far_first(count) + [0] for c in (1, 0) if (d, c) != (0, 1)]
    to_lat = [
        remote(part.at[1], red_y.at[yi], ry_send.at[2 * d + c], ry_recv.at[d],
               2 * ((yi + d) % count) + c, lon)
        for d, c in along_y
    ]

    @pl.when(jnp.logical_not(second))
    def _():
        to_plane[0].start()
        to_plane[0].wait_send()

    @pl.when(second)
    def _():
        red_p[LON + lon] = sums
        for c in range(2):
            for d in range(c, LON):
                remote(part.at[0], red_p.at[c * LON + lon], rp_send.at[d], rp_recv.at[c * LON + d],
                       lat, east).wait_recv()
        total = tree([red_p[k] for k in range(2 * LON)])
        part[1] = total
        red_y[yi] = total
        for copy in to_lat:
            copy.start()

    def arrived(d):
        remote(part.at[1], red_y.at[yi], ry_send.at[0], ry_recv.at[d], lat, east).wait_recv()

    @pl.when(jnp.logical_not(second))
    def _():
        arrived(0)

    for d in range(1, count):
        arrived(d)
    moments_out[...] = tree([red_y[k] for k in range(count)])

    @pl.when(second)
    def _():
        for copy in to_lat:
            copy.wait_send()

    for copy in to_plane[1:]:
        copy.wait_send()


def held(shape):
    return pltpu.VMEM(shape, F32)


def basis_and_moments(forcing, search, depth, mask, fold_map):
    vm = pltpu.VMEM
    dma = pltpu.SemaphoreType.DMA
    ext = (EXT, COLS)
    return pl.pallas_call(
        basis_kernel,
        out_shape=(held((FIELDS + 1,) + ext), held((STEPS + 1,) + ext), held((1, COLS))),
        in_specs=[pl.BlockSpec(memory_space=pl.ANY)] * 5,
        out_specs=(pl.BlockSpec(memory_space=vm),) * 3,
        scratch_shapes=[
            pltpu.SMEM((1024,), jnp.int32),
            vm((3,) + ext, F32), vm(ext, F32), vm(ext, F32),
            vm((ROWS, COLS), F32), vm((ROWS, COLS), jnp.int32),
            vm((40, COLS), F32), vm((40, COLS), F32), vm((40, COLS), F32), vm((40, COLS), F32),
            vm((4, 16, COLS), F32),
            vm((32, COLS), F32), vm((32, COLS), F32), vm((NX + 1, 32, COLS), F32),
            vm((NZ, 40, COLS), F32), vm((NZ, 40, COLS), F32),
        ]
        + [vm(ext, F32)] * 6
        + [vm((7,) + ext, F32)] * 2
        + [
            vm((COLS, COLS), F32), vm((2, 1, COLS), F32),
            vm((2 * LON, 1, COLS), F32), vm((LAT // 2, 1, COLS), F32),
            pltpu.SemaphoreType.REGULAR((4,)), dma((5,)), dma((8,)), dma((8,)),
            dma((NZ - 1,)), dma((NZ - 1,)), dma((NX - 1,)), dma((NX - 1,)),
            dma((LON,)), dma((2 * LON,)), dma((LAT,)), dma((LAT // 2,)),
        ],
        compiler_params=pltpu.CompilerParams(collective_id=0, has_side_effects=True),
        name="basis",
    )(fold_map, forcing, search, depth, mask)


def rows_of(shape):
    return lax.broadcasted_iota(jnp.int32, shape, 0)


def applied_to_coords(c):
    row = rows_of(c.shape)
    below = jnp.where(row == 0, 0.0, jnp.where(row == 1, 1.0, 0.5)).astype(F32)
    above = jnp.where(row == c.shape[0] - 1, 0.0, 0.5).astype(F32)
    return c + below * pltpu.roll(c, 1, 0) + above * pltpu.roll(c, c.shape[0] - 1, 0)


def applied_to_moments(m):
    row = rows_of(m.shape)
    up, down = pltpu.roll(m, m.shape[0] - 1, 0), pltpu.roll(m, 1, 0)
    return m + 0.5 * (up + jnp.where(row == 0, up, down))


def moment_rows(raw, kind, count):
    k = rows_of((count, COLS))
    odd = k & 1
    high = jnp.minimum(6 * ((k + 1) >> 1) + 2 * kind + odd, COLS - 1)
    spread = jnp.broadcast_to(raw, (count, COLS))
    base = jnp.where(odd == 1, 7 + 2 * kind, 2 * kind)
    return 2.0 * jnp.take_along_axis(spread, high, axis=1) - jnp.take_along_axis(spread, base, axis=1)


def dot_rows(coords, moments):
    (cp, cr), (mp, mr) = coords, moments
    products = cp * mp[0:16]
    return jnp.sum(products[0:8] + products[8:16] + cr * mr[0:8], axis=0, keepdims=True)


def pair(function, one, two):
    return tuple(function(a, b) for a, b in zip(one, two))


def coordinates(raw):
    search_search = moment_rows(raw, 0, 24)
    residual_residual = moment_rows(raw, 1, 16)
    mixed_long, mixed = moment_rows(raw, 2, 24), moment_rows(raw, 2, 16)
    first16 = (rows_of((16, COLS)) == 0).astype(F32)
    first8 = (rows_of((8, COLS)) == 0).astype(F32)
    p, pm = (first16, jnp.zeros((8, COLS), F32)), (search_search, mixed)
    r, rm = (jnp.zeros((16, COLS), F32), first8), (mixed_long, residual_residual)
    x = (jnp.zeros((16, COLS), F32), jnp.zeros((8, COLS), F32))
    q, qm = tuple(map(applied_to_coords, p)), tuple(map(applied_to_moments, pm))
    norm, curvature = dot_rows(r, rm), dot_rows(p, qm)
    for inner in range(STEPS):
        t = norm / curvature
        x = pair(lambda a, b: a + t * b, x, p)
        r = pair(lambda a, b: a - t * b, r, q)
        if inner == STEPS - 1:
            break
        rm = pair(lambda a, b: a - t * b, rm, qm)
        am = tuple(map(applied_to_moments, rm))
        fresh, own, cross = dot_rows(r, rm), dot_rows(r, am), dot_rows(p, am)
        beta = fresh / norm
        curvature = own + beta * (2.0 * cross + beta * curvature)
        norm = fresh
        p = pair(lambda a, b: a + beta * b, r, p)
        q = tuple(map(applied_to_coords, p))
        qm = pair(lambda a, b: a + beta * b, am, qm)
    return x, r


def combine_kernel(moments_ref, basis_ref, strips_ref, height_ref, residual_ref):
    found = coordinates(moments_ref[...])
    lane1 = lanes_of((1, COLS))
    search_half = within((lane1 + 32) & (COLS - 1), 14, 78)
    size = 32
    for (of_p, of_r), out_ref in zip(found, (height_ref, residual_ref)):
        coords = [of_p[k : k + 1, :] for k in range(FIRST)] + [of_r[k : k + 1, :] for k in range(STEPS)]
        mixed = []
        for n in range(STEPS + 1):
            other = coords[FIRST + n] if n < STEPS else jnp.zeros((1, COLS), F32)
            mixed.append(jnp.where(search_half, coords[n], other))
        for at in range(0, ROWS, size):
            rows = slice(16 + at, 16 + at + size)
            main = sum(coords[k] * basis_ref[k, rows, :] for k in range(FIELDS))
            strip = sum(mixed[n] * strips_ref[n, rows, :] for n in range(STEPS + 1))
            strip = strip + shift(strip, 64)
            out_ref[at : at + size, :] = jnp.where(
                lane1 >= 119, strip, jnp.where(lane1 < 9, shift(strip, -WEST), main)
            )


def per_device(forcing, search, depth, mask, fold_map):
    made = basis_and_moments(forcing, search, depth, mask, fold_map)
    basis, strips, moments = (pltpu.with_memory_space_constraint(v, pltpu.VMEM) for v in made)
    block = jax.ShapeDtypeStruct((ROWS, COLS), F32)
    return pl.pallas_call(
        combine_kernel,
        out_shape=(block, block),
        in_specs=[pl.BlockSpec(memory_space=pltpu.VMEM)] * 3,
        name="combine",
    )(moments, basis, strips)


def solution(mesh):
    return jax.shard_map(
        per_device,
        mesh=mesh,
        in_specs=(P("lat", "lon"),) * 4 + (P(),),
        out_specs=(P("lat", "lon"),) * 2,
        check_vma=False,
    )
```

```python
import functools

import jax
import jax.numpy as jnp
from jax import lax
from jax.experimental import pallas as pl
from jax.experimental.pallas import tpu as pltpu
from jax.sharding import PartitionSpec as P

STEPS = 8
REACH = 256
LAT, LON, NX, NZ = 16, 32, 4, 8
ROWS, COLS = 160, 128
EXT = ROWS + 32
LO = 8
FIELDS = 2 * STEPS + 1
FIRST = STEPS + 1
OTHER = STEPS + 2
HIGHEST = lax.Precision.HIGHEST
F32 = jnp.float32


def lanes_of(shape):
    return lax.broadcasted_iota(jnp.int32, shape, len(shape) - 1)


def from_east(x):
    return pltpu.roll(x, COLS - 1, 1)


def from_west(x):
    return pltpu.roll(x, 1, 1)


def shift(x, by):
    by %= COLS
    return pltpu.roll(x, by, 1) if by else x


WEST = 28


def strip_lanes(lane, half):
    lane = (lane - half) & (COLS - 1)
    return (lane >= 119) | ((lane >= WEST) & (lane < WEST + 9))


def within(lane, start, stop):
    return (lane >= start) & (lane < stop)


def remote(src, dst, send, recv, lat, lon):
    return pltpu.make_async_remote_copy(
        src_ref=src,
        dst_ref=dst,
        send_sem=send,
        recv_sem=recv,
        device_id={"lat": lat, "lon": lon},
        device_id_type=pl.DeviceIdType.MESH,
    )


CHUNK = 16


def far_first(count):
    return sorted(range(1, count), key=lambda d: (-min(d, count - d), d))


def chunks(start, stop):
    return [(r, min(CHUNK, stop - r)) for r in range(start, stop, CHUNK)]


def basis_kernel(
    fold_ref, forcing_ref, search_ref, depth_ref, mask_ref,
    b_m, b_s, moments_out,
    fold_buf, raw_m, side_depth, side_state, depth_buf, mask_buf, pack_w, pack_e, got_w, got_e, corner,
    fold_x, fold_src, fold_row, fold_send, fold_got,
    s_m, s_s, de_m, de_s, se_m, se_s,
    w_m, w_s, rows_acc, part, red_p, red_y,
    plane_sem, local_sem, halo_send, halo_recv, fz_send, fz_recv, fx_send, fx_recv,
    rp_send, rp_recv, ry_send, ry_recv,
):
    lat = lax.axis_index("lat")
    lon = lax.axis_index("lon")
    zi, xi = lon // NX, lon % NX
    core, yi = lat % 2, lat // 2
    top = lat == LAT - 1
    bottom = lat == 0
    north, south = (lat + 1) % LAT, (lat + LAT - 1) % LAT
    east, west = (lon + 1) % LON, (lon + LON - 1) % LON
    barrier = pltpu.get_barrier_semaphore()

    loads = [
        pltpu.make_async_copy(depth_ref, depth_buf, local_sem.at[0]),
        pltpu.make_async_copy(mask_ref, mask_buf, local_sem.at[1]),
        pltpu.make_async_copy(forcing_ref, raw_m.at[1, pl.ds(16, ROWS), :], local_sem.at[2]),
        pltpu.make_async_copy(search_ref, raw_m.at[2, pl.ds(16, ROWS), :], local_sem.at[3]),
        pltpu.make_async_copy(fold_ref.at[pl.ds(0, 1024)], fold_buf, local_sem.at[4]),
    ]
    for copy in loads:
        copy.start()

    def greet(semaphore, to):
        for a, b in to:
            pl.semaphore_signal(
                semaphore, inc=1, device_id={"lat": a, "lon": b}, device_id_type=pl.DeviceIdType.MESH
            )

    def around(far):
        if 2 * far == NZ:
            return [(lat, (lon + NX * far) % LON)]
        to = [(lat, (lon + NX * far) % LON), (lat, (lon + LON - NX * far) % LON)]
        if 2 * far < LAT:
            to += [((lat + 2 * far) % LAT, lon), ((lat + LAT - 2 * far) % LAT, lon)]
        return to

    beside = [(lat, zi * NX + (xi + d) % NX) for d in far_first(NX)]
    beside += [(north, east), (north, west), (south, east), (south, west)]
    beside += [(lat, east), (lat, west), (north, lon), (south, lon)] + around(1)

    beside += [(lat + 1 - 2 * core, zi * NX + (xi + d) % NX) for d in far_first(NX)]
    greet(barrier, beside)

    levels = 3

    def next_level(level):
        if level > 0:
            pl.semaphore_wait(plane_sem.at[level - 1], len(around(1 << (level - 1))))
        if level < levels:
            greet(plane_sem.at[level], around(1 << level))

    rows_acc[...] = jnp.zeros_like(rows_acc)
    for ref, slot in ((b_m, 0), (b_m, OTHER), (b_s, 0)):
        ref[slot] = jnp.zeros((EXT, COLS), F32)
    for copy in loads:
        copy.wait()
    raw_m[0, 16 : 16 + ROWS, :] = depth_buf[...] * mask_buf[...].astype(F32)

    pivot = fold_buf[0]
    pivot_block, pivot_lane = lax.shift_right_logical(pivot, 7), pivot & (COLS - 1)

    @pl.when(top)
    def _():
        fold_x[...] = jnp.zeros_like(fold_x)
        for m in range(9):
            fold_x[m : m + 1, :] = raw_m[0, 175 - m : 176 - m, :]
        for m in range(8):
            fold_x[9 + m : 10 + m, :] = raw_m[1, 175 - m : 176 - m, :]
            fold_x[17 + m : 18 + m, :] = raw_m[2, 175 - m : 176 - m, :]
        source = lax.broadcasted_iota(jnp.int32, (COLS, COLS), 0)
        target = lax.broadcasted_iota(jnp.int32, (COLS, COLS), 1)
        choose = (source == ((pivot - target) & (COLS - 1))).astype(F32)
        turned = jnp.dot(fold_x[...], choose, precision=HIGHEST, preferred_element_type=F32)
        fold_src[...] = turned
        fold_row[xi] = turned
        fold_row[NX] = jnp.zeros_like(turned)

    lane40 = lanes_of((40, COLS))
    acc_w = jnp.zeros((40, COLS), F32)
    acc_e = jnp.zeros((40, COLS), F32)
    for g in range(4):
        for f in range(3):
            at = 32 * g + 9 * f
            block = raw_m[f, 16 + 40 * g : 56 + 40 * g, :]
            here = (lane40 >= at) & (lane40 < at + 9)
            acc_w = jnp.where(here, pltpu.roll(block, at, 1) if at else block, acc_w)
            acc_e = jnp.where(here, pltpu.roll(block, (at - 119) % COLS, 1), acc_e)
    pack_w[...] = acc_w
    pack_e[...] = acc_e

    pl.semaphore_wait(barrier, len(beside))

    fold_x_copies = [
        remote(fold_src, fold_row.at[xi], fx_send.at[d - 1], fx_recv.at[d - 1], lat, zi * NX + (xi + d) % NX)
        for d in range(1, NX)
    ]

    @pl.when(top)
    def _():
        for d in far_first(NX):
            fold_x_copies[d - 1].start()

    to_north = remote(raw_m.at[:, pl.ds(160, 16), :], raw_m.at[:, pl.ds(0, 16), :],
                      halo_send.at[0], halo_recv.at[0], north, lon)
    to_south = remote(raw_m.at[:, pl.ds(16, 16), :], raw_m.at[:, pl.ds(176, 16), :],
                      halo_send.at[1], halo_recv.at[1], south, lon)
    to_east = remote(pack_e, got_w, halo_send.at[2], halo_recv.at[2], lat, east)
    to_west = remote(pack_w, got_e, halo_send.at[3], halo_recv.at[3], lat, west)
    to_ne = remote(pack_e.at[pl.ds(24, 16), :], corner.at[0], halo_send.at[4], halo_recv.at[4], north, east)
    to_nw = remote(pack_w.at[pl.ds(24, 16), :], corner.at[1], halo_send.at[5], halo_recv.at[5], north, west)
    to_se = remote(pack_e.at[pl.ds(0, 16), :], corner.at[2], halo_send.at[6], halo_recv.at[6], south, east)
    to_sw = remote(pack_w.at[pl.ds(0, 16), :], corner.at[3], halo_send.at[7], halo_recv.at[7], south, west)

    to_east.start()
    to_west.start()
    next_level(0)

    @pl.when(jnp.logical_not(top))
    def _():
        to_ne.start()
        to_nw.start()
        to_north.start()

    @pl.when(jnp.logical_not(bottom))
    def _():
        to_se.start()
        to_sw.start()
        to_south.start()

    fold_z_copies = [
        remote(fold_send.at[d], fold_got.at[zi], fz_send.at[d - 1], fz_recv.at[d - 1],
               lat, ((zi + d) % NZ) * NX + xi)
        for d in range(1, NZ)
    ]
    lane32 = lanes_of((32, COLS))
    near = lane32 <= pivot_lane

    @pl.when(top)
    def _():
        next_level(1)
        next_level(2)
        for copy in fold_x_copies:
            copy.wait_recv()
        for d in far_first(NZ) + [0]:
            want = pivot_block - ((zi + d) % NZ) * NX - xi

            def block(b):
                mine = (lax.shift_right_logical(b & (LON - 1), 2) == zi)
                return fold_row[jnp.where(mine, b & (NX - 1), NX)]

            ahead, here, behind, beyond = (block(want + o) for o in (1, 0, -1, -2))
            window = jnp.where(near, here, behind)
            edge = jnp.where(
                lane32 < 9, jnp.where(near, behind, beyond),
                jnp.where(lane32 >= 119, jnp.where(near, ahead, here), 0.0),
            )
            edges = sum(pltpu.roll(edge[8 * g : 8 * g + 8], 16 + 32 * g, 1) for g in range(4))
            if d:
                fold_send[d, 0:32, :] = window
                fold_send[d, 32:40, :] = edges
            else:
                fold_got[zi, 0:32, :] = window
                fold_got[zi, 32:40, :] = edges
        for d in far_first(NZ):
            fold_z_copies[d - 1].start()

    def own_strips(spans):
        for r, n in spans:
            depth, residual, search = (raw_m[f, r : r + n, :] for f in range(3))
            lane = lanes_of((n, COLS))
            west_p, east_r, west_r = (within(lane, a, a + 18) for a in (WEST, 46, WEST + 64))
            east_p = lane >= 110
            for ref, p, q in ((side_depth, depth, depth), (side_state, search, residual)):
                ref[r : r + n, :] = jnp.where(
                    east_p, p, jnp.where(west_p, shift(p, WEST), jnp.where(
                        east_r, shift(q, 64), jnp.where(west_r, shift(q, WEST + 64), 0.0))))

    def far_strips(r, n, from_e, from_w, places):
        lane = lanes_of((n, COLS))
        west_p, east_r, west_r = (within(lane, a, a + 9) for a in (WEST - 9, 64, WEST + 55))
        east_p = lane < 9
        at_d, at_r, at_p = places
        for ref, p, q in ((side_depth, at_d, at_d), (side_state, at_p, at_r)):
            ref[r : r + n, :] = jnp.where(
                east_p, shift(from_e, -p), jnp.where(west_p, shift(from_w, WEST - 9 - p), jnp.where(
                    east_r, shift(from_e, 64 - q), jnp.where(
                        west_r, shift(from_w, WEST + 55 - q), ref[r : r + n, :]))))

    kinds = {
        "m": (raw_m.at[0], s_m, de_m, se_m, w_m),
        "s": (side_depth, s_s, de_s, se_s, w_s),
    }

    def fields(kind, spans):
        for r, n in spans:
            wet = (kinds[kind][0][r : r + n, :] > 0.0).astype(F32)
            if kind == "m":
                b_m[1, r : r + n, :] = wet * raw_m[2, r : r + n, :]
                b_m[OTHER + 1, r : r + n, :] = wet * raw_m[1, r : r + n, :]
            else:
                b_s[1, r : r + n, :] = wet * side_state[r : r + n, :]

    def roots(kind, spans):
        depth_ref_, s, de, se, _ = kinds[kind]
        for r, n in spans:
            up, depth, low = (depth_ref_[r + o : r + o + n, :] for o in (1, 0, -1))
            both = up + low
            column = depth + 0.5 * both
            wet_up, wet, wet_low = ((v > 0.0).astype(F32) for v in (up, depth, low))
            both_wet = wet_up + wet_low
            column_wet = wet + 0.5 * both_wet
            all_depth = both + (from_east(column) + from_west(column))
            all_wet = both_wet + (from_east(column_wet) + from_west(column_wet))
            total = 0.5 * (depth * all_wet + all_depth)
            diagonal = wet * (depth * (1.0 / (REACH * REACH)) + total) + (1.0 - wet)
            root = wet * lax.rsqrt(diagonal)
            s[r : r + n, :] = root
            se[r : r + n, :] = from_east(root)
            de[r : r + n, :] = from_east(depth)

    def links(kind, spans):
        depth_ref_, s, de, se, w = kinds[kind]
        for r, n in spans:
            d0, d1 = depth_ref_[r : r + n, :], depth_ref_[r + 1 : r + 1 + n, :]
            s0, s1 = s[r : r + n, :], s[r + 1 : r + 1 + n, :]
            de0, de1 = de[r : r + n, :], de[r + 1 : r + 1 + n, :]
            se0, se1 = se[r : r + n, :], se[r + 1 : r + 1 + n, :]
            east_w = -(d0 + de0) * (s0 * se0)
            ne_w = -0.5 * (d0 + de1) * (s0 * se1)
            nw_e = -0.5 * (de0 + d1) * (se0 * s1)
            w[0, r : r + n, :] = -(d0 + d1) * (s0 * s1)
            w[1, r : r + n, :] = east_w
            w[2, r : r + n, :] = from_west(east_w)
            w[3, r : r + n, :] = ne_w
            w[4, r : r + n, :] = from_west(ne_w)
            w[5, r : r + n, :] = from_west(nw_e)
            w[6, r : r + n, :] = nw_e

    def fold8(x):
        return sum(x[8 * k : 8 * k + 8] for k in range(x.shape[0] // 8))

    lane1 = lanes_of((1, COLS))
    main_lanes = within(lane1, 9, 119)
    strips_p, strips_r = strip_lanes(lane1, 0), strip_lanes(lane1, 64)

    def apply(b, k, w, r, size):
        up, mid, low = (b[k, r + o : r + o + size, :] for o in (1, 0, -1))
        a_u, a_d, e_u, e_c, e_d, f_u, f_c, f_d = w
        east_part = from_east(e_u * up + e_c * mid + e_d * low)
        west_part = from_west(f_u * up + f_c * mid + f_d * low)
        return mid, (a_u * up + a_d * low) + (east_part + west_part)

    def step(n, tasks):
        scale = jnp.where(n == 1, 0.5, 1.0)
        total = {}

        def add(key, product, lo, hi):
            value = fold8(product[lo:hi])
            total[key] = total[key] + value if key in total else value

        for kind, r, size, gram_lo, gram_hi in tasks:
            w = kinds[kind][4]
            weights = (
                w[0, r : r + size, :], w[0, r - 1 : r - 1 + size, :],
                w[4, r : r + size, :], w[2, r : r + size, :], w[5, r - 1 : r - 1 + size, :],
                w[6, r : r + size, :], w[1, r : r + size, :], w[3, r - 1 : r - 1 + size, :],
            )
            b, bases = (b_s, (0,)) if kind == "s" else (b_m, (0, OTHER))
            news, olds = [], []
            for base in bases:
                mid, out = apply(b, base + n, weights, r, size)
                out = scale * out - b[base + n - 1, r : r + size, :]
                b[base + n + 1, r : r + size, :] = out
                news.append(out)
                olds.append(mid)
            lo, hi = max(r, gram_lo) - r, min(r + size, gram_hi) - r
            if hi <= lo:
                continue
            p1, p0 = news[0], olds[0]
            if kind == "s":
                add("s0", p1 * p1, lo, hi)
                add("s1", p1 * p0, lo, hi)
                add("s4", p1 * shift(p1, 64), lo, hi)
                add("s5", p1 * shift(p0, 64), lo, hi)
                continue
            r1, r0 = news[1], olds[1]
            for c, product in enumerate((p1 * p1, p1 * p0, r1 * r1, r1 * r0, p1 * r1, p1 * r0)):
                add("m%d" % c, product, lo, hi)
        gather(n, total)

    def gather(n, total):
        rows = {key: jnp.sum(value, axis=0, keepdims=True) for key, value in total.items()}
        for c in range(6):
            row = jnp.zeros((1, COLS), F32)
            if "m%d" % c in rows:
                row = jnp.where(main_lanes, rows["m%d" % c], row)
            source = "s%d" % (c - 2 if c in (2, 3) else c)
            if source in rows:
                row = row + jnp.where(strips_r if c in (2, 3) else strips_p, rows[source], 0.0)
            at = pl.ds(6 * n + c, 1)
            rows_acc[at, :] = rows_acc[at, :] + row

    def steps(tasks):
        @pl.loop(1, STEPS + 1)
        def _(n):
            step(n, tasks)

    def tasks(kind, start, stop, gram_lo, gram_hi):
        return [(kind, r, n, gram_lo, gram_hi) for r, n in chunks(start, stop)]

    own_strips(chunks(16, 176))
    fields("m", chunks(16, 176))
    roots("m", [(17, 7)] + chunks(24, 168) + [(168, 7)])
    links("m", chunks(16, 168))

    @pl.when(jnp.logical_not(top))
    def _():
        next_level(1)

    start = {}
    for r, n in chunks(16, 176):
        p0, r0 = b_m[1, r : r + n, :], b_m[OTHER + 1, r : r + n, :]
        for key, value in (("m0", p0 * p0), ("m2", r0 * r0), ("m4", p0 * r0)):
            start[key] = start[key] + fold8(value) if key in start else fold8(value)
    gather(0, start)

    @pl.when(jnp.logical_not(top))
    def _():
        next_level(2)

    steps(tasks("m", 16, 168, 32, 160))

    to_east.wait()
    to_west.wait()
    for g in range(4):
        at = 32 * g
        far_strips(16 + 40 * g, 40, got_e[...], got_w[...], (at, at + 9, at + 18))
    fields("s", chunks(16, 176))
    start = {}
    for r, n in chunks(16, 176):
        p0 = b_s[1, r : r + n, :]
        for key, value in (("s0", p0 * p0), ("s4", p0 * shift(p0, 64))):
            start[key] = start[key] + fold8(value) if key in start else fold8(value)
    gather(0, start)

    roots("s", [(17, 7)] + chunks(24, 168) + [(168, 7)])
    links("s", chunks(16, 168))
    steps(tasks("s", 16, 168, 32, 160))

    @pl.when(jnp.logical_not(bottom))
    def _():
        to_se.wait_send()
        to_sw.wait_send()
        to_south.wait_send()
        to_ne.wait_recv()
        to_nw.wait_recv()
        to_north.wait_recv()
        own_strips([(0, 16)])
        far_strips(0, 16, corner[1], corner[0], (96, 105, 114))

    @pl.when(bottom)
    def _():
        for f in range(3):
            raw_m[f, 0:16, :] = jnp.zeros((16, COLS), F32)
        side_depth[0:16, :] = jnp.zeros((16, COLS), F32)
        side_state[0:16, :] = jnp.zeros((16, COLS), F32)

    @pl.when(jnp.logical_not(top))
    def _():
        to_ne.wait_send()
        to_nw.wait_send()
        to_north.wait_send()
        to_se.wait_recv()
        to_sw.wait_recv()
        to_south.wait_recv()
        own_strips([(176, 16)])
        far_strips(176, 16, corner[3], corner[2], (0, 9, 18))

    @pl.when(top)
    def _():
        for copy in fold_z_copies:
            copy.wait_recv()
        ghost = fold_got[0]
        for k in range(1, NZ):
            ghost = ghost + fold_got[k]
        edges = ghost[32:40]
        lane8 = lanes_of((8, COLS))
        side = []
        for g in range(4):
            edge = pltpu.roll(edges, (COLS - 16 - 32 * g) % COLS, 1)
            side.append(jnp.where((lane8 < 9) | (lane8 >= 119), edge, 0.0))
        side = jnp.concatenate(side, axis=0)
        for f in range(3):
            raw_m[f, 176:192, :] = jnp.zeros((16, COLS), F32)
        raw_m[0, 176:185, :] = ghost[0:9]
        raw_m[1, 176:184, :] = ghost[9:17]
        raw_m[2, 176:184, :] = ghost[17:25]
        own_strips([(176, 16)])
        fold_x[...] = side
        west_p, west_r, east_r = (within(lane1, a, a + 9) for a in (WEST - 9, WEST + 55, 64))
        for ref, p, q, count in ((side_depth, 0, 0, 9), (side_state, 17, 9, 8)):
            one, two = fold_x[p : p + count, :], fold_x[q : q + count, :]
            ref[176 : 176 + count, :] = jnp.where(
                lane1 < 9, one, jnp.where(west_p, shift(one, WEST), jnp.where(
                    east_r, shift(two, 64), jnp.where(
                        west_r, shift(two, WEST + 64), ref[176 : 176 + count, :]))))
        for copy in fold_x_copies + fold_z_copies:
            copy.wait_send()

    for kind in ("m", "s"):
        fields(kind, [(LO, 8), (176, 8)])
        roots(kind, [(LO, 16), (168, 16)])
        links(kind, [(LO, 16), (168, 16)])
    steps([(kind, r, 24, lo, lo + 16) for kind in ("m", "s") for r, lo in ((LO, 16), (160, 160))])

    ones = jnp.ones((8, COLS), F32)
    sums = lax.dot_general(
        ones, rows_acc[...], (((1,), (1,)), ((), ())), precision=HIGHEST, preferred_element_type=F32
    )[0:1]

    def tree(terms):
        while len(terms) > 1:
            terms = [a + b for a, b in zip(terms[::2], terms[1::2])]
        return terms[0]

    second = core == 1
    part[0] = sums
    next_level(levels)
    to_plane = [
        remote(part.at[0], red_p.at[core * LON + lon], rp_send.at[d], rp_recv.at[core * LON + d],
               2 * yi + 1, (lon + d) % LON)
        for d in range(LON)
    ]
    for d in far_first(LON):
        to_plane[d].start()
    count = LAT // 2
    along_y = [(d, c) for d in far_first(count) + [0] for c in (1, 0) if (d, c) != (0, 1)]
    to_lat = [
        remote(part.at[1], red_y.at[yi], ry_send.at[2 * d + c], ry_recv.at[d],
               2 * ((yi + d) % count) + c, lon)
        for d, c in along_y
    ]

    @pl.when(jnp.logical_not(second))
    def _():
        to_plane[0].start()
        to_plane[0].wait_send()

    @pl.when(second)
    def _():
        red_p[LON + lon] = sums
        for c in range(2):
            for d in range(c, LON):
                remote(part.at[0], red_p.at[c * LON + lon], rp_send.at[d], rp_recv.at[c * LON + d],
                       lat, east).wait_recv()
        total = tree([red_p[k] for k in range(2 * LON)])
        part[1] = total
        red_y[yi] = total
        for copy in to_lat:
            copy.start()

    def arrived(d):
        remote(part.at[1], red_y.at[yi], ry_send.at[0], ry_recv.at[d], lat, east).wait_recv()

    @pl.when(jnp.logical_not(second))
    def _():
        arrived(0)

    for d in range(1, count):
        arrived(d)
    moments_out[...] = tree([red_y[k] for k in range(count)])

    @pl.when(second)
    def _():
        for copy in to_lat:
            copy.wait_send()

    for copy in to_plane[1:]:
        copy.wait_send()


def held(shape):
    return pltpu.VMEM(shape, F32)


def basis_and_moments(forcing, search, depth, mask, fold_map):
    vm = pltpu.VMEM
    dma = pltpu.SemaphoreType.DMA
    ext = (EXT, COLS)
    return pl.pallas_call(
        basis_kernel,
        out_shape=(held((2 * OTHER,) + ext), held((OTHER,) + ext), held((1, COLS))),
        in_specs=[pl.BlockSpec(memory_space=pl.ANY)] * 5,
        out_specs=(pl.BlockSpec(memory_space=vm),) * 3,
        scratch_shapes=[
            pltpu.SMEM((1024,), jnp.int32),
            vm((3,) + ext, F32), vm(ext, F32), vm(ext, F32),
            vm((ROWS, COLS), F32), vm((ROWS, COLS), jnp.int32),
            vm((40, COLS), F32), vm((40, COLS), F32), vm((40, COLS), F32), vm((40, COLS), F32),
            vm((4, 16, COLS), F32),
            vm((32, COLS), F32), vm((32, COLS), F32), vm((NX + 1, 32, COLS), F32),
            vm((NZ, 40, COLS), F32), vm((NZ, 40, COLS), F32),
        ]
        + [vm(ext, F32)] * 6
        + [vm((7,) + ext, F32)] * 2
        + [
            vm((COLS, COLS), F32), vm((2, 1, COLS), F32),
            vm((2 * LON, 1, COLS), F32), vm((LAT // 2, 1, COLS), F32),
            pltpu.SemaphoreType.REGULAR((4,)), dma((5,)), dma((8,)), dma((8,)),
            dma((NZ - 1,)), dma((NZ - 1,)), dma((NX - 1,)), dma((NX - 1,)),
            dma((LON,)), dma((2 * LON,)), dma((LAT,)), dma((LAT // 2,)),
        ],
        compiler_params=pltpu.CompilerParams(collective_id=0, has_side_effects=True),
        name="basis",
    )(fold_map, forcing, search, depth, mask)


def rows_of(shape):
    return lax.broadcasted_iota(jnp.int32, shape, 0)


def applied_to_coords(c):
    row = rows_of(c.shape)
    below = jnp.where(row == 0, 0.0, jnp.where(row == 1, 1.0, 0.5)).astype(F32)
    above = jnp.where(row == c.shape[0] - 1, 0.0, 0.5).astype(F32)
    return c + below * pltpu.roll(c, 1, 0) + above * pltpu.roll(c, c.shape[0] - 1, 0)


def applied_to_moments(m):
    row = rows_of(m.shape)
    up, down = pltpu.roll(m, m.shape[0] - 1, 0), pltpu.roll(m, 1, 0)
    return m + 0.5 * (up + jnp.where(row == 0, up, down))


def moment_rows(raw, kind, count):
    k = rows_of((count, COLS))
    odd = k & 1
    high = jnp.minimum(6 * ((k + 1) >> 1) + 2 * kind + odd, COLS - 1)
    spread = jnp.broadcast_to(raw, (count, COLS))
    base = jnp.where(odd == 1, 7 + 2 * kind, 2 * kind)
    return 2.0 * jnp.take_along_axis(spread, high, axis=1) - jnp.take_along_axis(spread, base, axis=1)


def dot_rows(coords, moments):
    (cp, cr), (mp, mr) = coords, moments
    products = cp * mp[0:16]
    return jnp.sum(products[0:8] + products[8:16] + cr * mr[0:8], axis=0, keepdims=True)


def pair(function, one, two):
    return tuple(function(a, b) for a, b in zip(one, two))


def coordinates(raw):
    search_search = moment_rows(raw, 0, 24)
    residual_residual = moment_rows(raw, 1, 16)
    mixed_long, mixed = moment_rows(raw, 2, 24), moment_rows(raw, 2, 16)
    first16 = (rows_of((16, COLS)) == 0).astype(F32)
    first8 = (rows_of((8, COLS)) == 0).astype(F32)
    p, pm = (first16, jnp.zeros((8, COLS), F32)), (search_search, mixed)
    r, rm = (jnp.zeros((16, COLS), F32), first8), (mixed_long, residual_residual)
    x = (jnp.zeros((16, COLS), F32), jnp.zeros((8, COLS), F32))
    q, qm = tuple(map(applied_to_coords, p)), tuple(map(applied_to_moments, pm))
    norm, curvature = dot_rows(r, rm), dot_rows(p, qm)
    for inner in range(STEPS):
        t = norm / curvature
        x = pair(lambda a, b: a + t * b, x, p)
        r = pair(lambda a, b: a - t * b, r, q)
        if inner == STEPS - 1:
            break
        rm = pair(lambda a, b: a - t * b, rm, qm)
        am = tuple(map(applied_to_moments, rm))
        fresh, own, cross = dot_rows(r, rm), dot_rows(r, am), dot_rows(p, am)
        beta = fresh / norm
        curvature = own + beta * (2.0 * cross + beta * curvature)
        norm = fresh
        p = pair(lambda a, b: a + beta * b, r, p)
        q = tuple(map(applied_to_coords, p))
        qm = pair(lambda a, b: a + beta * b, am, qm)
    return x, r


def combine_kernel(moments_ref, basis_ref, strips_ref, height_ref, residual_ref):
    found = coordinates(moments_ref[...])
    lane1 = lanes_of((1, COLS))
    search_half = within((lane1 + 32) & (COLS - 1), 14, 78)
    size = 32
    for (of_p, of_r), out_ref in zip(found, (height_ref, residual_ref)):
        coords = [of_p[k : k + 1, :] for k in range(FIRST)] + [of_r[k : k + 1, :] for k in range(STEPS)]
        mixed = []
        for n in range(STEPS + 1):
            other = coords[FIRST + n] if n < STEPS else jnp.zeros((1, COLS), F32)
            mixed.append(jnp.where(search_half, coords[n], other))
        for at in range(0, ROWS, size):
            rows = slice(16 + at, 16 + at + size)
            main = sum(coords[k] * basis_ref[k + 1 if k < FIRST else OTHER + 1 + k - FIRST, rows, :] for k in range(FIELDS))
            strip = sum(mixed[n] * strips_ref[n + 1, rows, :] for n in range(STEPS + 1))
            strip = strip + shift(strip, 64)
            out_ref[at : at + size, :] = jnp.where(
                lane1 >= 119, strip, jnp.where(lane1 < 9, shift(strip, -WEST), main)
            )


def per_device(forcing, search, depth, mask, fold_map):
    made = basis_and_moments(forcing, search, depth, mask, fold_map)
    basis, strips, moments = (pltpu.with_memory_space_constraint(v, pltpu.VMEM) for v in made)
    block = jax.ShapeDtypeStruct((ROWS, COLS), F32)
    return pl.pallas_call(
        combine_kernel,
        out_shape=(block, block),
        in_specs=[pl.BlockSpec(memory_space=pltpu.VMEM)] * 3,
        name="combine",
    )(moments, basis, strips)


def solution(mesh):
    return jax.shard_map(
        per_device,
        mesh=mesh,
        in_specs=(P("lat", "lon"),) * 4 + (P(),),
        out_specs=(P("lat", "lon"),) * 2,
        check_vma=False,
    )
```
